32 devices in a mesh: groups: 2 (over x), pb: 16 (over z, y, core).
Axes of the slice: x: 2, y: 2, z: 4, core: 2. Of those that a mesh axis runs over, the one named last changes fastest.
Arguments:
- tokens: bfloat16 [6144, 512], P(('groups', 'pb')), parts along dimension 0, may hold values from -6 to 6
- stamps: int32 [6144], P(('groups', 'pb')), parts along dimension 0, may hold values from 0 to 1086324736, as said below
- norm_gain: float32 [512], replicated, may hold values from 0.5 to 1.5
- w_proj: bfloat16 [512, 2048], replicated, may hold values from -0.25 to 0.25
- rel_bias: float32 [8, 16], replicated, may hold values from -1.5 to 1.5
- attn_gain: float32 [512], replicated, may hold values from 0.5 to 1.5
- w_out: bfloat16 [512, 512], replicated, may hold values from -0.25 to 0.25
Outputs:
- mixed: bfloat16 [6144, 512], P(('groups', 'pb')), parts along dimension 0
The draws below stay inside these ranges and needn't reach their ends.
There are 2 independent parts, one for each index of `groups`. The reference program is written for one: setup_inputs(seed, part) draws one part's arguments, and reference() takes and returns one part's arrays. A program takes and returns all parts, laid end to end along the dimension named above; an argument that names none is the same for every part. Nothing has to cross between parts.
Inputs may be any that keep to these rules, and one draw needn't show every extreme that they name: `stamps`: stamps never fall from one row to the next.
All inputs are finite; a program needn't handle non-finite values.
Results may differ from the reference program's by a relative error of at most 0.008.
Values may be sent and summed in bfloat16 or wider, within the bound.
A program may use at most 128 MiB of HBM per device.

```python
import jax
import jax.numpy as jnp
from jax import lax

D = 512
HEADS = 8
HEAD = 64
BUCKETS = 16
TOK_DEV = 192
TOKENS = 3072


def draw_stamps(key, part):
    first_key = jax.random.fold_in(key, 11)
    second_key = jax.random.fold_in(key, 12)
    third_key = jax.random.fold_in(key, 13)
    exponent = jax.random.randint(first_key, (TOKENS,), 0, 13)
    chosen = jax.random.permutation(third_key, TOKENS)[:16]
    jump_bits = jnp.zeros((TOKENS,), jnp.int32).at[chosen].set(13 + jnp.arange(16, dtype=jnp.int32))
    jump_mask = jump_bits > 0
    exponent = jnp.where(jump_mask, jump_bits, exponent)
    ones_row = jnp.ones((TOKENS,), jnp.int32)
    low_end = jnp.where(jump_mask, jnp.left_shift(ones_row, exponent), 0)
    high_end = jnp.where(jump_mask, jnp.left_shift(ones_row, exponent + 1), jnp.left_shift(ones_row, exponent) + 1)
    spacing = jax.random.randint(second_key, (TOKENS,), low_end, high_end)
    running = jnp.cumsum(spacing).astype(jnp.int32)
    top_value = jnp.int32(4096 * TOKENS + 2 ** 30)
    return (running + (top_value - running[-1])).astype(jnp.int32)


def block_scale(key, extent, cuts, low, high):
    def one(position, blocks):
        draws = jax.random.uniform(jax.random.fold_in(jax.random.fold_in(key, 6), position), (blocks,), jnp.float32, low / len(cuts), high / len(cuts))
        return jnp.repeat(jnp.exp(draws), extent[position] // blocks).reshape((-1,) + (1,) * (len(extent) - position - 1))

    level = one(*cuts[0])
    for cut in cuts[1:]:
        level = level * one(*cut)
    return level


def gaussian(own_key, dims, scale, bound, cuts=(), kind=jnp.bfloat16):
    values = jax.random.normal(own_key, dims, jnp.float32) * scale
    if len(cuts) > 0:
        values = block_scale(own_key, dims, cuts, -0.22, 0.18) * values
    return jnp.clip(values, min=-bound, max=bound).astype(kind)


def setup_inputs(seed: int = 0, part: int = 0) -> dict:
    key_of = jax.random.split(jax.random.key(seed), 8)
    part_splits = jax.random.split(jax.random.fold_in(key_of[7], part), 8)
    return {
        "tokens": gaussian(part_splits[0], (TOKENS, D), 1.0, 6.0, ((0, 16),)),
        "stamps": draw_stamps(jax.random.fold_in(jax.random.fold_in(key_of[7], part), 71), part),
        "norm_gain": jnp.clip(1.0 + 0.1 * jax.random.normal(key_of[2], (D,), jnp.float32), 0.5, 1.5),
        "w_proj": gaussian(key_of[3], (D, 4 * D), D ** -0.5, 0.25),
        "rel_bias": jnp.clip(jax.random.uniform(key_of[4], (HEADS, BUCKETS), jnp.float32, -1.5, 1.5), -1.5, 1.5),
        "attn_gain": jnp.clip(1.0 + 0.1 * jax.random.normal(key_of[5], (D,), jnp.float32), 0.5, 1.5),
        "w_out": gaussian(key_of[6], (D, D), D ** -0.5, 0.25),
    }


epsilon = 1e-05

def layer_norm(values, gain):
    centered = values - lax.optimization_barrier(jnp.mean(values, axis=-1, keepdims=True))
    spread = lax.optimization_barrier(jnp.mean(centered * centered, axis=-1, keepdims=True))
    return centered * lax.rsqrt(spread + epsilon) * gain

def bucket_of(elapsed):
    bucket_ids = jnp.zeros(elapsed.shape, jnp.int32)
    for exponent in range(BUCKETS - 1):
        bucket_ids = bucket_ids + (elapsed >= 4 ** exponent).astype(jnp.int32)
    return bucket_ids

def reference(tokens, stamps, norm_gain, w_proj, rel_bias, attn_gain, w_out):
    normed = layer_norm(tokens.astype(jnp.float32), norm_gain).astype(jnp.bfloat16)
    projected = jnp.dot(normed, w_proj, preferred_element_type=jnp.float32)
    gate_vals = jax.nn.silu(projected[:, :D]).astype(jnp.bfloat16)
    queries = projected[:, D:2 * D].astype(jnp.bfloat16)
    key_rows = projected[:, 2 * D:3 * D].astype(jnp.bfloat16)
    value_rows = projected[:, 3 * D:].astype(jnp.bfloat16)
    q_heads = queries.astype(jnp.float32).reshape(TOKENS, HEADS, HEAD)
    k_heads = key_rows.astype(jnp.float32).reshape(TOKENS, HEADS, HEAD)
    v_heads = value_rows.astype(jnp.float32).reshape(TOKENS, HEADS, HEAD)
    positions = jnp.arange(TOKENS, dtype=jnp.int32)

    def one_block(start):
        q_block = lax.dynamic_slice_in_dim(q_heads, start, TOK_DEV, 0)
        q_pos = start + jnp.arange(TOK_DEV, dtype=jnp.int32)
        q_stamp = lax.dynamic_slice_in_dim(stamps, start, TOK_DEV, 0)
        scores = jnp.einsum('qhd,khd->hqk', q_block, k_heads) * HEAD ** (-0.5)
        bucket = bucket_of(q_stamp[:, None] - stamps[None, :])
        scores = scores + rel_bias[:, bucket]
        visible = positions[None, :] <= q_pos[:, None]
        weight = jnp.where(visible[None], jax.nn.silu(scores), 0.0).astype(jnp.bfloat16)
        mixture = jnp.einsum('hqk,khd->qhd', weight.astype(jnp.float32), v_heads)
        return mixture.reshape(TOK_DEV, D)
    block_starts = jnp.arange(0, TOKENS, TOK_DEV, dtype=jnp.int32)
    attended = lax.map(one_block, block_starts).reshape(TOKENS, D)
    gated = (layer_norm(attended, attn_gain) * gate_vals.astype(jnp.float32)).astype(jnp.bfloat16)
    result = tokens.astype(jnp.float32) + jnp.dot(gated, w_out, preferred_element_type=jnp.float32)
    return result.astype(jnp.bfloat16)
```

```python
import functools

import jax
import jax.numpy as jnp
from jax import lax
from jax.experimental import pallas as pl
from jax.experimental.pallas import tpu as pltpu
from jax.sharding import PartitionSpec as P

EPSILON = 1e-05
LANES = 128


def layer_norm(values, gain):
    centered = values - jnp.mean(values, axis=-1, keepdims=True)
    spread = jnp.mean(centered * centered, axis=-1, keepdims=True)
    return centered * lax.rsqrt(spread + EPSILON) * gain


LANE_LOOKUP = lax.GatherDimensionNumbers(
    offset_dims=(),
    collapsed_slice_dims=(1,),
    start_index_map=(1,),
    operand_batching_dims=(0,),
    start_indices_batching_dims=(0,),
)
ROW_LOOKUP = lax.GatherDimensionNumbers(
    offset_dims=(),
    collapsed_slice_dims=(1,),
    start_index_map=(1,),
    operand_batching_dims=(0, 2),
    start_indices_batching_dims=(0, 2),
)


def look_up(table, index, dimensions):
    return lax.gather(
        table,
        index[..., None],
        dimensions,
        (1,) * table.ndim,
        mode=lax.GatherScatterMode.PROMISE_IN_BOUNDS,
    )


def kernel(
    parts,
    heads,
    tokens_hbm,
    stamps_hbm,
    norm_gain_hbm,
    w_proj_hbm,
    bias_hbm,
    attn_gain_hbm,
    w_out_hbm,
    out_ref,
    tokens_ref,
    stamps_ref,
    norm_gain_ref,
    w_proj_ref,
    bias_ref,
    attn_gain_ref,
    w_out_ref,
    kv_send,
    q_send,
    kv_all,
    q_all,
    query_buf,
    stamp_all,
    stamp_keys,
    stamp_rows,
    total_buf,
    gate_buf,
    back_buf,
    att_buf,
    load_sem,
    kv_send_sem,
    q_send_sem,
    fwd_sem,
    kv_sem,
    q_sem,
    stamp_send_sem,
    stamp_sem,
    back_sem,
    att_sem,
):
    rows, width = tokens_ref.shape
    half = rows // 2
    head_size = width // heads
    splits = parts // heads
    slots = heads
    near = slots // 2
    blocks_per_tile = max(1, 384 // rows)
    key_tile = blocks_per_tile * rows
    group_tiles = splits // blocks_per_tile
    buckets = bias_ref.shape[1]

    loads = [
        pltpu.make_async_copy(source, target, load_sem.at[index])
        for index, (source, target) in enumerate(
            [
                (tokens_hbm, tokens_ref),
                (norm_gain_hbm, norm_gain_ref),
                (w_proj_hbm.at[:, width:], w_proj_ref.at[:, width:]),
                (stamps_hbm, stamps_ref),
                (bias_hbm, bias_ref),
                (w_proj_hbm.at[:, :width], w_proj_ref.at[:, :width]),
                (attn_gain_hbm, attn_gain_ref),
                (w_out_hbm, w_out_ref),
            ]
        )
    ]
    for load in loads:
        load.start()

    me = lax.axis_index("pb")
    my_head = me // splits
    my_split = me % splits
    upper = my_head // near
    my_place = my_head % near
    near_first = upper * near
    far_first = near - near_first

    def split_of(block):
        place = block % splits
        odd = (block // splits) % 2
        return place + odd * (splits - 1 - 2 * place)

    def block_of(slot, split):
        odd = slot % 2
        return slot * splits + split + odd * (splits - 1 - 2 * split)

    def remote(source, target, send, receive, device):
        return pltpu.make_async_remote_copy(
            src_ref=source,
            dst_ref=target,
            send_sem=send,
            recv_sem=receive,
            device_id={"pb": device},
            device_id_type=pl.DeviceIdType.MESH,
        )

    barrier = pltpu.get_barrier_semaphore()

    def greet(step, carry):
        other = lax.rem(me + step, parts)
        pl.semaphore_signal(
            barrier, inc=1, device_id={"pb": other}, device_id_type=pl.DeviceIdType.MESH
        )
        return carry

    lax.fori_loop(1, parts, greet, 0)

    low = lax.broadcasted_iota(jnp.int32, (1, LANES), 1) < head_size

    for load in loads[:3]:
        load.wait()
    normed = layer_norm(tokens_ref[...].astype(jnp.float32), norm_gain_ref[...]).astype(jnp.bfloat16)
    front = jnp.dot(normed, w_proj_ref[:, width : 2 * width], preferred_element_type=jnp.float32)
    scaled = front.astype(jnp.bfloat16).astype(jnp.float32) * (0.5 * head_size ** (-0.5))
    back = jnp.dot(normed, w_proj_ref[:, 2 * width :], preferred_element_type=jnp.float32)
    for pair in range(heads // 2):
        cols = slice(pair * LANES, (pair + 1) * LANES)
        key_cols = back[:, :width][:, cols]
        value_cols = back[:, width:][:, cols]
        query_cols = scaled[:, cols]
        kv_send[2 * pair] = jnp.where(
            low, key_cols, pltpu.roll(value_cols, head_size, 1)
        ).astype(jnp.bfloat16)
        kv_send[2 * pair + 1] = jnp.where(
            low, pltpu.roll(key_cols, head_size, 1), value_cols
        ).astype(jnp.bfloat16)
        top, bottom = query_cols[:half], query_cols[half:]
        q_send[2 * pair] = jnp.where(low, top, pltpu.roll(bottom, head_size, 1)).astype(jnp.bfloat16)
        q_send[2 * pair + 1] = jnp.where(low, pltpu.roll(top, head_size, 1), bottom).astype(jnp.bfloat16)
    loads[3].wait()
    loads[4].wait()

    my_home = split_of(me)

    def stamp_copy(target):
        return remote(
            stamps_ref, stamp_all.at[me], stamp_send_sem.at[target], stamp_sem.at[me], target
        )

    def kv_copy(head, target):
        return remote(kv_send.at[head], kv_all.at[me], kv_send_sem.at[head], kv_sem.at[me], target)

    def q_copy(head, target):
        return remote(q_send.at[head], q_all.at[my_head], q_send_sem.at[head], q_sem.at[my_head], target)

    def each_head(first, act):
        def one(step, carry):
            head = first + lax.rem(my_place + step, near)
            target = head * splits + my_home

            @pl.when(target != me)
            def _():
                act(head, target)

            return carry

        lax.fori_loop(0, near, one, 0)

    def send_stamps(step, carry):
        stamp_copy(lax.rem(me + step, parts)).start()
        return carry

    def start_both(head, target):
        q_copy(head, target).start()
        kv_copy(head, target).start()

    pl.semaphore_wait(barrier, parts - 1)
    lax.fori_loop(1, parts, send_stamps, 0)
    each_head(near_first, start_both)
    each_head(far_first, lambda head, target: q_copy(head, target).start())
    each_head(far_first, lambda head, target: kv_copy(head, target).start())

    stamp_all[me] = stamps_ref[...]

    @pl.when(my_home == my_split)
    def _():
        kv_all[me] = kv_send[my_head]
        q_all[my_head] = q_send[my_head]

    loads[5].wait()
    gate_proj = jnp.dot(normed, w_proj_ref[:, :width], preferred_element_type=jnp.float32)
    gate_buf[...] = jax.nn.silu(gate_proj).astype(jnp.bfloat16)
    total_buf[...] = jnp.zeros_like(total_buf)

    def half_bias(bucket):
        table = jnp.zeros((8, LANES), jnp.float32)
        for bucket_id in range(buckets):
            table = jnp.where(bucket == bucket_id, 0.5 * bias_ref[my_head, bucket_id], table)
        return table

    lane_id = lax.broadcasted_iota(jnp.int32, (8, LANES), 1)
    lane_table = half_bias(jnp.clip((33 - lane_id) >> 1, 0, buckets - 1))[:1]
    place_id = lax.broadcasted_iota(jnp.int32, (8, LANES), 0)
    far_table = half_bias(jnp.where(place_id == 0, 8, 16 - place_id))
    close_table = half_bias(jnp.where(place_id == 0, 0, 8 - place_id))

    def bias_of(elapsed, by_rows):
        if not by_rows:
            table = jnp.broadcast_to(lane_table, elapsed.shape)
            return look_up(table, lax.clz(elapsed), LANE_LOOKUP)
        tiles = (elapsed.shape[0] // 8, 8, LANES)
        zeros_count = lax.clz(jnp.minimum(elapsed, 2**30 - 1))
        index = ((zeros_count >> 1) & 7).reshape(tiles)
        far_bias = look_up(jnp.broadcast_to(far_table[None], tiles), index, ROW_LOOKUP)
        close_bias = look_up(jnp.broadcast_to(close_table[None], tiles), index, ROW_LOOKUP)
        return jnp.where(
            elapsed >= 4**7, far_bias.reshape(elapsed.shape), close_bias.reshape(elapsed.shape)
        )

    def wait_stamps(step, carry):
        source = lax.rem(me + step, parts)
        remote(
            stamps_ref, stamp_all.at[source], stamp_send_sem.at[source], stamp_sem.at[source], source
        ).wait_recv()
        return carry

    lax.fori_loop(1, parts, wait_stamps, 0)

    for tile in range(parts // blocks_per_tile):
        stamp_keys[tile] = jnp.concatenate(
            [stamp_all[tile * blocks_per_tile + place] for place in range(blocks_per_tile)], axis=1
        )

    def turn_stamps(slot, carry):
        block = block_of(slot, my_split)
        stamp_rows[slot] = jnp.transpose(jnp.broadcast_to(stamp_all[block], (LANES, rows)))
        return carry

    lax.fori_loop(0, slots, turn_stamps, 0)

    def forward(slot, source, step):
        peer = my_head * splits + lax.rem(my_split + step, splits)
        return remote(
            kv_all.at[source], kv_all.at[source], fwd_sem.at[slot, step], kv_sem.at[source], peer
        )

    def take_direct(slot):
        source = block_of(slot, my_split)

        @pl.when(source != me)
        def _():
            remote(
                kv_send.at[0], kv_all.at[source], kv_send_sem.at[0], kv_sem.at[source], source
            ).wait_recv()

        for step in range(1, splits):
            forward(slot, source, step).start()

    def take_forwarded(slot):
        for step in range(1, splits):
            source = block_of(slot, lax.rem(my_split + step, splits))
            forward(slot, source, step).wait_recv()

    def take_query(slot):
        source = block_of(slot, my_split)

        @pl.when(source != me)
        def _():
            remote(
                q_send.at[0], q_all.at[slot], q_send_sem.at[0], q_sem.at[slot], source
            ).wait_recv()

        packed = q_all[slot].astype(jnp.float32)
        query_buf[slot] = jnp.concatenate(
            [jnp.where(low, packed, 0.0), jnp.where(low, pltpu.roll(packed, head_size, 1), 0.0)], axis=0
        ).astype(jnp.bfloat16)

    chunk = 64
    row_id = lax.broadcasted_iota(jnp.int32, (chunk, LANES), 0)
    col_id = lax.broadcasted_iota(jnp.int32, (chunk, LANES), 1)
    spread = col_id - row_id

    def visit_tile(slot, count, tile, masked):
        key_value = kv_all[pl.ds(tile * blocks_per_tile, blocks_per_tile)]
        key_value = key_value.reshape(key_tile, LANES)
        queries = query_buf[pl.ds(slot, count)].reshape(count * rows, LANES)
        scores = lax.dot_general(
            queries, key_value, (((1,), (1,)), ((), ())), preferred_element_type=jnp.float32
        )
        weights = []
        for first in range(0, key_tile, LANES):
            column = []
            for top in range(0, count * rows, chunk):
                place, start = top // rows, top % rows
                query_stamp = stamp_rows[slot + place, start : start + chunk]
                elapsed = query_stamp - stamp_keys[tile, :, first : first + LANES]
                bias = bias_of(elapsed, (top // chunk + first // LANES) % 3 != 0)
                halved = scores[top : top + chunk, first : first + LANES] + bias
                halved = halved.astype(jnp.bfloat16)
                weight = halved + halved * jnp.tanh(halved)
                if masked and place == 0:
                    ahead = tile * key_tile + first - block_of(slot, my_split) * rows - start
                    weight = jnp.where(spread <= -ahead, weight.astype(jnp.float32), 0.0)
                    weight = weight.astype(jnp.bfloat16)
                column.append(weight)
            weights.append(jnp.concatenate(column, axis=0))
        sums = jnp.dot(
            jnp.concatenate(weights, axis=1), key_value, preferred_element_type=jnp.float32
        )
        total_buf[pl.ds(slot, count)] += sums.reshape(count, rows, LANES)

    def visit(slot, count, group, masked):
        if group_tiles == 1:
            visit_tile(slot, count, group, masked)
            return

        def one(tile, carry):
            visit_tile(slot, count, tile, masked)
            return carry

        lax.fori_loop(group * group_tiles, (group + 1) * group_tiles, one, 0)

    def visit_wedge(group, first):
        for offset in range(near):

            @pl.when(group - first == offset)
            def _():
                visit(group, near - offset, group, True)

    def send_back(slot, target):
        return remote(
            back_buf.at[slot], att_buf.at[my_head], back_sem.at[slot], att_sem.at[my_head], target
        )

    def finish(slot, carry):
        block = block_of(slot, my_split)
        total = total_buf[slot]
        result = jnp.where(low, pltpu.roll(total[:half], head_size, 1), total[half:]).astype(jnp.bfloat16)
        back_buf[slot] = result

        @pl.when(block == me)
        def _():
            att_buf[my_head] = result

        @pl.when(block != me)
        def _():
            send_back(slot, block).start()

        return carry

    def take_near(slot, carry):
        take_direct(slot)
        take_query(slot)
        return carry

    lax.fori_loop(near_first, near_first + near, take_near, 0)

    lower_end = near * (1 - upper)

    def far_at(step):
        return far_first + lax.rem(my_place - step + near, near)

    def stage(step, carry):
        turn, place = step // near, step % near

        @pl.when(step == near)
        def _():
            lax.fori_loop(0, lower_end, finish, 0)
            lax.fori_loop(far_first, far_first + near, far_query, 0)

        far = turn == 2
        group = jnp.where(far, far_at(place), place + jnp.where(turn == 0, near_first, 0))

        @pl.when(step == 2 * near)
        def _():
            take_direct(far_at(0))

        @pl.when(step == 3 * near - 1)
        def _():
            lax.fori_loop(lower_end, group, finish, 0)

        @pl.when(turn != 1)
        def _():
            take_forwarded(group)

        @pl.when(far & (place + 1 < near))
        def _():
            take_direct(far_at(place + 1))

        @pl.when(turn != 1)
        def _():
            visit_wedge(group, jnp.where(far, far_first, near_first))

        @pl.when(turn == 2 - (1 - upper))
        def _():
            visit(near, near, group, False)

        return carry

    def far_query(slot, carry):
        take_query(slot)
        return carry

    lax.fori_loop(0, 3 * near, stage, 0)
    lax.fori_loop(far_at(near - 1), slots, finish, 0)

    def drain_both(head, target):
        q_copy(head, target).wait_send()
        kv_copy(head, target).wait_send()

    each_head(near_first, drain_both)
    each_head(far_first, drain_both)

    def drain(step, carry):
        stamp_copy(lax.rem(me + step, parts)).wait_send()
        return carry

    lax.fori_loop(1, parts, drain, 0)

    def drain_slot(slot, carry):
        source = block_of(slot, my_split)
        for step in range(1, splits):
            forward(slot, source, step).wait_send()

        @pl.when(source != me)
        def _():
            send_back(slot, source).wait_send()

        return carry

    lax.fori_loop(0, slots, drain_slot, 0)
    loads[6].wait()
    loads[7].wait()

    def take_back(step, carry):
        head = lax.rem(my_head + step, heads)
        source = head * splits + my_home

        @pl.when(source != me)
        def _():
            remote(
                back_buf.at[0], att_buf.at[head], back_sem.at[0], att_sem.at[head], source
            ).wait_recv()

        return carry

    lax.fori_loop(0, heads, take_back, 0)

    pieces = []
    for pair in range(heads // 2):
        even = att_buf[2 * pair].astype(jnp.float32)
        odd = att_buf[2 * pair + 1].astype(jnp.float32)
        pieces.append(
            jnp.concatenate(
                [
                    jnp.where(low, even, pltpu.roll(odd, head_size, 1)),
                    jnp.where(low, pltpu.roll(even, head_size, 1), odd),
                ],
                axis=0,
            )
        )
    attended = jnp.concatenate(pieces, axis=1)
    gated = layer_norm(attended, attn_gain_ref[...]) * gate_buf[...].astype(jnp.float32)
    mixed = tokens_ref[...].astype(jnp.float32) + jnp.dot(
        gated.astype(jnp.bfloat16), w_out_ref[...], preferred_element_type=jnp.float32
    )
    out_ref[...] = mixed.astype(jnp.bfloat16)


def solution(mesh):
    parts = mesh.shape["pb"]

    def body(tokens, stamps, norm_gain, w_proj, rel_bias, attn_gain, w_out):
        rows, width = tokens.shape
        heads = rel_bias.shape[0]
        splits = parts // heads
        slots = parts // splits
        blocks_per_tile = max(1, 384 // rows)
        vmem = pl.BlockSpec(memory_space=pltpu.VMEM)
        return pl.pallas_call(
            functools.partial(kernel, parts, heads),
            out_shape=jax.ShapeDtypeStruct((rows, width), jnp.bfloat16),
            in_specs=[pl.BlockSpec(memory_space=pltpu.HBM)] * 7,
            out_specs=vmem,
            scratch_shapes=[
                pltpu.VMEM((rows, width), jnp.bfloat16),
                pltpu.VMEM((1, rows), jnp.int32),
                pltpu.VMEM((1, width), jnp.float32),
                pltpu.VMEM(w_proj.shape, jnp.bfloat16),
                pltpu.SMEM(rel_bias.shape, jnp.float32),
                pltpu.VMEM((1, width), jnp.float32),
                pltpu.VMEM(w_out.shape, jnp.bfloat16),
                pltpu.VMEM((heads, rows, LANES), jnp.bfloat16),
                pltpu.VMEM((heads, rows // 2, LANES), jnp.bfloat16),
                pltpu.VMEM((parts, rows, LANES), jnp.bfloat16),
                pltpu.VMEM((slots, rows // 2, LANES), jnp.bfloat16),
                pltpu.VMEM((slots, rows, LANES), jnp.bfloat16),
                pltpu.VMEM((parts, 1, rows), jnp.int32),
                pltpu.VMEM((parts // blocks_per_tile, 1, blocks_per_tile * rows), jnp.int32),
                pltpu.VMEM((slots, rows, LANES), jnp.int32),
                pltpu.VMEM((slots, rows, LANES), jnp.float32),
                pltpu.VMEM((rows, width), jnp.bfloat16),
                pltpu.VMEM((slots, rows // 2, LANES), jnp.bfloat16),
                pltpu.VMEM((heads, rows // 2, LANES), jnp.bfloat16),
                pltpu.SemaphoreType.DMA((8,)),
                pltpu.SemaphoreType.DMA((heads,)),
                pltpu.SemaphoreType.DMA((heads,)),
                pltpu.SemaphoreType.DMA((slots, splits)),
                pltpu.SemaphoreType.DMA((parts,)),
                pltpu.SemaphoreType.DMA((slots,)),
                pltpu.SemaphoreType.DMA((parts,)),
                pltpu.SemaphoreType.DMA((parts,)),
                pltpu.SemaphoreType.DMA((slots,)),
                pltpu.SemaphoreType.DMA((heads,)),
            ],
            compiler_params=pltpu.CompilerParams(
                collective_id=0, has_side_effects=True
            ),
        )(
            tokens,
            stamps.reshape(1, rows),
            norm_gain.reshape(1, width),
            w_proj,
            rel_bias,
            attn_gain.reshape(1, width),
            w_out,
        )

    return jax.shard_map(
        body,
        mesh=mesh,
        in_specs=(P(("groups", "pb"), None), P(("groups", "pb")), P(), P(), P(), P(), P()),
        out_specs=P(("groups", "pb"), None),
        check_vma=False,
    )
```

```python
import functools

import jax
import jax.numpy as jnp
from jax import lax
from jax.experimental import pallas as pl
from jax.experimental.pallas import tpu as pltpu
from jax.sharding import PartitionSpec as P

EPSILON = 1e-05
LANES = 128


def layer_norm(values, gain):
    centered = values - jnp.mean(values, axis=-1, keepdims=True)
    spread = jnp.mean(centered * centered, axis=-1, keepdims=True)
    return centered * lax.rsqrt(spread + EPSILON) * gain


LANE_LOOKUP = lax.GatherDimensionNumbers(
    offset_dims=(),
    collapsed_slice_dims=(1,),
    start_index_map=(1,),
    operand_batching_dims=(0,),
    start_indices_batching_dims=(0,),
)
ROW_LOOKUP = lax.GatherDimensionNumbers(
    offset_dims=(),
    collapsed_slice_dims=(1,),
    start_index_map=(1,),
    operand_batching_dims=(0, 2),
    start_indices_batching_dims=(0, 2),
)


def look_up(table, index, dimensions):
    return lax.gather(
        table,
        index[..., None],
        dimensions,
        (1,) * table.ndim,
        mode=lax.GatherScatterMode.PROMISE_IN_BOUNDS,
    )


def kernel(
    parts,
    heads,
    tokens_hbm,
    stamps_hbm,
    norm_gain_hbm,
    w_proj_hbm,
    bias_hbm,
    attn_gain_hbm,
    w_out_hbm,
    out_ref,
    tokens_ref,
    stamps_ref,
    norm_gain_ref,
    w_proj_ref,
    bias_ref,
    attn_gain_ref,
    w_out_ref,
    kv_send,
    q_send,
    kv_all,
    q_all,
    query_buf,
    stamp_all,
    stamp_keys,
    stamp_rows,
    total_buf,
    gate_buf,
    back_buf,
    att_buf,
    part_buf,
    load_sem,
    kv_send_sem,
    q_send_sem,
    far_send_sem,
    fwd_sem,
    kv_sem,
    q_sem,
    stamp_send_sem,
    stamp_sem,
    back_sem,
    att_sem,
    part_sem,
):
    rows, width = tokens_ref.shape
    half = rows // 2
    head_size = width // heads
    splits = parts // heads
    near = heads // 2
    side = parts // 2
    blocks_per_tile = max(1, 384 // rows)
    key_tile = blocks_per_tile * rows
    group_tiles = splits // blocks_per_tile
    buckets = bias_ref.shape[1]

    loads = [
        pltpu.make_async_copy(source, target, load_sem.at[index])
        for index, (source, target) in enumerate(
            [
                (tokens_hbm, tokens_ref),
                (norm_gain_hbm, norm_gain_ref),
                (w_proj_hbm.at[:, width:], w_proj_ref.at[:, width:]),
                (stamps_hbm, stamps_ref),
                (bias_hbm, bias_ref),
                (w_proj_hbm.at[:, :width], w_proj_ref.at[:, :width]),
                (attn_gain_hbm, attn_gain_ref),
                (w_out_hbm, w_out_ref),
            ]
        )
    ]
    for load in loads:
        load.start()

    me = lax.axis_index("pb")
    my_group = me // splits
    my_split = me % splits
    upper = my_group // near
    my_place = my_group % near
    near_first = upper * near
    far_first = near - near_first
    side_first = upper * side

    def split_of(block):
        place = block % splits
        odd = (block // splits) % 2
        return place + odd * (splits - 1 - 2 * place)

    def block_of(slot, split):
        odd = slot % 2
        return slot * splits + split + odd * (splits - 1 - 2 * split)

    def remote(source, target, send, receive, device):
        return pltpu.make_async_remote_copy(
            src_ref=source,
            dst_ref=target,
            send_sem=send,
            recv_sem=receive,
            device_id={"pb": device},
            device_id_type=pl.DeviceIdType.MESH,
        )

    barrier = pltpu.get_barrier_semaphore()

    def greet(step, carry):
        other = lax.rem(me + step, parts)
        pl.semaphore_signal(
            barrier, inc=1, device_id={"pb": other}, device_id_type=pl.DeviceIdType.MESH
        )
        return carry

    lax.fori_loop(1, parts, greet, 0)

    low = lax.broadcasted_iota(jnp.int32, (1, LANES), 1) < head_size

    for load in loads[:3]:
        load.wait()
    normed = layer_norm(tokens_ref[...].astype(jnp.float32), norm_gain_ref[...]).astype(jnp.bfloat16)
    front = jnp.dot(normed, w_proj_ref[:, width : 2 * width], preferred_element_type=jnp.float32)
    scaled = front.astype(jnp.bfloat16).astype(jnp.float32) * (0.5 * head_size ** (-0.5))
    back = jnp.dot(normed, w_proj_ref[:, 2 * width :], preferred_element_type=jnp.float32)
    for pair in range(near):
        cols = slice(pair * LANES, (pair + 1) * LANES)
        key_cols = back[:, :width][:, cols]
        value_cols = back[:, width:][:, cols]
        query_cols = scaled[:, cols]
        kv_send[pair, 0] = jnp.where(
            low, key_cols, pltpu.roll(value_cols, head_size, 1)
        ).astype(jnp.bfloat16)
        kv_send[pair, 1] = jnp.where(
            low, pltpu.roll(key_cols, head_size, 1), value_cols
        ).astype(jnp.bfloat16)
        top, bottom = query_cols[:half], query_cols[half:]
        q_send[pair, 0] = jnp.where(low, top, pltpu.roll(bottom, head_size, 1)).astype(jnp.bfloat16)
        q_send[pair, 1] = jnp.where(low, pltpu.roll(top, head_size, 1), bottom).astype(jnp.bfloat16)
    loads[3].wait()
    loads[4].wait()

    my_home = split_of(me)

    def stamp_copy(target):
        return remote(
            stamps_ref, stamp_all.at[me], stamp_send_sem.at[target], stamp_sem.at[me], target
        )

    def kv_copy(place, target):
        return remote(kv_send.at[place], kv_all.at[me], kv_send_sem.at[place], kv_sem.at[me], target)

    def q_copy(place, target):
        return remote(
            q_send.at[place], q_all.at[my_group], q_send_sem.at[place], q_sem.at[my_group], target
        )

    def late_kv_copy(place, target):
        return remote(
            kv_send.at[place, 1], kv_all.at[me, 1], far_send_sem.at[place], kv_sem.at[me], target
        )

    def early_q_copy(place, target):
        return remote(
            q_send.at[place, 0], q_all.at[my_group, 0], far_send_sem.at[place], q_sem.at[my_group], target
        )

    def each_near(act):
        def one(step, carry):
            place = lax.rem(my_place + step, near)
            target = (near_first + place) * splits + my_home

            @pl.when(target != me)
            def _():
                act(place, target)

            return carry

        lax.fori_loop(0, near, one, 0)

    def each_far(act):
        def one(step, carry):
            place = lax.rem(my_place + step, near)
            target = (far_first + place) * splits + my_home

            @pl.when(upper == 0)
            def _():
                act(late_kv_copy(place, target))

            @pl.when(upper == 1)
            def _():
                act(early_q_copy(place, target))

            return carry

        lax.fori_loop(0, near, one, 0)

    def near_peer(step):
        return side_first + lax.rem(me - side_first + step, side)

    def far_peer(step):
        return side - side_first + lax.rem(me - side_first + step, side)

    def send_near_stamps(step, carry):
        stamp_copy(near_peer(step)).start()
        return carry

    def send_far_stamps(step, carry):
        stamp_copy(far_peer(step)).start()
        return carry

    def start_both(place, target):
        q_copy(place, target).start()
        kv_copy(place, target).start()

    pl.semaphore_wait(barrier, parts - 1)
    lax.fori_loop(1, side, send_near_stamps, 0)
    each_near(start_both)
    lax.fori_loop(0, side, send_far_stamps, 0)
    each_far(lambda copy: copy.start())

    stamp_all[me] = stamps_ref[...]

    @pl.when(my_home == my_split)
    def _():
        kv_all[me] = kv_send[my_place]
        q_all[my_group] = q_send[my_place]

    @pl.when(upper == 0)
    def _():
        part_buf[...] = jnp.zeros_like(part_buf)

    loads[5].wait()
    gate_proj = jnp.dot(normed, w_proj_ref[:, :width], preferred_element_type=jnp.float32)
    gate_buf[...] = jax.nn.silu(gate_proj).astype(jnp.bfloat16)
    total_buf[...] = jnp.zeros_like(total_buf)

    lane_id = lax.broadcasted_iota(jnp.int32, (8, LANES), 1)
    place_id = lax.broadcasted_iota(jnp.int32, (8, LANES), 0)

    def tables_of(head):
        def half_bias(bucket):
            table = jnp.zeros((8, LANES), jnp.float32)
            for bucket_id in range(buckets):
                table = jnp.where(bucket == bucket_id, 0.5 * bias_ref[head, bucket_id], table)
            return table

        return (
            half_bias(jnp.clip((33 - lane_id) >> 1, 0, buckets - 1))[:1],
            half_bias(jnp.where(place_id == 0, 8, 16 - place_id)),
            half_bias(jnp.where(place_id == 0, 0, 8 - place_id)),
        )

    near_tables = [tables_of(2 * my_place), tables_of(2 * my_place + 1)]
    square_tables = [tables_of(2 * my_place + upper)]

    def biases_of(elapsed, tables, by_rows):
        if not by_rows:
            index = lax.clz(elapsed)
            return [look_up(jnp.broadcast_to(lane, elapsed.shape), index, LANE_LOOKUP) for lane, _, _ in tables]
        tiles = (elapsed.shape[0] // 8, 8, LANES)
        zeros_count = lax.clz(jnp.minimum(elapsed, 2**30 - 1))
        index = ((zeros_count >> 1) & 7).reshape(tiles)
        old = elapsed >= 4**7
        biases = []
        for _, far_table, close_table in tables:
            far_bias = look_up(jnp.broadcast_to(far_table[None], tiles), index, ROW_LOOKUP)
            close_bias = look_up(jnp.broadcast_to(close_table[None], tiles), index, ROW_LOOKUP)
            biases.append(
                jnp.where(old, far_bias.reshape(elapsed.shape), close_bias.reshape(elapsed.shape))
            )
        return biases

    def wait_stamps(source):
        remote(
            stamps_ref, stamp_all.at[source], stamp_send_sem.at[source], stamp_sem.at[source], source
        ).wait_recv()

    def wait_near_stamps(step, carry):
        wait_stamps(near_peer(step))
        return carry

    def wait_far_stamps(step, carry):
        wait_stamps(far_peer(step))
        return carry

    def join_stamps(tile, carry):
        stamp_keys[tile] = jnp.concatenate(
            [stamp_all[tile * blocks_per_tile + place] for place in range(blocks_per_tile)], axis=1
        )
        return carry

    def turn_stamps(slot, carry):
        block = block_of(slot, my_split)
        stamp_rows[slot] = jnp.transpose(jnp.broadcast_to(stamp_all[block], (LANES, rows)))
        return carry

    lax.fori_loop(1, side, wait_near_stamps, 0)
    lax.fori_loop(near_first * group_tiles, (near_first + near) * group_tiles, join_stamps, 0)
    lax.fori_loop(near_first, near_first + near, turn_stamps, 0)

    def forward(slot, source, step):
        peer = my_group * splits + lax.rem(my_split + step, splits)
        return remote(
            kv_all.at[source], kv_all.at[source], fwd_sem.at[slot, step], kv_sem.at[source], peer
        )

    def late_forward(slot, source, step):
        peer = my_group * splits + lax.rem(my_split + step, splits)
        return remote(
            kv_all.at[source, 1], kv_all.at[source, 1], fwd_sem.at[slot, step], kv_sem.at[source], peer
        )

    def take_direct(slot):
        source = block_of(slot, my_split)

        @pl.when(source != me)
        def _():
            remote(
                kv_send.at[0], kv_all.at[source], kv_send_sem.at[0], kv_sem.at[source], source
            ).wait_recv()

        for step in range(1, splits):
            forward(slot, source, step).start()

    def take_forwarded(slot):
        for step in range(1, splits):
            source = block_of(slot, lax.rem(my_split + step, splits))
            forward(slot, source, step).wait_recv()

    def take_late_direct(slot):
        source = block_of(slot, my_split)
        remote(
            kv_send.at[0, 1], kv_all.at[source, 1], far_send_sem.at[0], kv_sem.at[source], source
        ).wait_recv()
        for step in range(1, splits):
            late_forward(slot, source, step).start()

    def take_late_forwarded(slot):
        for step in range(1, splits):
            source = block_of(slot, lax.rem(my_split + step, splits))
            late_forward(slot, source, step).wait_recv()

    def unpack(packed):
        packed = packed.astype(jnp.float32)
        return jnp.concatenate(
            [jnp.where(low, packed, 0.0), jnp.where(low, pltpu.roll(packed, head_size, 1), 0.0)], axis=0
        ).astype(jnp.bfloat16)

    def take_query(slot):
        source = block_of(slot, my_split)

        @pl.when(source != me)
        def _():
            remote(
                q_send.at[0], q_all.at[slot], q_send_sem.at[0], q_sem.at[slot], source
            ).wait_recv()

        for head in range(2):
            query_buf[head, slot - near_first] = unpack(q_all[slot, head])

    def take_far_query(slot, carry):
        source = block_of(slot, my_split)
        remote(
            q_send.at[0, 0], q_all.at[slot, 0], far_send_sem.at[0], q_sem.at[slot], source
        ).wait_recv()
        query_buf[2, slot - near] = unpack(q_all[slot, 0])
        return carry

    chunk = 64
    row_id = lax.broadcasted_iota(jnp.int32, (chunk, LANES), 0)
    col_id = lax.broadcasted_iota(jnp.int32, (chunk, LANES), 1)
    spread = col_id - row_id

    def visit_tile(slot, count, tile, jobs, tables, masked):
        unit = slot - jnp.where(slot >= near, near, 0)
        key_values, scores = [], []
        for query_head, key_head in jobs:
            key_value = kv_all[pl.ds(tile * blocks_per_tile, blocks_per_tile), key_head]
            key_values.append(key_value.reshape(key_tile, LANES))
            queries = query_buf[query_head, pl.ds(unit, count)].reshape(count * rows, LANES)
            scores.append(
                lax.dot_general(
                    queries,
                    key_values[-1],
                    (((1,), (1,)), ((), ())),
                    preferred_element_type=jnp.float32,
                )
            )
        weights = [[] for _ in jobs]
        for first in range(0, key_tile, LANES):
            columns = [[] for _ in jobs]
            for top in range(0, count * rows, chunk):
                place, start = top // rows, top % rows
                query_stamp = stamp_rows[slot + place, start : start + chunk]
                elapsed = query_stamp - stamp_keys[tile, :, first : first + LANES]
                biases = biases_of(elapsed, tables, (top // chunk + first // LANES) % 3 != 0)
                for score, bias, column in zip(scores, biases, columns):
                    halved = score[top : top + chunk, first : first + LANES] + bias
                    halved = halved.astype(jnp.bfloat16)
                    weight = halved + halved * jnp.tanh(halved)
                    if masked and place == 0:
                        ahead = tile * key_tile + first - block_of(slot, my_split) * rows - start
                        weight = jnp.where(spread <= -ahead, weight.astype(jnp.float32), 0.0)
                        weight = weight.astype(jnp.bfloat16)
                    column.append(weight)
            for weight, column in zip(weights, columns):
                weight.append(jnp.concatenate(column, axis=0))
        for (query_head, _), weight, key_value in zip(jobs, weights, key_values):
            sums = jnp.dot(
                jnp.concatenate(weight, axis=1), key_value, preferred_element_type=jnp.float32
            )
            total_buf[query_head, pl.ds(unit, count)] += sums.reshape(count, rows, LANES)

    def visit(slot, count, group, jobs, tables, masked):
        if group_tiles == 1:
            visit_tile(slot, count, group, jobs, tables, masked)
            return

        def one(tile, carry):
            visit_tile(slot, count, tile, jobs, tables, masked)
            return carry

        lax.fori_loop(group * group_tiles, (group + 1) * group_tiles, one, 0)

    def visit_near(slot, count, group, masked):
        visit(slot, count, group, [(0, 0), (1, 1)], near_tables, masked)

    def back_copy(kind, unit):
        slot = unit + (near if kind == 2 else near_first)
        target, semaphore = (
            (part_buf.at[my_place], part_sem.at[my_place])
            if kind == 2
            else (att_buf.at[2 * my_place + kind], att_sem.at[2 * my_place + kind])
        )
        block = block_of(slot, my_split)
        return block, remote(
            back_buf.at[kind, unit], target, back_sem.at[kind, unit], semaphore, block
        )

    def finish(kind):
        def one(unit, carry):
            block, copy = back_copy(kind, unit)
            total = total_buf[kind, unit]
            result = jnp.where(low, pltpu.roll(total[:half], head_size, 1), total[half:])
            result = result.astype(jnp.bfloat16)
            back_buf[kind, unit] = result
            if kind == 2:
                copy.start()
                return carry

            @pl.when(block == me)
            def _():
                att_buf[2 * my_place + kind] = result

            @pl.when(block != me)
            def _():
                copy.start()

            return carry

        lax.fori_loop(0, near, one, 0)

    def take_near(slot, carry):
        take_direct(slot)
        take_query(slot)
        return carry

    lax.fori_loop(near_first, near_first + near, take_near, 0)

    def near_group(group, carry):
        take_forwarded(group)
        rest = near_first + near - group

        @pl.when(rest == 1)
        def _():
            visit_near(group, 1, group, True)

        @pl.when(rest > 1)
        def _():
            visit_near(group, 2, group, True)

        def two(step, inner):
            visit_near(group + 2 + 2 * step, 2, group, False)
            return inner

        lax.fori_loop(0, (rest - 2) // 2, two, 0)

        @pl.when((rest > 2) & (rest % 2 == 1))
        def _():
            visit_near(group + rest - 1, 1, group, False)

        return carry

    lax.fori_loop(near_first, near_first + near, near_group, 0)
    finish(0)

    @pl.when(upper == 0)
    def _():
        finish(1)

    lax.fori_loop(0, side, wait_far_stamps, 0)

    @pl.when(upper == 0)
    def _():
        lax.fori_loop(near, 2 * near, turn_stamps, 0)
        lax.fori_loop(near, 2 * near, take_far_query, 0)

    def late_at(step):
        return lax.rem(my_place - step + near, near)

    @pl.when(upper == 1)
    def _():
        lax.fori_loop(0, near * group_tiles, join_stamps, 0)
        take_late_direct(late_at(0))

    def square(step, carry):
        group = late_at(step)

        @pl.when(upper == 1)
        def _():
            take_late_forwarded(group)

            @pl.when(step + 1 < near)
            def _():
                take_late_direct(late_at(step + 1))

        visit(near, near, group, [(2 - upper, upper)], square_tables, False)
        return carry

    lax.fori_loop(0, near, square, 0)

    @pl.when(upper == 0)
    def _():
        finish(2)

    @pl.when(upper == 1)
    def _():
        finish(1)

    def drain_both(place, target):
        q_copy(place, target).wait_send()
        kv_copy(place, target).wait_send()

    each_near(drain_both)
    each_far(lambda copy: copy.wait_send())

    def drain(step, carry):
        stamp_copy(lax.rem(me + step, parts)).wait_send()
        return carry

    lax.fori_loop(1, parts, drain, 0)

    def drain_near(slot, carry):
        for step in range(1, splits):
            forward(slot, block_of(slot, my_split), step).wait_send()
        return carry

    def drain_late(slot, carry):
        for step in range(1, splits):
            late_forward(slot, block_of(slot, my_split), step).wait_send()
        return carry

    def drain_back(kind):
        def one(unit, carry):
            block, copy = back_copy(kind, unit)

            @pl.when(block != me)
            def _():
                copy.wait_send()

            return carry

        lax.fori_loop(0, near, one, 0)

    lax.fori_loop(near_first, near_first + near, drain_near, 0)
    drain_back(0)
    drain_back(1)

    @pl.when(upper == 0)
    def _():
        drain_back(2)

    @pl.when(upper == 1)
    def _():
        lax.fori_loop(0, near, drain_late, 0)

    loads[6].wait()
    loads[7].wait()

    def take_back(step, carry):
        place = lax.rem(my_place + step, near)
        source = (near_first + place) * splits + my_home

        @pl.when(source != me)
        def _():
            for head in range(2):
                remote(
                    back_buf.at[0, 0],
                    att_buf.at[2 * place + head],
                    back_sem.at[0, 0],
                    att_sem.at[2 * place + head],
                    source,
                ).wait_recv()

        @pl.when(upper == 1)
        def _():
            remote(
                back_buf.at[0, 0],
                part_buf.at[place],
                back_sem.at[0, 0],
                part_sem.at[place],
                place * splits + my_home,
            ).wait_recv()

        return carry

    lax.fori_loop(0, near, take_back, 0)

    pieces = []
    for pair in range(near):
        even = att_buf[2 * pair].astype(jnp.float32) + part_buf[pair].astype(jnp.float32)
        odd = att_buf[2 * pair + 1].astype(jnp.float32)
        pieces.append(
            jnp.concatenate(
                [
                    jnp.where(low, even, pltpu.roll(odd, head_size, 1)),
                    jnp.where(low, pltpu.roll(even, head_size, 1), odd),
                ],
                axis=0,
            )
        )
    attended = jnp.concatenate(pieces, axis=1)
    gated = layer_norm(attended, attn_gain_ref[...]) * gate_buf[...].astype(jnp.float32)
    mixed = tokens_ref[...].astype(jnp.float32) + jnp.dot(
        gated.astype(jnp.bfloat16), w_out_ref[...], preferred_element_type=jnp.float32
    )
    out_ref[...] = mixed.astype(jnp.bfloat16)


def solution(mesh):
    parts = mesh.shape["pb"]

    def body(tokens, stamps, norm_gain, w_proj, rel_bias, attn_gain, w_out):
        rows, width = tokens.shape
        heads = rel_bias.shape[0]
        splits = parts // heads
        near = heads // 2
        blocks_per_tile = max(1, 384 // rows)
        vmem = pl.BlockSpec(memory_space=pltpu.VMEM)
        return pl.pallas_call(
            functools.partial(kernel, parts, heads),
            out_shape=jax.ShapeDtypeStruct((rows, width), jnp.bfloat16),
            in_specs=[pl.BlockSpec(memory_space=pltpu.HBM)] * 7,
            out_specs=vmem,
            scratch_shapes=[
                pltpu.VMEM((rows, width), jnp.bfloat16),
                pltpu.VMEM((1, rows), jnp.int32),
                pltpu.VMEM((1, width), jnp.float32),
                pltpu.VMEM(w_proj.shape, jnp.bfloat16),
                pltpu.SMEM(rel_bias.shape, jnp.float32),
                pltpu.VMEM((1, width), jnp.float32),
                pltpu.VMEM(w_out.shape, jnp.bfloat16),
                pltpu.VMEM((near, 2, rows, LANES), jnp.bfloat16),
                pltpu.VMEM((near, 2, rows // 2, LANES), jnp.bfloat16),
                pltpu.VMEM((parts, 2, rows, LANES), jnp.bfloat16),
                pltpu.VMEM((heads, 2, rows // 2, LANES), jnp.bfloat16),
                pltpu.VMEM((3, near, rows, LANES), jnp.bfloat16),
                pltpu.VMEM((parts, 1, rows), jnp.int32),
                pltpu.VMEM((parts // blocks_per_tile, 1, blocks_per_tile * rows), jnp.int32),
                pltpu.VMEM((heads, rows, LANES), jnp.int32),
                pltpu.VMEM((3, near, rows, LANES), jnp.float32),
                pltpu.VMEM((rows, width), jnp.bfloat16),
                pltpu.VMEM((3, near, rows // 2, LANES), jnp.bfloat16),
                pltpu.VMEM((heads, rows // 2, LANES), jnp.bfloat16),
                pltpu.VMEM((near, rows // 2, LANES), jnp.bfloat16),
                pltpu.SemaphoreType.DMA((8,)),
                pltpu.SemaphoreType.DMA((near,)),
                pltpu.SemaphoreType.DMA((near,)),
                pltpu.SemaphoreType.DMA((near,)),
                pltpu.SemaphoreType.DMA((heads, splits)),
                pltpu.SemaphoreType.DMA((parts,)),
                pltpu.SemaphoreType.DMA((heads,)),
                pltpu.SemaphoreType.DMA((parts,)),
                pltpu.SemaphoreType.DMA((parts,)),
                pltpu.SemaphoreType.DMA((3, near)),
                pltpu.SemaphoreType.DMA((heads,)),
                pltpu.SemaphoreType.DMA((near,)),
            ],
            compiler_params=pltpu.CompilerParams(
                collective_id=0, has_side_effects=True
            ),
        )(
            tokens,
            stamps.reshape(1, rows),
            norm_gain.reshape(1, width),
            w_proj,
            rel_bias,
            attn_gain.reshape(1, width),
            w_out,
        )

    return jax.shard_map(
        body,
        mesh=mesh,
        in_specs=(P(("groups", "pb"), None), P(("groups", "pb")), P(), P(), P(), P(), P()),
        out_specs=P(("groups", "pb"), None),
        check_vma=False,
    )
```

```python
import functools

import jax
import jax.numpy as jnp
from jax import lax
from jax.experimental import pallas as pl
from jax.experimental.pallas import tpu as pltpu
from jax.sharding import PartitionSpec as P

EPSILON = 1e-05
LANES = 128


def layer_norm(values, gain):
    centered = values - jnp.mean(values, axis=-1, keepdims=True)
    spread = jnp.mean(centered * centered, axis=-1, keepdims=True)
    return centered * lax.rsqrt(spread + EPSILON) * gain


LANE_LOOKUP = lax.GatherDimensionNumbers(
    offset_dims=(),
    collapsed_slice_dims=(1,),
    start_index_map=(1,),
    operand_batching_dims=(0,),
    start_indices_batching_dims=(0,),
)
ROW_LOOKUP = lax.GatherDimensionNumbers(
    offset_dims=(),
    collapsed_slice_dims=(1,),
    start_index_map=(1,),
    operand_batching_dims=(0, 2),
    start_indices_batching_dims=(0, 2),
)


def look_up(table, index, dimensions):
    return lax.gather(
        table,
        index[..., None],
        dimensions,
        (1,) * table.ndim,
        mode=lax.GatherScatterMode.PROMISE_IN_BOUNDS,
    )


def kernel(
    parts,
    heads,
    tokens_hbm,
    stamps_hbm,
    norm_gain_hbm,
    w_proj_hbm,
    bias_hbm,
    attn_gain_hbm,
    w_out_hbm,
    out_ref,
    tokens_ref,
    stamps_ref,
    norm_gain_ref,
    w_proj_ref,
    bias_ref,
    attn_gain_ref,
    w_out_ref,
    kv_send,
    q_send,
    kv_all,
    q_all,
    query_buf,
    stamp_all,
    stamp_keys,
    stamp_rows,
    total_buf,
    gate_buf,
    back_buf,
    att_buf,
    part_buf,
    load_sem,
    kv_send_sem,
    q_send_sem,
    far_send_sem,
    fwd_sem,
    kv_sem,
    q_sem,
    stamp_send_sem,
    stamp_sem,
    back_sem,
    att_sem,
    part_sem,
    far_ready,
):
    rows, width = tokens_ref.shape
    half = rows // 2
    head_size = width // heads
    splits = parts // heads
    near = heads // 2
    side = parts // 2
    blocks_per_tile = max(1, 384 // rows)
    key_tile = blocks_per_tile * rows
    group_tiles = splits // blocks_per_tile
    buckets = bias_ref.shape[1]

    loads = [
        pltpu.make_async_copy(source, target, load_sem.at[index])
        for index, (source, target) in enumerate(
            [
                (tokens_hbm, tokens_ref),
                (norm_gain_hbm, norm_gain_ref),
                (w_proj_hbm.at[:, width:], w_proj_ref.at[:, width:]),
                (stamps_hbm, stamps_ref),
                (bias_hbm, bias_ref),
                (w_proj_hbm.at[:, :width], w_proj_ref.at[:, :width]),
                (attn_gain_hbm, attn_gain_ref),
                (w_out_hbm, w_out_ref),
            ]
        )
    ]
    for load in loads:
        load.start()

    me = lax.axis_index("pb")
    my_group = me // splits
    my_split = me % splits
    upper = my_group // near
    my_place = my_group % near
    near_first = upper * near
    far_first = near - near_first
    side_first = upper * side

    def split_of(block):
        place = block % splits
        odd = (block // splits) % 2
        return place + odd * (splits - 1 - 2 * place)

    def block_of(slot, split):
        odd = slot % 2
        return slot * splits + split + odd * (splits - 1 - 2 * split)

    def remote(source, target, send, receive, device):
        return pltpu.make_async_remote_copy(
            src_ref=source,
            dst_ref=target,
            send_sem=send,
            recv_sem=receive,
            device_id={"pb": device},
            device_id_type=pl.DeviceIdType.MESH,
        )

    barrier = pltpu.get_barrier_semaphore()

    def signal(semaphore, other):
        pl.semaphore_signal(
            semaphore, inc=1, device_id={"pb": other}, device_id_type=pl.DeviceIdType.MESH
        )

    def near_peer(step):
        return side_first + lax.rem(me - side_first + step, side)

    def far_peer(step):
        return side - side_first + lax.rem(me - side_first + step, side)

    def greet(step, carry):
        signal(barrier, near_peer(step))
        return carry

    lax.fori_loop(1, side, greet, 0)
    signal(barrier, far_peer(0))

    low = lax.broadcasted_iota(jnp.int32, (1, LANES), 1) < head_size

    for load in loads[:3]:
        load.wait()
    normed = layer_norm(tokens_ref[...].astype(jnp.float32), norm_gain_ref[...]).astype(jnp.bfloat16)
    front = jnp.dot(normed, w_proj_ref[:, width : 2 * width], preferred_element_type=jnp.float32)
    scaled = front.astype(jnp.bfloat16).astype(jnp.float32) * (0.5 * head_size ** (-0.5))
    back = jnp.dot(normed, w_proj_ref[:, 2 * width :], preferred_element_type=jnp.float32)
    for pair in range(near):
        cols = slice(pair * LANES, (pair + 1) * LANES)
        key_cols = back[:, :width][:, cols]
        value_cols = back[:, width:][:, cols]
        query_cols = scaled[:, cols]
        kv_send[pair, 0] = jnp.where(
            low, key_cols, pltpu.roll(value_cols, head_size, 1)
        ).astype(jnp.bfloat16)
        kv_send[pair, 1] = jnp.where(
            low, pltpu.roll(key_cols, head_size, 1), value_cols
        ).astype(jnp.bfloat16)
        top, bottom = query_cols[:half], query_cols[half:]
        q_send[pair, 0] = jnp.where(low, top, pltpu.roll(bottom, head_size, 1)).astype(jnp.bfloat16)
        q_send[pair, 1] = jnp.where(low, pltpu.roll(top, head_size, 1), bottom).astype(jnp.bfloat16)
    loads[3].wait()
    loads[4].wait()

    my_home = split_of(me)

    def stamp_copy(target):
        return remote(
            stamps_ref, stamp_all.at[me], stamp_send_sem.at[target], stamp_sem.at[me], target
        )

    def kv_copy(place, target):
        return remote(kv_send.at[place], kv_all.at[me], kv_send_sem.at[place], kv_sem.at[me], target)

    def q_copy(place, target):
        return remote(
            q_send.at[place], q_all.at[my_group], q_send_sem.at[place], q_sem.at[my_group], target
        )

    def late_kv_copy(place, target):
        return remote(
            kv_send.at[place, 1], kv_all.at[me, 1], far_send_sem.at[place], kv_sem.at[me], target
        )

    def early_q_copy(place, target):
        return remote(
            q_send.at[place, 0], q_all.at[my_group, 0], far_send_sem.at[place], q_sem.at[my_group], target
        )

    def each_near(act):
        def one(step, carry):
            place = lax.rem(my_place + step, near)
            target = (near_first + place) * splits + my_home

            @pl.when(target != me)
            def _():
                act(place, target)

            return carry

        lax.fori_loop(0, near, one, 0)

    def far_place(step):
        place = step + (my_place % 2) * (1 - 2 * (step % 2))
        return place + upper * (near - 1 - 2 * place)

    def each_far(act):
        def one(step, carry):
            place = far_place(step)
            target = (far_first + place) * splits + my_home

            @pl.when(upper == 0)
            def _():
                act(late_kv_copy(place, target))

            @pl.when(upper == 1)
            def _():
                act(early_q_copy(place, target))

            return carry

        lax.fori_loop(0, near, one, 0)

    def send_near_stamps(step, carry):
        stamp_copy(near_peer(step)).start()
        return carry

    def send_far_stamps(step, carry):
        stamp_copy(far_peer(step)).start()
        return carry

    def start_both(place, target):
        q_copy(place, target).start()
        kv_copy(place, target).start()

    pl.semaphore_wait(barrier, side)

    def pass_on(step, carry):
        signal(far_ready, near_peer(step))
        return carry

    lax.fori_loop(1, side, pass_on, 0)
    lax.fori_loop(1, side, send_near_stamps, 0)
    each_near(start_both)

    stamp_all[me] = stamps_ref[...]

    @pl.when(my_home == my_split)
    def _():
        kv_all[me] = kv_send[my_place]
        q_all[my_group] = q_send[my_place]

    @pl.when(upper == 0)
    def _():
        part_buf[...] = jnp.zeros_like(part_buf)

    loads[5].wait()
    gate_proj = jnp.dot(normed, w_proj_ref[:, :width], preferred_element_type=jnp.float32)
    gate_buf[...] = jax.nn.silu(gate_proj).astype(jnp.bfloat16)
    total_buf[...] = jnp.zeros_like(total_buf)

    pl.semaphore_wait(far_ready, side - 1)
    lax.fori_loop(0, side, send_far_stamps, 0)
    each_far(lambda copy: copy.start())

    lane_id = lax.broadcasted_iota(jnp.int32, (8, LANES), 1)
    place_id = lax.broadcasted_iota(jnp.int32, (8, LANES), 0)

    def tables_of(head):
        def half_bias(bucket):
            table = jnp.zeros((8, LANES), jnp.float32)
            for bucket_id in range(buckets):
                table = jnp.where(bucket == bucket_id, 0.5 * bias_ref[head, bucket_id], table)
            return table

        return (
            half_bias(jnp.clip((33 - lane_id) >> 1, 0, buckets - 1))[:1],
            half_bias(jnp.where(place_id == 0, 8, 16 - place_id)),
            half_bias(jnp.where(place_id == 0, 0, 8 - place_id)),
        )

    near_tables = [tables_of(2 * my_place), tables_of(2 * my_place + 1)]
    square_tables = [tables_of(2 * my_place + upper)]

    def biases_of(elapsed, tables, by_rows):
        if not by_rows:
            index = lax.clz(elapsed)
            return [look_up(jnp.broadcast_to(lane, elapsed.shape), index, LANE_LOOKUP) for lane, _, _ in tables]
        tiles = (elapsed.shape[0] // 8, 8, LANES)
        zeros_count = lax.clz(jnp.minimum(elapsed, 2**30 - 1))
        index = ((zeros_count >> 1) & 7).reshape(tiles)
        old = elapsed >= 4**7
        biases = []
        for _, far_table, close_table in tables:
            far_bias = look_up(jnp.broadcast_to(far_table[None], tiles), index, ROW_LOOKUP)
            close_bias = look_up(jnp.broadcast_to(close_table[None], tiles), index, ROW_LOOKUP)
            biases.append(
                jnp.where(old, far_bias.reshape(elapsed.shape), close_bias.reshape(elapsed.shape))
            )
        return biases

    def wait_stamps(source):
        remote(
            stamps_ref, stamp_all.at[source], stamp_send_sem.at[source], stamp_sem.at[source], source
        ).wait_recv()

    def wait_near_stamps(step, carry):
        wait_stamps(near_peer(step))
        return carry

    def wait_far_stamps(step, carry):
        wait_stamps(far_peer(step))
        return carry

    def join_stamps(tile, carry):
        stamp_keys[tile] = jnp.concatenate(
            [stamp_all[tile * blocks_per_tile + place] for place in range(blocks_per_tile)], axis=1
        )
        return carry

    def turn_stamps(slot, carry):
        block = block_of(slot, my_split)
        stamp_rows[slot] = jnp.transpose(jnp.broadcast_to(stamp_all[block], (LANES, rows)))
        return carry

    lax.fori_loop(1, side, wait_near_stamps, 0)
    lax.fori_loop(near_first * group_tiles, (near_first + near) * group_tiles, join_stamps, 0)
    lax.fori_loop(near_first, near_first + near, turn_stamps, 0)

    def forward(slot, source, step):
        peer = my_group * splits + lax.rem(my_split + step, splits)
        return remote(
            kv_all.at[source], kv_all.at[source], fwd_sem.at[slot, step], kv_sem.at[source], peer
        )

    def late_forward(slot, source, step):
        peer = my_group * splits + lax.rem(my_split + step, splits)
        return remote(
            kv_all.at[source, 1], kv_all.at[source, 1], fwd_sem.at[slot, step], kv_sem.at[source], peer
        )

    def take_direct(slot):
        source = block_of(slot, my_split)

        @pl.when(source != me)
        def _():
            remote(
                kv_send.at[0], kv_all.at[source], kv_send_sem.at[0], kv_sem.at[source], source
            ).wait_recv()

        for step in range(1, splits):
            forward(slot, source, step).start()

    def take_forwarded(slot):
        for step in range(1, splits):
            source = block_of(slot, lax.rem(my_split + step, splits))
            forward(slot, source, step).wait_recv()

    def take_late_direct(slot):
        source = block_of(slot, my_split)
        remote(
            kv_send.at[0, 1], kv_all.at[source, 1], far_send_sem.at[0], kv_sem.at[source], source
        ).wait_recv()
        for step in range(1, splits):
            late_forward(slot, source, step).start()

    def take_late_forwarded(slot):
        for step in range(1, splits):
            source = block_of(slot, lax.rem(my_split + step, splits))
            late_forward(slot, source, step).wait_recv()

    def unpack(packed):
        packed = packed.astype(jnp.float32)
        return jnp.concatenate(
            [jnp.where(low, packed, 0.0), jnp.where(low, pltpu.roll(packed, head_size, 1), 0.0)], axis=0
        ).astype(jnp.bfloat16)

    def take_query(slot):
        source = block_of(slot, my_split)

        @pl.when(source != me)
        def _():
            remote(
                q_send.at[0], q_all.at[slot], q_send_sem.at[0], q_sem.at[slot], source
            ).wait_recv()

        for head in range(2):
            query_buf[head, slot - near_first] = unpack(q_all[slot, head])

    def take_far_query(slot, carry):
        source = block_of(slot, my_split)
        remote(
            q_send.at[0, 0], q_all.at[slot, 0], far_send_sem.at[0], q_sem.at[slot], source
        ).wait_recv()
        query_buf[2, slot - near] = unpack(q_all[slot, 0])
        return carry

    chunk = 64
    row_id = lax.broadcasted_iota(jnp.int32, (chunk, LANES), 0)
    col_id = lax.broadcasted_iota(jnp.int32, (chunk, LANES), 1)
    spread = col_id - row_id

    def visit_tiles(sections, jobs, tables):
        for slot, count, tile, span, masked in sections:
            unit = slot - jnp.where(slot >= near, near, 0)
            keys = span * key_tile
            key_values, scores = [], []
            for query_head, key_head in jobs:
                key_value = kv_all[pl.ds(tile * blocks_per_tile, span * blocks_per_tile), key_head]
                key_values.append(key_value.reshape(keys, LANES))
                queries = query_buf[query_head, pl.ds(unit, count)].reshape(count * rows, LANES)
                scores.append(
                    lax.dot_general(
                        queries,
                        key_values[-1],
                        (((1,), (1,)), ((), ())),
                        preferred_element_type=jnp.float32,
                    )
                )
            weights = [[] for _ in jobs]
            for first in range(0, keys, LANES):
                columns = [[] for _ in jobs]
                key_stamp = stamp_keys[
                    tile + first // key_tile, :, first % key_tile : first % key_tile + LANES
                ]
                for top in range(0, count * rows, chunk):
                    place, start = top // rows, top % rows
                    query_stamp = stamp_rows[slot + place, start : start + chunk]
                    elapsed = query_stamp - key_stamp
                    biases = biases_of(elapsed, tables, (top // chunk + first // LANES) % 3 != 0)
                    for score, bias, column in zip(scores, biases, columns):
                        halved = score[top : top + chunk, first : first + LANES] + bias
                        halved = halved.astype(jnp.bfloat16)
                        weight = halved + halved * jnp.tanh(halved)
                        if masked:
                            ahead = tile * key_tile + first - block_of(slot, my_split) * rows - start
                            weight = jnp.where(spread <= -ahead, weight.astype(jnp.float32), 0.0)
                            weight = weight.astype(jnp.bfloat16)
                        column.append(weight)
                for weight, column in zip(weights, columns):
                    weight.append(jnp.concatenate(column, axis=0))
            for (query_head, _), weight, key_value in zip(jobs, weights, key_values):
                sums = jnp.dot(
                    jnp.concatenate(weight, axis=1), key_value, preferred_element_type=jnp.float32
                )
                total_buf[query_head, pl.ds(unit, count)] += sums.reshape(count, rows, LANES)

    def visit(sections, jobs, tables):
        def one(step, carry):
            visit_tiles(
                [
                    (slot, count, group * group_tiles + span * step, span, masked)
                    for slot, count, group, span, masked in sections
                ],
                jobs,
                tables,
            )
            return carry

        if group_tiles == 1:
            one(0, 0)
        else:
            lax.fori_loop(0, group_tiles, one, 0)

    def visit_near(*pairs):
        visit(
            [
                (jnp.maximum(one, other), 1, jnp.minimum(one, other), 1, masked)
                for one, other, masked in pairs
            ],
            [(0, 0), (1, 1)],
            near_tables,
        )

    def back_copy(kind, unit):
        slot = unit + (near if kind == 2 else near_first)
        target, semaphore = (
            (part_buf.at[my_place], part_sem.at[my_place])
            if kind == 2
            else (att_buf.at[2 * my_place + kind], att_sem.at[2 * my_place + kind])
        )
        block = block_of(slot, my_split)
        return block, remote(
            back_buf.at[kind, unit], target, back_sem.at[kind, unit], semaphore, block
        )

    def finish(kind, first, count):
        def one(unit, carry):
            block, copy = back_copy(kind, unit)
            total = total_buf[kind, unit]
            result = jnp.where(low, pltpu.roll(total[:half], head_size, 1), total[half:])
            result = result.astype(jnp.bfloat16)
            back_buf[kind, unit] = result
            if kind == 2:
                copy.start()
                return carry

            @pl.when(block == me)
            def _():
                att_buf[2 * my_place + kind] = result

            @pl.when(block != me)
            def _():
                copy.start()

            return carry

        lax.fori_loop(first, first + count, one, 0)

    def near_at(step):
        return near_first + lax.rem(my_place - step + near, near)

    take_direct(near_at(0))

    def near_step(step, carry):
        group = near_at(step)

        @pl.when(step + 1 < near)
        def _():
            take_direct(near_at(step + 1))

        @pl.when((step + 1 == near) & (upper == 1))
        def _():
            for late in range(near // 2):
                take_late_direct(near - 1 - late)

        take_forwarded(group)
        take_query(group)

        @pl.when(step == 0)
        def _():
            visit_near((group, group, True))

        @pl.when(step > 0)
        def _():
            visit_near((group, group, True), (group, near_at(step - 1), False))

        def two(pair, inner):
            visit_near((group, near_at(2 * pair), False), (group, near_at(2 * pair + 1), False))
            return inner

        lax.fori_loop(0, jnp.maximum(step - 1, 0) // 2, two, 0)

        @pl.when((step > 1) & (step % 2 == 0))
        def _():
            visit_near((group, near_at(step - 2), False))

        return carry

    lax.fori_loop(0, near, near_step, 0)

    @pl.when(upper == 1)
    def _():
        for late in range(near // 2, near):
            take_late_direct(near - 1 - late)

    finish(0, 0, near)

    @pl.when(upper == 0)
    def _():
        finish(1, 0, near)

    lax.fori_loop(0, side, wait_far_stamps, 0)

    @pl.when(upper == 0)
    def _():
        lax.fori_loop(near, 2 * near, turn_stamps, 0)
        lax.fori_loop(near, 2 * near, take_far_query, 0)

    @pl.when(upper == 1)
    def _():
        lax.fori_loop(0, near * group_tiles, join_stamps, 0)

    halves = near // 2

    def square(step, carry):
        major, minor = step // halves, step % halves
        slots = 2 * jnp.where(upper == 0, major, minor)
        groups = 2 * (halves - 1 - jnp.where(upper == 0, minor, major))

        @pl.when((upper == 1) & (minor == 0))
        def _():
            take_late_forwarded(groups)
            take_late_forwarded(groups + 1)

        visit([(near + slots, 2, groups, 2, False)], [(2 - upper, upper)], square_tables)

        @pl.when((upper == 0) & (minor == halves - 1))
        def _():
            finish(2, slots, 2)

        @pl.when((upper == 1) & (major == halves - 1))
        def _():
            finish(1, slots, 2)

        return carry

    lax.fori_loop(0, halves * halves, square, 0)

    loads[6].wait()
    loads[7].wait()

    def take_back(step, carry):
        place = lax.rem(my_place + step, near)
        source = (near_first + place) * splits + my_home

        @pl.when(source != me)
        def _():
            for head in range(2):
                remote(
                    back_buf.at[0, 0],
                    att_buf.at[2 * place + head],
                    back_sem.at[0, 0],
                    att_sem.at[2 * place + head],
                    source,
                ).wait_recv()

        @pl.when(upper == 1)
        def _():
            remote(
                back_buf.at[0, 0],
                part_buf.at[place],
                back_sem.at[0, 0],
                part_sem.at[place],
                place * splits + my_home,
            ).wait_recv()

        return carry

    lax.fori_loop(0, near, take_back, 0)

    pieces = []
    for pair in range(near):
        even = att_buf[2 * pair].astype(jnp.float32) + part_buf[pair].astype(jnp.float32)
        odd = att_buf[2 * pair + 1].astype(jnp.float32)
        pieces.append(
            jnp.concatenate(
                [
                    jnp.where(low, even, pltpu.roll(odd, head_size, 1)),
                    jnp.where(low, pltpu.roll(even, head_size, 1), odd),
                ],
                axis=0,
            )
        )
    attended = jnp.concatenate(pieces, axis=1)
    gated = layer_norm(attended, attn_gain_ref[...]) * gate_buf[...].astype(jnp.float32)
    mixed = tokens_ref[...].astype(jnp.float32) + jnp.dot(
        gated.astype(jnp.bfloat16), w_out_ref[...], preferred_element_type=jnp.float32
    )
    out_ref[...] = mixed.astype(jnp.bfloat16)

    def drain_both(place, target):
        q_copy(place, target).wait_send()
        kv_copy(place, target).wait_send()

    each_near(drain_both)
    each_far(lambda copy: copy.wait_send())

    def drain(step, carry):
        stamp_copy(lax.rem(me + step, parts)).wait_send()
        return carry

    lax.fori_loop(1, parts, drain, 0)

    def drain_near(slot, carry):
        for step in range(1, splits):
            forward(slot, block_of(slot, my_split), step).wait_send()
        return carry

    def drain_late(slot, carry):
        for step in range(1, splits):
            late_forward(slot, block_of(slot, my_split), step).wait_send()
        return carry

    def drain_back(kind):
        def one(unit, carry):
            block, copy = back_copy(kind, unit)

            @pl.when(block != me)
            def _():
                copy.wait_send()

            return carry

        lax.fori_loop(0, near, one, 0)

    lax.fori_loop(near_first, near_first + near, drain_near, 0)
    drain_back(0)
    drain_back(1)

    @pl.when(upper == 0)
    def _():
        drain_back(2)

    @pl.when(upper == 1)
    def _():
        lax.fori_loop(0, near, drain_late, 0)


def solution(mesh):
    parts = mesh.shape["pb"]

    def body(tokens, stamps, norm_gain, w_proj, rel_bias, attn_gain, w_out):
        rows, width = tokens.shape
        heads = rel_bias.shape[0]
        splits = parts // heads
        near = heads // 2
        blocks_per_tile = max(1, 384 // rows)
        vmem = pl.BlockSpec(memory_space=pltpu.VMEM)
        return pl.pallas_call(
            functools.partial(kernel, parts, heads),
            out_shape=jax.ShapeDtypeStruct((rows, width), jnp.bfloat16),
            in_specs=[pl.BlockSpec(memory_space=pltpu.HBM)] * 7,
            out_specs=vmem,
            scratch_shapes=[
                pltpu.VMEM((rows, width), jnp.bfloat16),
                pltpu.VMEM((1, rows), jnp.int32),
                pltpu.VMEM((1, width), jnp.float32),
                pltpu.VMEM(w_proj.shape, jnp.bfloat16),
                pltpu.SMEM(rel_bias.shape, jnp.float32),
                pltpu.VMEM((1, width), jnp.float32),
                pltpu.VMEM(w_out.shape, jnp.bfloat16),
                pltpu.VMEM((near, 2, rows, LANES), jnp.bfloat16),
                pltpu.VMEM((near, 2, rows // 2, LANES), jnp.bfloat16),
                pltpu.VMEM((parts, 2, rows, LANES), jnp.bfloat16),
                pltpu.VMEM((heads, 2, rows // 2, LANES), jnp.bfloat16),
                pltpu.VMEM((3, near, rows, LANES), jnp.bfloat16),
                pltpu.VMEM((parts, 1, rows), jnp.int32),
                pltpu.VMEM((parts // blocks_per_tile, 1, blocks_per_tile * rows), jnp.int32),
                pltpu.VMEM((heads, rows, LANES), jnp.int32),
                pltpu.VMEM((3, near, rows, LANES), jnp.float32),
                pltpu.VMEM((rows, width), jnp.bfloat16),
                pltpu.VMEM((3, near, rows // 2, LANES), jnp.bfloat16),
                pltpu.VMEM((heads, rows // 2, LANES), jnp.bfloat16),
                pltpu.VMEM((near, rows // 2, LANES), jnp.bfloat16),
                pltpu.SemaphoreType.DMA((8,)),
                pltpu.SemaphoreType.DMA((near,)),
                pltpu.SemaphoreType.DMA((near,)),
                pltpu.SemaphoreType.DMA((near,)),
                pltpu.SemaphoreType.DMA((heads, splits)),
                pltpu.SemaphoreType.DMA((parts,)),
                pltpu.SemaphoreType.DMA((heads,)),
                pltpu.SemaphoreType.DMA((parts,)),
                pltpu.SemaphoreType.DMA((parts,)),
                pltpu.SemaphoreType.DMA((3, near)),
                pltpu.SemaphoreType.DMA((heads,)),
                pltpu.SemaphoreType.DMA((near,)),
                pltpu.SemaphoreType.REGULAR,
            ],
            compiler_params=pltpu.CompilerParams(
                collective_id=0, has_side_effects=True
            ),
        )(
            tokens,
            stamps.reshape(1, rows),
            norm_gain.reshape(1, width),
            w_proj,
            rel_bias,
            attn_gain.reshape(1, width),
            w_out,
        )

    return jax.shard_map(
        body,
        mesh=mesh,
        in_specs=(P(("groups", "pb"), None), P(("groups", "pb")), P(), P(), P(), P(), P()),
        out_specs=P(("groups", "pb"), None),
        check_vma=False,
    )
```

```python
import functools

import jax
import jax.numpy as jnp
from jax import lax
from jax.experimental import pallas as pl
from jax.experimental.pallas import tpu as pltpu
from jax.sharding import PartitionSpec as P

EPSILON = 1e-05
LANES = 128


def layer_norm(values, gain):
    centered = values - jnp.mean(values, axis=-1, keepdims=True)
    spread = jnp.mean(centered * centered, axis=-1, keepdims=True)
    return centered * lax.rsqrt(spread + EPSILON) * gain


LANE_LOOKUP = lax.GatherDimensionNumbers(
    offset_dims=(),
    collapsed_slice_dims=(1,),
    start_index_map=(1,),
    operand_batching_dims=(0,),
    start_indices_batching_dims=(0,),
)
ROW_LOOKUP = lax.GatherDimensionNumbers(
    offset_dims=(),
    collapsed_slice_dims=(1,),
    start_index_map=(1,),
    operand_batching_dims=(0, 2),
    start_indices_batching_dims=(0, 2),
)


def look_up(table, index, dimensions):
    return lax.gather(
        table,
        index[..., None],
        dimensions,
        (1,) * table.ndim,
        mode=lax.GatherScatterMode.PROMISE_IN_BOUNDS,
    )


def kernel(
    parts,
    heads,
    tokens_hbm,
    stamps_hbm,
    norm_gain_hbm,
    w_proj_hbm,
    bias_hbm,
    att_out,
    part_out,
    gate_out,
    tokens_ref,
    stamps_ref,
    norm_gain_ref,
    w_proj_ref,
    bias_ref,
    kv_send,
    q_send,
    kv_all,
    q_all,
    query_buf,
    stamp_all,
    stamp_keys,
    stamp_rows,
    total_buf,
    gate_buf,
    back_buf,
    zero_buf,
    load_sem,
    kv_send_sem,
    q_send_sem,
    far_send_sem,
    fwd_sem,
    kv_sem,
    q_sem,
    stamp_send_sem,
    stamp_sem,
    back_sem,
    att_sem,
    part_sem,
    far_ready,
    own_sem,
):
    rows, width = tokens_ref.shape
    half = rows // 2
    head_size = width // heads
    splits = parts // heads
    near = heads // 2
    side = parts // 2
    blocks_per_tile = max(1, 384 // rows)
    key_tile = blocks_per_tile * rows
    group_tiles = splits // blocks_per_tile
    buckets = bias_ref.shape[1]

    loads = [
        pltpu.make_async_copy(source, target, load_sem.at[index])
        for index, (source, target) in enumerate(
            [
                (tokens_hbm, tokens_ref),
                (norm_gain_hbm, norm_gain_ref),
                (w_proj_hbm.at[:, width:], w_proj_ref.at[:, width:]),
                (stamps_hbm, stamps_ref),
                (bias_hbm, bias_ref),
                (w_proj_hbm.at[:, :width], w_proj_ref.at[:, :width]),
            ]
        )
    ]
    for load in loads:
        load.start()

    me = lax.axis_index("pb")
    my_group = me // splits
    my_split = me % splits
    upper = my_group // near
    my_place = my_group % near
    near_first = upper * near
    far_first = near - near_first
    side_first = upper * side

    def split_of(block):
        place = block % splits
        odd = (block // splits) % 2
        return place + odd * (splits - 1 - 2 * place)

    def block_of(slot, split):
        odd = slot % 2
        return slot * splits + split + odd * (splits - 1 - 2 * split)

    def remote(source, target, send, receive, device):
        return pltpu.make_async_remote_copy(
            src_ref=source,
            dst_ref=target,
            send_sem=send,
            recv_sem=receive,
            device_id={"pb": device},
            device_id_type=pl.DeviceIdType.MESH,
        )

    barrier = pltpu.get_barrier_semaphore()

    def signal(semaphore, other):
        pl.semaphore_signal(
            semaphore, inc=1, device_id={"pb": other}, device_id_type=pl.DeviceIdType.MESH
        )

    def near_peer(step):
        return side_first + lax.rem(me - side_first + step, side)

    def far_peer(step):
        return side - side_first + lax.rem(me - side_first + step, side)

    def greet(step, carry):
        signal(barrier, near_peer(step))
        return carry

    lax.fori_loop(1, side, greet, 0)
    signal(barrier, far_peer(0))

    low = lax.broadcasted_iota(jnp.int32, (1, LANES), 1) < head_size

    for load in loads[:3]:
        load.wait()
    normed = layer_norm(tokens_ref[...].astype(jnp.float32), norm_gain_ref[...]).astype(jnp.bfloat16)
    front = jnp.dot(normed, w_proj_ref[:, width : 2 * width], preferred_element_type=jnp.float32)
    scaled = front.astype(jnp.bfloat16).astype(jnp.float32) * (0.5 * head_size ** (-0.5))
    back = jnp.dot(normed, w_proj_ref[:, 2 * width :], preferred_element_type=jnp.float32)
    for pair in range(near):
        cols = slice(pair * LANES, (pair + 1) * LANES)
        key_cols = back[:, :width][:, cols]
        value_cols = back[:, width:][:, cols]
        query_cols = scaled[:, cols]
        kv_send[pair, 0] = jnp.where(
            low, key_cols, pltpu.roll(value_cols, head_size, 1)
        ).astype(jnp.bfloat16)
        kv_send[pair, 1] = jnp.where(
            low, pltpu.roll(key_cols, head_size, 1), value_cols
        ).astype(jnp.bfloat16)
        top, bottom = query_cols[:half], query_cols[half:]
        q_send[pair, 0] = jnp.where(low, top, pltpu.roll(bottom, head_size, 1)).astype(jnp.bfloat16)
        q_send[pair, 1] = jnp.where(low, pltpu.roll(top, head_size, 1), bottom).astype(jnp.bfloat16)
    loads[3].wait()
    loads[4].wait()

    my_home = split_of(me)

    def stamp_copy(target):
        return remote(
            stamps_ref, stamp_all.at[me], stamp_send_sem.at[target], stamp_sem.at[me], target
        )

    def kv_copy(place, target):
        return remote(kv_send.at[place], kv_all.at[me], kv_send_sem.at[place], kv_sem.at[me], target)

    def q_copy(place, target):
        return remote(
            q_send.at[place], q_all.at[my_group], q_send_sem.at[place], q_sem.at[my_group], target
        )

    def late_kv_copy(place, target):
        return remote(
            kv_send.at[place, 1], kv_all.at[me, 1], far_send_sem.at[place], kv_sem.at[me], target
        )

    def early_q_copy(place, target):
        return remote(
            q_send.at[place, 0], q_all.at[my_group, 0], far_send_sem.at[place], q_sem.at[my_group], target
        )

    def each_near(act):
        def one(step, carry):
            place = my_place ^ jnp.where(step == 0, 0, near - step)
            target = (near_first + place) * splits + my_home

            @pl.when(target != me)
            def _():
                act(place, target)

            return carry

        lax.fori_loop(0, near, one, 0)

    def far_place(step):
        place = step + (my_place % 2) * (1 - 2 * (step % 2))
        return place + upper * (near - 1 - 2 * place)

    def each_far(first, count, act):
        def one(step, carry):
            place = far_place(step)
            target = (far_first + place) * splits + my_home

            @pl.when(upper == 0)
            def _():
                act(late_kv_copy(place, target))

            @pl.when(upper == 1)
            def _():
                act(early_q_copy(place, target))

            return carry

        lax.fori_loop(first, first + count, one, 0)

    def send_near_stamps(step, carry):
        stamp_copy(near_peer(step)).start()
        return carry

    def send_far_stamps(step, carry):
        stamp_copy(far_peer(step)).start()
        return carry

    def start_both(place, target):
        q_copy(place, target).start()
        kv_copy(place, target).start()

    pl.semaphore_wait(barrier, side)

    def pass_on(step, carry):
        signal(far_ready, near_peer(step))
        return carry

    lax.fori_loop(1, side, pass_on, 0)
    lax.fori_loop(1, side, send_near_stamps, 0)
    each_near(start_both)

    stamp_all[me] = stamps_ref[...]

    @pl.when(my_home == my_split)
    def _():
        kv_all[me] = kv_send[my_place]
        q_all[my_group] = q_send[my_place]

    gate_store = pltpu.make_async_copy(gate_buf, gate_out, own_sem.at[2])
    no_part = pltpu.make_async_copy(zero_buf, part_out, own_sem.at[3])

    @pl.when(upper == 0)
    def _():
        zero_buf[...] = jnp.zeros_like(zero_buf)
        no_part.start()

    loads[5].wait()
    gate_proj = jnp.dot(normed, w_proj_ref[:, :width], preferred_element_type=jnp.float32)
    gate_buf[...] = jax.nn.silu(gate_proj).astype(jnp.bfloat16)
    gate_store.start()
    total_buf[...] = jnp.zeros_like(total_buf)

    pl.semaphore_wait(far_ready, side - 1)
    lax.fori_loop(0, side, send_far_stamps, 0)
    each_far(0, near // 2, lambda copy: copy.start())

    lane_id = lax.broadcasted_iota(jnp.int32, (8, LANES), 1)
    place_id = lax.broadcasted_iota(jnp.int32, (8, LANES), 0)

    def tables_of(head):
        def half_bias(bucket):
            table = jnp.zeros((8, LANES), jnp.float32)
            for bucket_id in range(buckets):
                table = jnp.where(bucket == bucket_id, 0.5 * bias_ref[head, bucket_id], table)
            return table

        return (
            half_bias(jnp.clip((33 - lane_id) >> 1, 0, buckets - 1))[:1],
            half_bias(jnp.where(place_id == 0, 8, 16 - place_id)),
            half_bias(jnp.where(place_id == 0, 0, 8 - place_id)),
        )

    near_tables = [tables_of(2 * my_place), tables_of(2 * my_place + 1)]
    square_tables = [tables_of(2 * my_place + upper)]

    def biases_of(elapsed, tables, by_rows):
        if not by_rows:
            index = lax.clz(elapsed)
            return [look_up(jnp.broadcast_to(lane, elapsed.shape), index, LANE_LOOKUP) for lane, _, _ in tables]
        tiles = (elapsed.shape[0] // 8, 8, LANES)
        zeros_count = lax.clz(jnp.minimum(elapsed, 2**30 - 1))
        index = ((zeros_count >> 1) & 7).reshape(tiles)
        old = elapsed >= 4**7
        biases = []
        for _, far_table, close_table in tables:
            far_bias = look_up(jnp.broadcast_to(far_table[None], tiles), index, ROW_LOOKUP)
            close_bias = look_up(jnp.broadcast_to(close_table[None], tiles), index, ROW_LOOKUP)
            biases.append(
                jnp.where(old, far_bias.reshape(elapsed.shape), close_bias.reshape(elapsed.shape))
            )
        return biases

    def wait_stamps(source):
        remote(
            stamps_ref, stamp_all.at[source], stamp_send_sem.at[source], stamp_sem.at[source], source
        ).wait_recv()

    def wait_near_stamps(step, carry):
        wait_stamps(near_peer(step))
        return carry

    def wait_far_stamps(step, carry):
        wait_stamps(far_peer(step))
        return carry

    def join_stamps(tile, carry):
        stamp_keys[tile] = jnp.concatenate(
            [stamp_all[tile * blocks_per_tile + place] for place in range(blocks_per_tile)], axis=1
        )
        return carry

    def turn_stamps(slot, carry):
        block = block_of(slot, my_split)
        stamp_rows[slot] = jnp.transpose(jnp.broadcast_to(stamp_all[block], (LANES, rows)))
        return carry

    lax.fori_loop(1, side, wait_near_stamps, 0)
    lax.fori_loop(near_first * group_tiles, (near_first + near) * group_tiles, join_stamps, 0)
    lax.fori_loop(near_first, near_first + near, turn_stamps, 0)

    def forward(slot, source, step):
        peer = my_group * splits + lax.rem(my_split + step, splits)
        return remote(
            kv_all.at[source], kv_all.at[source], fwd_sem.at[slot, step], kv_sem.at[source], peer
        )

    def late_forward(slot, source, step):
        peer = my_group * splits + lax.rem(my_split + step, splits)
        return remote(
            kv_all.at[source, 1], kv_all.at[source, 1], fwd_sem.at[slot, step], kv_sem.at[source], peer
        )

    def take_direct(slot):
        source = block_of(slot, my_split)

        @pl.when(source != me)
        def _():
            remote(
                kv_send.at[0], kv_all.at[source], kv_send_sem.at[0], kv_sem.at[source], source
            ).wait_recv()

        for step in range(1, splits):
            forward(slot, source, step).start()

    def take_forwarded(slot):
        for step in range(1, splits):
            source = block_of(slot, lax.rem(my_split + step, splits))
            forward(slot, source, step).wait_recv()

    def take_late_direct(slot):
        source = block_of(slot, my_split)
        remote(
            kv_send.at[0, 1], kv_all.at[source, 1], far_send_sem.at[0], kv_sem.at[source], source
        ).wait_recv()
        for step in range(1, splits):
            late_forward(slot, source, step).start()

    def take_late_forwarded(slot):
        for step in range(1, splits):
            source = block_of(slot, lax.rem(my_split + step, splits))
            late_forward(slot, source, step).wait_recv()

    def unpack(packed):
        packed = packed.astype(jnp.float32)
        return jnp.concatenate(
            [jnp.where(low, packed, 0.0), jnp.where(low, pltpu.roll(packed, head_size, 1), 0.0)], axis=0
        ).astype(jnp.bfloat16)

    def take_query(slot):
        source = block_of(slot, my_split)

        @pl.when(source != me)
        def _():
            remote(
                q_send.at[0], q_all.at[slot], q_send_sem.at[0], q_sem.at[slot], source
            ).wait_recv()

        for head in range(2):
            query_buf[head, slot - near_first] = unpack(q_all[slot, head])

    def take_far_query(slot, carry):
        source = block_of(slot, my_split)
        remote(
            q_send.at[0, 0], q_all.at[slot, 0], far_send_sem.at[0], q_sem.at[slot], source
        ).wait_recv()
        query_buf[2, slot - near] = unpack(q_all[slot, 0])
        return carry

    chunk = 64
    row_id = lax.broadcasted_iota(jnp.int32, (chunk, LANES), 0)
    col_id = lax.broadcasted_iota(jnp.int32, (chunk, LANES), 1)
    spread = col_id - row_id

    def visit_tiles(sections, jobs, tables):
        for slot, count, tile, span, masked in sections:
            unit = slot - jnp.where(slot >= near, near, 0)
            keys = span * key_tile
            key_values, scores = [], []
            for query_head, key_head in jobs:
                key_value = kv_all[pl.ds(tile * blocks_per_tile, span * blocks_per_tile), key_head]
                key_values.append(key_value.reshape(keys, LANES))
                queries = query_buf[query_head, pl.ds(unit, count)].reshape(count * rows, LANES)
                scores.append(
                    lax.dot_general(
                        queries,
                        key_values[-1],
                        (((1,), (1,)), ((), ())),
                        preferred_element_type=jnp.float32,
                    )
                )
            weights = [[] for _ in jobs]
            for first in range(0, keys, LANES):
                columns = [[] for _ in jobs]
                key_stamp = stamp_keys[
                    tile + first // key_tile, :, first % key_tile : first % key_tile + LANES
                ]
                for top in range(0, count * rows, chunk):
                    place, start = top // rows, top % rows
                    query_stamp = stamp_rows[slot + place, start : start + chunk]
                    elapsed = query_stamp - key_stamp
                    biases = biases_of(elapsed, tables, (top // chunk + first // LANES) % 3 != 0)
                    for score, bias, column in zip(scores, biases, columns):
                        halved = score[top : top + chunk, first : first + LANES] + bias
                        halved = halved.astype(jnp.bfloat16)
                        weight = halved + halved * jnp.tanh(halved)
                        if masked:
                            ahead = tile * key_tile + first - block_of(slot, my_split) * rows - start
                            weight = jnp.where(spread <= -ahead, weight.astype(jnp.float32), 0.0)
                            weight = weight.astype(jnp.bfloat16)
                        column.append(weight)
                for weight, column in zip(weights, columns):
                    weight.append(jnp.concatenate(column, axis=0))
            for (query_head, _), weight, key_value in zip(jobs, weights, key_values):
                sums = jnp.dot(
                    jnp.concatenate(weight, axis=1), key_value, preferred_element_type=jnp.float32
                )
                total_buf[query_head, pl.ds(unit, count)] += sums.reshape(count, rows, LANES)

    def visit(sections, jobs, tables):
        def one(step, carry):
            visit_tiles(
                [
                    (slot, count, group * group_tiles + span * step, span, masked)
                    for slot, count, group, span, masked in sections
                ],
                jobs,
                tables,
            )
            return carry

        if group_tiles == 1:
            one(0, 0)
        else:
            lax.fori_loop(0, group_tiles, one, 0)

    def visit_near(*pairs):
        visit(
            [
                (jnp.maximum(one, other), 1, jnp.minimum(one, other), 1, masked)
                for one, other, masked in pairs
            ],
            [(0, 0), (1, 1)],
            near_tables,
        )

    def back_copy(kind, unit):
        slot = unit + (near if kind == 2 else near_first)
        target, semaphore = (
            (part_out.at[my_place], part_sem.at[my_place])
            if kind == 2
            else (att_out.at[2 * my_place + kind], att_sem.at[2 * my_place + kind])
        )
        block = block_of(slot, my_split)
        return block, remote(
            back_buf.at[kind, unit], target, back_sem.at[kind, unit], semaphore, block
        )

    def own_copy(kind, unit):
        return pltpu.make_async_copy(
            back_buf.at[kind, unit], att_out.at[2 * my_place + kind], own_sem.at[kind]
        )

    def finish(kind, first, count):
        def one(unit, carry):
            block, copy = back_copy(kind, unit)
            total = total_buf[kind, unit]
            result = jnp.where(low, pltpu.roll(total[:half], head_size, 1), total[half:])
            result = result.astype(jnp.bfloat16)
            back_buf[kind, unit] = result
            if kind == 2:
                copy.start()
                return carry

            @pl.when(block == me)
            def _():
                own_copy(kind, unit).start()

            @pl.when(block != me)
            def _():
                copy.start()

            return carry

        lax.fori_loop(first, first + count, one, 0)

    def near_at(step):
        return near_first + (my_place ^ jnp.where(step == 0, 0, near - step))

    take_direct(near_at(0))

    def near_step(step, carry):
        group = near_at(step)

        @pl.when(step == 1)
        def _():
            each_far(near // 2, near // 2, lambda copy: copy.start())

        @pl.when(step + 1 < near)
        def _():
            take_direct(near_at(step + 1))

        take_forwarded(group)
        take_query(group)

        @pl.when(step == 0)
        def _():
            visit_near((group, group, True))

        @pl.when(step > 0)
        def _():
            visit_near((group, group, True), (group, near_at(step - 1), False))

        def two(pair, inner):
            visit_near((group, near_at(2 * pair), False), (group, near_at(2 * pair + 1), False))
            return inner

        lax.fori_loop(0, jnp.maximum(step - 1, 0) // 2, two, 0)

        @pl.when((step > 1) & (step % 2 == 0))
        def _():
            visit_near((group, near_at(step - 2), False))

        return carry

    lax.fori_loop(0, near, near_step, 0)

    @pl.when(upper == 1)
    def _():
        for late in range(near):
            take_late_direct(near - 1 - late)

    finish(0, 0, near)

    @pl.when(upper == 0)
    def _():
        finish(1, 0, near)

    lax.fori_loop(0, side, wait_far_stamps, 0)

    @pl.when(upper == 0)
    def _():
        lax.fori_loop(near, 2 * near, turn_stamps, 0)
        lax.fori_loop(near, 2 * near, take_far_query, 0)

    @pl.when(upper == 1)
    def _():
        lax.fori_loop(0, near * group_tiles, join_stamps, 0)

    halves = near // 2

    def square(step, carry):
        major, minor = step // halves, step % halves
        slots = 2 * jnp.where(upper == 0, major, minor)
        groups = 2 * (halves - 1 - jnp.where(upper == 0, minor, major))

        @pl.when((upper == 1) & (minor == 0))
        def _():
            take_late_forwarded(groups)
            take_late_forwarded(groups + 1)

        visit([(near + slots, 2, groups, 2, False)], [(2 - upper, upper)], square_tables)

        @pl.when((upper == 0) & (minor == halves - 1))
        def _():
            finish(2, slots, 2)

        @pl.when((upper == 1) & (major == halves - 1))
        def _():
            finish(1, slots, 2)

        return carry

    lax.fori_loop(0, halves * halves, square, 0)

    def drain_both(place, target):
        q_copy(place, target).wait_send()
        kv_copy(place, target).wait_send()

    each_near(drain_both)
    each_far(0, near, lambda copy: copy.wait_send())

    def drain(step, carry):
        stamp_copy(lax.rem(me + step, parts)).wait_send()
        return carry

    lax.fori_loop(1, parts, drain, 0)

    def drain_near(slot, carry):
        for step in range(1, splits):
            forward(slot, block_of(slot, my_split), step).wait_send()
        return carry

    def drain_late(slot, carry):
        for step in range(1, splits):
            late_forward(slot, block_of(slot, my_split), step).wait_send()
        return carry

    lax.fori_loop(near_first, near_first + near, drain_near, 0)

    @pl.when(upper == 1)
    def _():
        lax.fori_loop(0, near, drain_late, 0)

    def take_back(step, carry):
        place = lax.rem(my_place + step, near)
        source = (near_first + place) * splits + my_home

        @pl.when(source == me)
        def _():
            for head in range(2):
                own_copy(head, 0).wait()

        @pl.when(source != me)
        def _():
            for head in range(2):
                remote(
                    back_buf.at[0, 0],
                    att_out.at[2 * place + head],
                    back_sem.at[0, 0],
                    att_sem.at[2 * place + head],
                    source,
                ).wait_recv()

        @pl.when(upper == 1)
        def _():
            remote(
                back_buf.at[0, 0],
                part_out.at[place],
                back_sem.at[0, 0],
                part_sem.at[place],
                place * splits + my_home,
            ).wait_recv()

        return carry

    lax.fori_loop(0, near, take_back, 0)

    def drain_back(kind):
        def one(unit, carry):
            block, copy = back_copy(kind, unit)

            @pl.when(block != me)
            def _():
                copy.wait_send()

            return carry

        lax.fori_loop(0, near, one, 0)

    drain_back(0)
    drain_back(1)

    @pl.when(upper == 0)
    def _():
        drain_back(2)

    gate_store.wait()

    @pl.when(upper == 0)
    def _():
        no_part.wait()


def final_kernel(
    att_hbm,
    part_hbm,
    gate_hbm,
    tokens_hbm,
    attn_gain_hbm,
    w_out_hbm,
    out_hbm,
    att_buf,
    part_buf,
    gate_buf,
    tokens_ref,
    attn_gain_ref,
    w_out_ref,
    out_buf,
    load_sem,
    store_sem,
):
    loads = [
        pltpu.make_async_copy(source, target, load_sem.at[index])
        for index, (source, target) in enumerate(
            [
                (att_hbm, att_buf),
                (part_hbm, part_buf),
                (gate_hbm, gate_buf),
                (attn_gain_hbm, attn_gain_ref),
                (w_out_hbm, w_out_ref),
                (tokens_hbm, tokens_ref),
            ]
        )
    ]
    for load in loads:
        load.start()
    heads, half, _ = att_buf.shape
    head_size = tokens_ref.shape[1] // heads
    low = lax.broadcasted_iota(jnp.int32, (1, LANES), 1) < head_size
    for load in loads[:4]:
        load.wait()
    sides = []
    for side in range(2):
        pieces = []
        for pair in range(heads // 2):
            even = att_buf[2 * pair].astype(jnp.float32) + part_buf[pair].astype(jnp.float32)
            odd = att_buf[2 * pair + 1].astype(jnp.float32)
            if side == 0:
                pieces.append(jnp.where(low, even, pltpu.roll(odd, head_size, 1)))
            else:
                pieces.append(jnp.where(low, pltpu.roll(even, head_size, 1), odd))
        attended = jnp.concatenate(pieces, axis=1)
        part = slice(side * half, (side + 1) * half)
        gated = layer_norm(attended, attn_gain_ref[...]) * gate_buf[part].astype(jnp.float32)
        sides.append(gated.astype(jnp.bfloat16))
    loads[4].wait()
    loads[5].wait()
    stores = []
    for side in range(2):
        part = pl.ds(side * half, half)
        mixed = tokens_ref[part].astype(jnp.float32) + jnp.dot(
            sides[side], w_out_ref[...], preferred_element_type=jnp.float32
        )
        out_buf[part] = mixed.astype(jnp.bfloat16)
        stores.append(
            pltpu.make_async_copy(out_buf.at[part], out_hbm.at[part], store_sem.at[side])
        )
        stores[-1].start()
    for store in stores:
        store.wait()


def solution(mesh):
    parts = mesh.shape["pb"]

    def body(tokens, stamps, norm_gain, w_proj, rel_bias, attn_gain, w_out):
        rows, width = tokens.shape
        heads = rel_bias.shape[0]
        splits = parts // heads
        near = heads // 2
        blocks_per_tile = max(1, 384 // rows)
        att, part, gate = pl.pallas_call(
            functools.partial(kernel, parts, heads),
            out_shape=[
                jax.ShapeDtypeStruct((heads, rows // 2, LANES), jnp.bfloat16),
                jax.ShapeDtypeStruct((near, rows // 2, LANES), jnp.bfloat16),
                jax.ShapeDtypeStruct((rows, width), jnp.bfloat16),
            ],
            in_specs=[pl.BlockSpec(memory_space=pltpu.HBM)] * 5,
            out_specs=[pl.BlockSpec(memory_space=pltpu.HBM)] * 3,
            scratch_shapes=[
                pltpu.VMEM((rows, width), jnp.bfloat16),
                pltpu.VMEM((1, rows), jnp.int32),
                pltpu.VMEM((1, width), jnp.float32),
                pltpu.VMEM(w_proj.shape, jnp.bfloat16),
                pltpu.SMEM(rel_bias.shape, jnp.float32),
                pltpu.VMEM((near, 2, rows, LANES), jnp.bfloat16),
                pltpu.VMEM((near, 2, rows // 2, LANES), jnp.bfloat16),
                pltpu.VMEM((parts, 2, rows, LANES), jnp.bfloat16),
                pltpu.VMEM((heads, 2, rows // 2, LANES), jnp.bfloat16),
                pltpu.VMEM((3, near, rows, LANES), jnp.bfloat16),
                pltpu.VMEM((parts, 1, rows), jnp.int32),
                pltpu.VMEM((parts // blocks_per_tile, 1, blocks_per_tile * rows), jnp.int32),
                pltpu.VMEM((heads, rows, LANES), jnp.int32),
                pltpu.VMEM((3, near, rows, LANES), jnp.float32),
                pltpu.VMEM((rows, width), jnp.bfloat16),
                pltpu.VMEM((3, near, rows // 2, LANES), jnp.bfloat16),
                pltpu.VMEM((near, rows // 2, LANES), jnp.bfloat16),
                pltpu.SemaphoreType.DMA((6,)),
                pltpu.SemaphoreType.DMA((near,)),
                pltpu.SemaphoreType.DMA((near,)),
                pltpu.SemaphoreType.DMA((near,)),
                pltpu.SemaphoreType.DMA((heads, splits)),
                pltpu.SemaphoreType.DMA((parts,)),
                pltpu.SemaphoreType.DMA((heads,)),
                pltpu.SemaphoreType.DMA((parts,)),
                pltpu.SemaphoreType.DMA((parts,)),
                pltpu.SemaphoreType.DMA((3, near)),
                pltpu.SemaphoreType.DMA((heads,)),
                pltpu.SemaphoreType.DMA((near,)),
                pltpu.SemaphoreType.REGULAR,
                pltpu.SemaphoreType.DMA((4,)),
            ],
            compiler_params=pltpu.CompilerParams(
                collective_id=0, has_side_effects=True
            ),
        )(
            tokens,
            stamps.reshape(1, rows),
            norm_gain.reshape(1, width),
            w_proj,
            rel_bias,
        )
        hbm = pl.BlockSpec(memory_space=pltpu.HBM)
        return pl.pallas_call(
            final_kernel,
            out_shape=jax.ShapeDtypeStruct((rows, width), jnp.bfloat16),
            in_specs=[hbm] * 6,
            out_specs=hbm,
            scratch_shapes=[
                pltpu.VMEM((heads, rows // 2, LANES), jnp.bfloat16),
                pltpu.VMEM((near, rows // 2, LANES), jnp.bfloat16),
                pltpu.VMEM((rows, width), jnp.bfloat16),
                pltpu.VMEM((rows, width), jnp.bfloat16),
                pltpu.VMEM((1, width), jnp.float32),
                pltpu.VMEM(w_out.shape, jnp.bfloat16),
                pltpu.VMEM((rows, width), jnp.bfloat16),
                pltpu.SemaphoreType.DMA((6,)),
                pltpu.SemaphoreType.DMA((2,)),
            ],
        )(att, part, gate, tokens, attn_gain.reshape(1, width), w_out)

    return jax.shard_map(
        body,
        mesh=mesh,
        in_specs=(P(("groups", "pb"), None), P(("groups", "pb")), P(), P(), P(), P(), P()),
        out_specs=P(("groups", "pb"), None),
        check_vma=False,
    )
```

```python
import functools

import jax
import jax.numpy as jnp
from jax import lax
from jax.experimental import pallas as pl
from jax.experimental.pallas import tpu as pltpu
from jax.sharding import PartitionSpec as P

EPSILON = 1e-05
LANES = 128


def layer_norm(values, gain):
    centered = values - jnp.mean(values, axis=-1, keepdims=True)
    spread = jnp.mean(centered * centered, axis=-1, keepdims=True)
    return centered * lax.rsqrt(spread + EPSILON) * gain


LANE_LOOKUP = lax.GatherDimensionNumbers(
    offset_dims=(),
    collapsed_slice_dims=(1,),
    start_index_map=(1,),
    operand_batching_dims=(0,),
    start_indices_batching_dims=(0,),
)
ROW_LOOKUP = lax.GatherDimensionNumbers(
    offset_dims=(),
    collapsed_slice_dims=(1,),
    start_index_map=(1,),
    operand_batching_dims=(0, 2),
    start_indices_batching_dims=(0, 2),
)


def look_up(table, index, dimensions):
    return lax.gather(
        table,
        index[..., None],
        dimensions,
        (1,) * table.ndim,
        mode=lax.GatherScatterMode.PROMISE_IN_BOUNDS,
    )


def kernel(
    parts,
    heads,
    tokens_hbm,
    stamps_hbm,
    norm_gain_hbm,
    w_proj_hbm,
    bias_hbm,
    att_out,
    part_out,
    gate_out,
    tokens_ref,
    stamps_ref,
    norm_gain_ref,
    w_proj_ref,
    bias_ref,
    kv_send,
    q_send,
    kv_all,
    q_all,
    query_buf,
    stamp_all,
    stamp_keys,
    stamp_rows,
    total_buf,
    gate_buf,
    back_buf,
    zero_buf,
    load_sem,
    kv_send_sem,
    q_send_sem,
    far_send_sem,
    fwd_sem,
    kv_sem,
    q_sem,
    far_q_sem,
    stamp_send_sem,
    stamp_sem,
    back_sem,
    att_sem,
    part_sem,
    far_ready,
    own_sem,
):
    rows, width = tokens_ref.shape
    half = rows // 2
    head_size = width // heads
    splits = parts // heads
    near = heads // 2
    side = parts // 2
    blocks_per_tile = max(1, 384 // rows)
    key_tile = blocks_per_tile * rows
    group_tiles = splits // blocks_per_tile
    buckets = bias_ref.shape[1]

    loads = [
        pltpu.make_async_copy(source, target, load_sem.at[index])
        for index, (source, target) in enumerate(
            [
                (tokens_hbm, tokens_ref),
                (norm_gain_hbm, norm_gain_ref),
                (w_proj_hbm.at[:, width:], w_proj_ref.at[:, width:]),
                (stamps_hbm, stamps_ref),
                (bias_hbm, bias_ref),
                (w_proj_hbm.at[:, :width], w_proj_ref.at[:, :width]),
            ]
        )
    ]
    for load in loads:
        load.start()

    me = lax.axis_index("pb")
    my_group = me // splits
    my_split = me % splits
    upper = my_group // near
    my_place = my_group % near
    near_first = upper * near
    far_first = near - near_first
    side_first = upper * side

    def split_of(block):
        place = block % splits
        odd = (block // splits) % 2
        return place + odd * (splits - 1 - 2 * place)

    def block_of(slot, split):
        odd = slot % 2
        return slot * splits + split + odd * (splits - 1 - 2 * split)

    def remote(source, target, send, receive, device):
        return pltpu.make_async_remote_copy(
            src_ref=source,
            dst_ref=target,
            send_sem=send,
            recv_sem=receive,
            device_id={"pb": device},
            device_id_type=pl.DeviceIdType.MESH,
        )

    barrier = pltpu.get_barrier_semaphore()

    def signal(semaphore, other):
        pl.semaphore_signal(
            semaphore, inc=1, device_id={"pb": other}, device_id_type=pl.DeviceIdType.MESH
        )

    def near_peer(step):
        return side_first + lax.rem(me - side_first + step, side)

    def far_peer(step):
        return side - side_first + lax.rem(me - side_first + step, side)

    def greet(step, carry):
        signal(barrier, near_peer(step))
        return carry

    lax.fori_loop(1, side, greet, 0)
    signal(barrier, far_peer(0))

    low = lax.broadcasted_iota(jnp.int32, (1, LANES), 1) < head_size

    for load in loads[:3]:
        load.wait()
    normed = layer_norm(tokens_ref[...].astype(jnp.float32), norm_gain_ref[...]).astype(jnp.bfloat16)
    front = jnp.dot(normed, w_proj_ref[:, width : 2 * width], preferred_element_type=jnp.float32)
    scaled = front.astype(jnp.bfloat16).astype(jnp.float32) * (0.5 * head_size ** (-0.5))
    back = jnp.dot(normed, w_proj_ref[:, 2 * width :], preferred_element_type=jnp.float32)
    for pair in range(near):
        cols = slice(pair * LANES, (pair + 1) * LANES)
        key_cols = back[:, :width][:, cols]
        value_cols = back[:, width:][:, cols]
        query_cols = scaled[:, cols]
        kv_send[pair, 0] = jnp.where(
            low, key_cols, pltpu.roll(value_cols, head_size, 1)
        ).astype(jnp.bfloat16)
        kv_send[pair, 1] = jnp.where(
            low, pltpu.roll(key_cols, head_size, 1), value_cols
        ).astype(jnp.bfloat16)
        top, bottom = query_cols[:half], query_cols[half:]
        q_send[pair, 0] = jnp.where(low, top, pltpu.roll(bottom, head_size, 1)).astype(jnp.bfloat16)
        q_send[pair, 1] = jnp.where(low, pltpu.roll(top, head_size, 1), bottom).astype(jnp.bfloat16)
    loads[3].wait()
    loads[4].wait()

    my_home = split_of(me)

    def stamp_copy(target, kind):
        return remote(
            stamps_ref, stamp_all.at[me], stamp_send_sem.at[kind], stamp_sem.at[kind], target
        )

    def all_stamps(kind):
        some = stamp_all.at[pl.ds(0, side - 1 + kind)]
        return remote(some, some, stamp_send_sem.at[kind], stamp_sem.at[kind], near_peer(1))

    def kv_copy(place, target):
        return remote(kv_send.at[place], kv_all.at[me], kv_send_sem, kv_sem.at[me], target)

    def q_copy(place, target):
        return remote(
            q_send.at[place], q_all.at[my_group], q_send_sem, q_sem.at[my_place], target
        )

    def late_kv_copy(place, target):
        return remote(
            kv_send.at[place, 1], kv_all.at[me, 1], far_send_sem, kv_sem.at[me], target
        )

    def early_q_copy(place, target):
        return remote(
            q_send.at[place, 0], q_all.at[my_group, 0], far_send_sem, far_q_sem, target
        )

    def each_near(act):
        def one(step, carry):
            place = my_place ^ jnp.where(step == 0, 0, near - step)
            target = (near_first + place) * splits + my_home

            @pl.when(target != me)
            def _():
                act(place, target)

            return carry

        lax.fori_loop(0, near, one, 0)

    def far_place(step):
        place = step + (my_place % 2) * (1 - 2 * (step % 2))
        return place + upper * (near - 1 - 2 * place)

    def each_far(first, count, act):
        def one(step, carry):
            place = far_place(step)
            target = (far_first + place) * splits + my_home

            @pl.when(upper == 0)
            def _():
                act(late_kv_copy(place, target))

            @pl.when(upper == 1)
            def _():
                act(early_q_copy(place, target))

            return carry

        lax.fori_loop(first, first + count, one, 0)

    def send_near_stamps(step, carry):
        stamp_copy(near_peer(step), 0).start()
        return carry

    def send_far_stamps(step, carry):
        stamp_copy(far_peer(step), 1).start()
        return carry

    def start_both(place, target):
        q_copy(place, target).start()
        kv_copy(place, target).start()

    pl.semaphore_wait(barrier, side)

    def pass_on(step, carry):
        signal(far_ready, near_peer(step))
        return carry

    lax.fori_loop(1, side, pass_on, 0)
    lax.fori_loop(1, side, send_near_stamps, 0)
    each_near(start_both)

    stamp_all[me] = stamps_ref[...]

    @pl.when(my_home == my_split)
    def _():
        kv_all[me] = kv_send[my_place]
        q_all[my_group] = q_send[my_place]

    gate_store = pltpu.make_async_copy(gate_buf, gate_out, own_sem.at[2])
    no_part = pltpu.make_async_copy(zero_buf, part_out, own_sem.at[3])

    @pl.when(upper == 0)
    def _():
        zero_buf[...] = jnp.zeros_like(zero_buf)
        no_part.start()

    loads[5].wait()
    gate_proj = jnp.dot(normed, w_proj_ref[:, :width], preferred_element_type=jnp.float32)
    gate_buf[...] = jax.nn.silu(gate_proj).astype(jnp.bfloat16)
    gate_store.start()
    total_buf[...] = jnp.zeros_like(total_buf)

    pl.semaphore_wait(far_ready, side - 1)
    lax.fori_loop(0, side, send_far_stamps, 0)
    each_far(0, near // 2, lambda copy: copy.start())

    lane_id = lax.broadcasted_iota(jnp.int32, (8, LANES), 1)
    place_id = lax.broadcasted_iota(jnp.int32, (8, LANES), 0)

    def tables_of(head):
        def half_bias(bucket):
            table = jnp.zeros((8, LANES), jnp.float32)
            for bucket_id in range(buckets):
                table = jnp.where(bucket == bucket_id, 0.5 * bias_ref[head, bucket_id], table)
            return table

        return (
            half_bias(jnp.clip((33 - lane_id) >> 1, 0, buckets - 1))[:1],
            half_bias(jnp.where(place_id == 0, 8, 16 - place_id)),
            half_bias(jnp.where(place_id == 0, 0, 8 - place_id)),
        )

    near_tables = [tables_of(2 * my_place), tables_of(2 * my_place + 1)]
    square_tables = [tables_of(2 * my_place + upper)]

    def biases_of(elapsed, tables, by_rows):
        if not by_rows:
            index = lax.clz(elapsed)
            return [look_up(jnp.broadcast_to(lane, elapsed.shape), index, LANE_LOOKUP) for lane, _, _ in tables]
        tiles = (elapsed.shape[0] // 8, 8, LANES)
        zeros_count = lax.clz(jnp.minimum(elapsed, 2**30 - 1))
        index = ((zeros_count >> 1) & 7).reshape(tiles)
        old = elapsed >= 4**7
        biases = []
        for _, far_table, close_table in tables:
            far_bias = look_up(jnp.broadcast_to(far_table[None], tiles), index, ROW_LOOKUP)
            close_bias = look_up(jnp.broadcast_to(close_table[None], tiles), index, ROW_LOOKUP)
            biases.append(
                jnp.where(old, far_bias.reshape(elapsed.shape), close_bias.reshape(elapsed.shape))
            )
        return biases

    def join_stamps(tile, carry):
        stamp_keys[tile] = jnp.concatenate(
            [stamp_all[tile * blocks_per_tile + place] for place in range(blocks_per_tile)], axis=1
        )
        return carry

    def turn_stamps(slot, carry):
        block = block_of(slot, my_split)
        stamp_rows[slot] = jnp.transpose(jnp.broadcast_to(stamp_all[block], (LANES, rows)))
        return carry

    all_stamps(0).wait_recv()
    lax.fori_loop(near_first * group_tiles, (near_first + near) * group_tiles, join_stamps, 0)
    lax.fori_loop(near_first, near_first + near, turn_stamps, 0)

    def forward(source, step):
        peer = my_group * splits + lax.rem(my_split + step, splits)
        return remote(
            kv_all.at[source], kv_all.at[source], fwd_sem.at[0], kv_sem.at[source], peer
        )

    def late_forward(source, step):
        peer = my_group * splits + lax.rem(my_split + step, splits)
        return remote(
            kv_all.at[source, 1], kv_all.at[source, 1], fwd_sem.at[1], kv_sem.at[source], peer
        )

    def take_direct(slot):
        source = block_of(slot, my_split)

        @pl.when(source != me)
        def _():
            remote(
                kv_send.at[0], kv_all.at[source], kv_send_sem, kv_sem.at[source], source
            ).wait_recv()

        for step in range(1, splits):
            forward(source, step).start()

    def take_forwarded(slot):
        for step in range(1, splits):
            source = block_of(slot, lax.rem(my_split + step, splits))
            forward(source, step).wait_recv()

    def take_late_direct(slot):
        source = block_of(slot, my_split)
        remote(
            kv_send.at[0, 1], kv_all.at[source, 1], far_send_sem, kv_sem.at[source], source
        ).wait_recv()
        for step in range(1, splits):
            late_forward(source, step).start()

    def take_late_forwarded(slot):
        for step in range(1, splits):
            source = block_of(slot, lax.rem(my_split + step, splits))
            late_forward(source, step).wait_recv()

    def unpack(packed):
        packed = packed.astype(jnp.float32)
        return jnp.concatenate(
            [jnp.where(low, packed, 0.0), jnp.where(low, pltpu.roll(packed, head_size, 1), 0.0)], axis=0
        ).astype(jnp.bfloat16)

    def take_query(slot):
        source = block_of(slot, my_split)

        @pl.when(source != me)
        def _():
            remote(
                q_send.at[0], q_all.at[slot], q_send_sem, q_sem.at[slot - near_first], source
            ).wait_recv()

        for head in range(2):
            query_buf[head, slot - near_first] = unpack(q_all[slot, head])

    def take_far_query(slot, carry):
        query_buf[2, slot - near] = unpack(q_all[slot, 0])
        return carry

    def all_far_queries():
        some = q_all.at[pl.ds(0, near), 0]
        return remote(some, some, far_send_sem, far_q_sem, near_peer(1))

    chunk = 64
    row_id = lax.broadcasted_iota(jnp.int32, (chunk, LANES), 0)
    col_id = lax.broadcasted_iota(jnp.int32, (chunk, LANES), 1)
    spread = col_id - row_id

    def visit_tiles(sections, jobs, tables):
        for slot, count, tile, span, masked in sections:
            unit = slot - jnp.where(slot >= near, near, 0)
            keys = span * key_tile
            key_values, scores = [], []
            for query_head, key_head in jobs:
                key_value = kv_all[pl.ds(tile * blocks_per_tile, span * blocks_per_tile), key_head]
                key_values.append(key_value.reshape(keys, LANES))
                queries = query_buf[query_head, pl.ds(unit, count)].reshape(count * rows, LANES)
                scores.append(
                    lax.dot_general(
                        queries,
                        key_values[-1],
                        (((1,), (1,)), ((), ())),
                        preferred_element_type=jnp.float32,
                    )
                )
            weights = [[] for _ in jobs]
            for first in range(0, keys, LANES):
                columns = [[] for _ in jobs]
                key_stamp = stamp_keys[
                    tile + first // key_tile, :, first % key_tile : first % key_tile + LANES
                ]
                for top in range(0, count * rows, chunk):
                    place, start = top // rows, top % rows
                    query_stamp = stamp_rows[slot + place, start : start + chunk]
                    elapsed = query_stamp - key_stamp
                    biases = biases_of(elapsed, tables, (top // chunk + first // LANES) % 3 != 0)
                    for score, bias, column in zip(scores, biases, columns):
                        halved = score[top : top + chunk, first : first + LANES] + bias
                        halved = halved.astype(jnp.bfloat16)
                        weight = halved + halved * jnp.tanh(halved)
                        if masked:
                            ahead = tile * key_tile + first - block_of(slot, my_split) * rows - start
                            weight = jnp.where(spread <= -ahead, weight.astype(jnp.float32), 0.0)
                            weight = weight.astype(jnp.bfloat16)
                        column.append(weight)
                for weight, column in zip(weights, columns):
                    weight.append(jnp.concatenate(column, axis=0))
            for (query_head, _), weight, key_value in zip(jobs, weights, key_values):
                sums = jnp.dot(
                    jnp.concatenate(weight, axis=1), key_value, preferred_element_type=jnp.float32
                )
                total_buf[query_head, pl.ds(unit, count)] += sums.reshape(count, rows, LANES)

    def visit(sections, jobs, tables):
        def one(step, carry):
            visit_tiles(
                [
                    (slot, count, group * group_tiles + span * step, span, masked)
                    for slot, count, group, span, masked in sections
                ],
                jobs,
                tables,
            )
            return carry

        if group_tiles == 1:
            one(0, 0)
        else:
            lax.fori_loop(0, group_tiles, one, 0)

    def visit_near(*pairs):
        visit(
            [
                (jnp.maximum(one, other), 1, jnp.minimum(one, other), 1, masked)
                for one, other, masked in pairs
            ],
            [(0, 0), (1, 1)],
            near_tables,
        )

    def back_copy(kind, unit):
        slot = unit + (near if kind == 2 else near_first)
        target, semaphore = (
            (part_out.at[my_place], part_sem)
            if kind == 2
            else (att_out.at[2 * my_place + kind], att_sem)
        )
        block = block_of(slot, my_split)
        return block, remote(
            back_buf.at[kind, unit], target, back_sem.at[kind], semaphore, block
        )

    def own_copy(kind, unit):
        return pltpu.make_async_copy(
            back_buf.at[kind, unit], att_out.at[2 * my_place + kind], own_sem.at[kind]
        )

    def finish(kind, first, count):
        def one(unit, carry):
            block, copy = back_copy(kind, unit)
            total = total_buf[kind, unit]
            result = jnp.where(low, pltpu.roll(total[:half], head_size, 1), total[half:])
            result = result.astype(jnp.bfloat16)
            back_buf[kind, unit] = result
            if kind == 2:
                copy.start()
                return carry

            @pl.when(block == me)
            def _():
                own_copy(kind, unit).start()

            @pl.when(block != me)
            def _():
                copy.start()

            return carry

        lax.fori_loop(first, first + count, one, 0)

    def near_at(step):
        return near_first + (my_place ^ jnp.where(step == 0, 0, near - step))

    take_direct(near_at(0))

    def near_step(step, carry):
        group = near_at(step)

        @pl.when(step == 1)
        def _():
            each_far(near // 2, near // 2, lambda copy: copy.start())

        @pl.when(step + 1 < near)
        def _():
            take_direct(near_at(step + 1))

        take_forwarded(group)
        take_query(group)

        @pl.when(step == 0)
        def _():
            visit_near((group, group, True))

        @pl.when(step > 0)
        def _():
            visit_near((group, group, True), (group, near_at(step - 1), False))

        def two(pair, inner):
            visit_near((group, near_at(2 * pair), False), (group, near_at(2 * pair + 1), False))
            return inner

        lax.fori_loop(0, jnp.maximum(step - 1, 0) // 2, two, 0)

        @pl.when((step > 1) & (step % 2 == 0))
        def _():
            visit_near((group, near_at(step - 2), False))

        return carry

    lax.fori_loop(0, near, near_step, 0)

    @pl.when(upper == 1)
    def _():
        for late in range(near):
            take_late_direct(near - 1 - late)

    finish(0, 0, near)

    @pl.when(upper == 0)
    def _():
        finish(1, 0, near)

    all_stamps(1).wait_recv()

    @pl.when(upper == 0)
    def _():
        lax.fori_loop(near, 2 * near, turn_stamps, 0)
        all_far_queries().wait_recv()
        lax.fori_loop(near, 2 * near, take_far_query, 0)

    @pl.when(upper == 1)
    def _():
        lax.fori_loop(0, near * group_tiles, join_stamps, 0)

    halves = near // 2

    def square(step, carry):
        major, minor = step // halves, step % halves
        slots = 2 * jnp.where(upper == 0, major, minor)
        groups = 2 * (halves - 1 - jnp.where(upper == 0, minor, major))

        @pl.when((upper == 1) & (minor == 0))
        def _():
            take_late_forwarded(groups)
            take_late_forwarded(groups + 1)

        visit([(near + slots, 2, groups, 2, False)], [(2 - upper, upper)], square_tables)

        @pl.when((upper == 0) & (minor == halves - 1))
        def _():
            finish(2, slots, 2)

        @pl.when((upper == 1) & (major == halves - 1))
        def _():
            finish(1, slots, 2)

        return carry

    lax.fori_loop(0, halves * halves, square, 0)

    all_stamps(0).wait_send()
    all_stamps(1).wait_send()

    def forwards():
        some = kv_all.at[pl.ds(0, near * (splits - 1))]
        return remote(some, some, fwd_sem.at[0], fwd_sem.at[0], near_peer(1))

    def late_forwards():
        some = kv_all.at[pl.ds(0, near * (splits - 1)), 1]
        return remote(some, some, fwd_sem.at[1], fwd_sem.at[1], near_peer(1))

    def wait_near(count):
        some = kv_all.at[pl.ds(0, count)]
        remote(some, some, kv_send_sem, kv_send_sem, near_peer(1)).wait_send()
        some = q_all.at[pl.ds(0, count)]
        remote(some, some, q_send_sem, q_send_sem, near_peer(1)).wait_send()

    def results(count, send, receive):
        some = att_out.at[pl.ds(0, count)]
        return remote(some, some, send, receive, near_peer(1))

    home = my_home == my_split
    forwards().wait_send()

    @pl.when(home)
    def _():
        wait_near(near - 1)
        results(2 * near - 2, att_sem, att_sem).wait_recv()
        for kind in range(2):
            own_copy(kind, 0).wait()
            results(near - 1, back_sem.at[kind], back_sem.at[kind]).wait_send()

    @pl.when(jnp.logical_not(home))
    def _():
        wait_near(near)
        results(2 * near, att_sem, att_sem).wait_recv()
        for kind in range(2):
            results(near, back_sem.at[kind], back_sem.at[kind]).wait_send()

    @pl.when(upper == 0)
    def _():
        some = kv_send.at[:, 1]
        remote(some, some, far_send_sem, far_send_sem, near_peer(1)).wait_send()
        results(near, back_sem.at[2], back_sem.at[2]).wait_send()
        no_part.wait()

    @pl.when(upper == 1)
    def _():
        all_far_queries().wait_send()
        late_forwards().wait_send()
        results(near, part_sem, part_sem).wait_recv()

    gate_store.wait()


def final_kernel(
    att_hbm,
    part_hbm,
    gate_hbm,
    tokens_hbm,
    attn_gain_hbm,
    w_out_hbm,
    out_hbm,
    att_buf,
    part_buf,
    gate_buf,
    tokens_ref,
    attn_gain_ref,
    w_out_ref,
    out_buf,
    load_sem,
    store_sem,
):
    loads = [
        pltpu.make_async_copy(source, target, load_sem.at[index])
        for index, (source, target) in enumerate(
            [
                (att_hbm, att_buf),
                (part_hbm, part_buf),
                (gate_hbm, gate_buf),
                (attn_gain_hbm, attn_gain_ref),
                (w_out_hbm, w_out_ref),
                (tokens_hbm, tokens_ref),
            ]
        )
    ]
    for load in loads:
        load.start()
    heads, half, _ = att_buf.shape
    head_size = tokens_ref.shape[1] // heads
    low = lax.broadcasted_iota(jnp.int32, (1, LANES), 1) < head_size
    for load in loads[:4]:
        load.wait()
    sides = []
    for side in range(2):
        pieces = []
        for pair in range(heads // 2):
            even = att_buf[2 * pair].astype(jnp.float32) + part_buf[pair].astype(jnp.float32)
            odd = att_buf[2 * pair + 1].astype(jnp.float32)
            if side == 0:
                pieces.append(jnp.where(low, even, pltpu.roll(odd, head_size, 1)))
            else:
                pieces.append(jnp.where(low, pltpu.roll(even, head_size, 1), odd))
        attended = jnp.concatenate(pieces, axis=1)
        part = slice(side * half, (side + 1) * half)
        gated = layer_norm(attended, attn_gain_ref[...]) * gate_buf[part].astype(jnp.float32)
        sides.append(gated.astype(jnp.bfloat16))
    loads[4].wait()
    loads[5].wait()
    stores = []
    for side in range(2):
        part = pl.ds(side * half, half)
        mixed = tokens_ref[part].astype(jnp.float32) + jnp.dot(
            sides[side], w_out_ref[...], preferred_element_type=jnp.float32
        )
        out_buf[part] = mixed.astype(jnp.bfloat16)
        stores.append(
            pltpu.make_async_copy(out_buf.at[part], out_hbm.at[part], store_sem.at[side])
        )
        stores[-1].start()
    for store in stores:
        store.wait()


def solution(mesh):
    parts = mesh.shape["pb"]

    def body(tokens, stamps, norm_gain, w_proj, rel_bias, attn_gain, w_out):
        rows, width = tokens.shape
        heads = rel_bias.shape[0]
        splits = parts // heads
        near = heads // 2
        blocks_per_tile = max(1, 384 // rows)
        att, part, gate = pl.pallas_call(
            functools.partial(kernel, parts, heads),
            out_shape=[
                jax.ShapeDtypeStruct((heads, rows // 2, LANES), jnp.bfloat16),
                jax.ShapeDtypeStruct((near, rows // 2, LANES), jnp.bfloat16),
                jax.ShapeDtypeStruct((rows, width), jnp.bfloat16),
            ],
            in_specs=[pl.BlockSpec(memory_space=pltpu.HBM)] * 5,
            out_specs=[pl.BlockSpec(memory_space=pltpu.HBM)] * 3,
            scratch_shapes=[
                pltpu.VMEM((rows, width), jnp.bfloat16),
                pltpu.VMEM((1, rows), jnp.int32),
                pltpu.VMEM((1, width), jnp.float32),
                pltpu.VMEM(w_proj.shape, jnp.bfloat16),
                pltpu.SMEM(rel_bias.shape, jnp.float32),
                pltpu.VMEM((near, 2, rows, LANES), jnp.bfloat16),
                pltpu.VMEM((near, 2, rows // 2, LANES), jnp.bfloat16),
                pltpu.VMEM((parts, 2, rows, LANES), jnp.bfloat16),
                pltpu.VMEM((heads, 2, rows // 2, LANES), jnp.bfloat16),
                pltpu.VMEM((3, near, rows, LANES), jnp.bfloat16),
                pltpu.VMEM((parts, 1, rows), jnp.int32),
                pltpu.VMEM((parts // blocks_per_tile, 1, blocks_per_tile * rows), jnp.int32),
                pltpu.VMEM((heads, rows, LANES), jnp.int32),
                pltpu.VMEM((3, near, rows, LANES), jnp.float32),
                pltpu.VMEM((rows, width), jnp.bfloat16),
                pltpu.VMEM((3, near, rows // 2, LANES), jnp.bfloat16),
                pltpu.VMEM((near, rows // 2, LANES), jnp.bfloat16),
                pltpu.SemaphoreType.DMA((6,)),
                pltpu.SemaphoreType.DMA,
                pltpu.SemaphoreType.DMA,
                pltpu.SemaphoreType.DMA,
                pltpu.SemaphoreType.DMA((2,)),
                pltpu.SemaphoreType.DMA((parts,)),
                pltpu.SemaphoreType.DMA((near,)),
                pltpu.SemaphoreType.DMA,
                pltpu.SemaphoreType.DMA((2,)),
                pltpu.SemaphoreType.DMA((2,)),
                pltpu.SemaphoreType.DMA((3,)),
                pltpu.SemaphoreType.DMA,
                pltpu.SemaphoreType.DMA,
                pltpu.SemaphoreType.REGULAR,
                pltpu.SemaphoreType.DMA((4,)),
            ],
            compiler_params=pltpu.CompilerParams(
                collective_id=0, has_side_effects=True
            ),
        )(
            tokens,
            stamps.reshape(1, rows),
            norm_gain.reshape(1, width),
            w_proj,
            rel_bias,
        )
        hbm = pl.BlockSpec(memory_space=pltpu.HBM)
        return pl.pallas_call(
            final_kernel,
            out_shape=jax.ShapeDtypeStruct((rows, width), jnp.bfloat16),
            in_specs=[hbm] * 6,
            out_specs=hbm,
            scratch_shapes=[
                pltpu.VMEM((heads, rows // 2, LANES), jnp.bfloat16),
                pltpu.VMEM((near, rows // 2, LANES), jnp.bfloat16),
                pltpu.VMEM((rows, width), jnp.bfloat16),
                pltpu.VMEM((rows, width), jnp.bfloat16),
                pltpu.VMEM((1, width), jnp.float32),
                pltpu.VMEM(w_out.shape, jnp.bfloat16),
                pltpu.VMEM((rows, width), jnp.bfloat16),
                pltpu.SemaphoreType.DMA((6,)),
                pltpu.SemaphoreType.DMA((2,)),
            ],
        )(att, part, gate, tokens, attn_gain.reshape(1, width), w_out)

    return jax.shard_map(
        body,
        mesh=mesh,
        in_specs=(P(("groups", "pb"), None), P(("groups", "pb")), P(), P(), P(), P(), P()),
        out_specs=P(("groups", "pb"), None),
        check_vma=False,
    )
```

```python
import functools

import jax
import jax.numpy as jnp
from jax import lax
from jax.experimental import pallas as pl
from jax.experimental.pallas import tpu as pltpu
from jax.sharding import PartitionSpec as P

EPSILON = 1e-05
LANES = 128


def layer_norm(values, gain):
    centered = values - jnp.mean(values, axis=-1, keepdims=True)
    spread = jnp.mean(centered * centered, axis=-1, keepdims=True)
    return centered * lax.rsqrt(spread + EPSILON) * gain


LANE_LOOKUP = lax.GatherDimensionNumbers(
    offset_dims=(),
    collapsed_slice_dims=(1,),
    start_index_map=(1,),
    operand_batching_dims=(0,),
    start_indices_batching_dims=(0,),
)
ROW_LOOKUP = lax.GatherDimensionNumbers(
    offset_dims=(),
    collapsed_slice_dims=(1,),
    start_index_map=(1,),
    operand_batching_dims=(0, 2),
    start_indices_batching_dims=(0, 2),
)


def look_up(table, index, dimensions):
    return lax.gather(
        table,
        index[..., None],
        dimensions,
        (1,) * table.ndim,
        mode=lax.GatherScatterMode.PROMISE_IN_BOUNDS,
    )


def kernel(
    parts,
    heads,
    tokens_hbm,
    stamps_hbm,
    norm_gain_hbm,
    w_proj_hbm,
    bias_hbm,
    att_out,
    part_out,
    gate_out,
    tokens_ref,
    stamps_ref,
    norm_gain_ref,
    w_proj_ref,
    bias_ref,
    kv_send,
    q_send,
    kv_all,
    q_all,
    query_buf,
    stamp_all,
    stamp_keys,
    stamp_rows,
    total_buf,
    gate_buf,
    back_buf,
    zero_buf,
    load_sem,
    kv_send_sem,
    q_send_sem,
    far_send_sem,
    fwd_sem,
    kv_sem,
    q_sem,
    far_q_sem,
    stamp_send_sem,
    stamp_sem,
    back_sem,
    att_sem,
    part_sem,
    far_ready,
    own_sem,
):
    rows, width = tokens_ref.shape
    half = rows // 2
    head_size = width // heads
    splits = parts // heads
    near = heads // 2
    side = parts // 2
    blocks_per_tile = max(1, 384 // rows)
    key_tile = blocks_per_tile * rows
    group_tiles = splits // blocks_per_tile
    buckets = bias_ref.shape[1]

    loads = [
        pltpu.make_async_copy(source, target, load_sem.at[index])
        for index, (source, target) in enumerate(
            [
                (tokens_hbm, tokens_ref),
                (norm_gain_hbm, norm_gain_ref),
                (w_proj_hbm.at[:, width:], w_proj_ref.at[:, width:]),
                (stamps_hbm, stamps_ref),
                (bias_hbm, bias_ref),
                (w_proj_hbm.at[:, :width], w_proj_ref.at[:, :width]),
            ]
        )
    ]
    for load in loads:
        load.start()

    me = lax.axis_index("pb")
    my_group = me // splits
    my_split = me % splits
    upper = my_group // near
    my_place = my_group % near
    near_first = upper * near
    far_first = near - near_first
    side_first = upper * side

    def split_of(block):
        place = block % splits
        odd = (block // splits) % 2
        return place + odd * (splits - 1 - 2 * place)

    def block_of(slot, split):
        odd = slot % 2
        return slot * splits + split + odd * (splits - 1 - 2 * split)

    def remote(source, target, send, receive, device):
        return pltpu.make_async_remote_copy(
            src_ref=source,
            dst_ref=target,
            send_sem=send,
            recv_sem=receive,
            device_id={"pb": device},
            device_id_type=pl.DeviceIdType.MESH,
        )

    barrier = pltpu.get_barrier_semaphore()

    def signal(semaphore, other):
        pl.semaphore_signal(
            semaphore, inc=1, device_id={"pb": other}, device_id_type=pl.DeviceIdType.MESH
        )

    def near_peer(step):
        return side_first + lax.rem(me - side_first + step, side)

    def far_peer(step):
        return side - side_first + lax.rem(me - side_first + step, side)

    def greet(step, carry):
        signal(barrier, near_peer(step))
        return carry

    lax.fori_loop(1, side, greet, 0)
    signal(barrier, far_peer(0))

    low = lax.broadcasted_iota(jnp.int32, (1, LANES), 1) < head_size

    for load in loads[:3]:
        load.wait()
    normed = layer_norm(tokens_ref[...].astype(jnp.float32), norm_gain_ref[...]).astype(jnp.bfloat16)
    front = jnp.dot(normed, w_proj_ref[:, width : 2 * width], preferred_element_type=jnp.float32)
    scaled = front.astype(jnp.bfloat16).astype(jnp.float32) * (0.5 * head_size ** (-0.5))
    back = jnp.dot(normed, w_proj_ref[:, 2 * width :], preferred_element_type=jnp.float32)
    for pair in range(near):
        cols = slice(pair * LANES, (pair + 1) * LANES)
        key_cols = back[:, :width][:, cols]
        value_cols = back[:, width:][:, cols]
        query_cols = scaled[:, cols]
        kv_send[pair, 0] = jnp.where(
            low, key_cols, pltpu.roll(value_cols, head_size, 1)
        ).astype(jnp.bfloat16)
        kv_send[pair, 1] = jnp.where(
            low, pltpu.roll(key_cols, head_size, 1), value_cols
        ).astype(jnp.bfloat16)
        top, bottom = query_cols[:half], query_cols[half:]
        q_send[pair, 0] = jnp.where(low, top, pltpu.roll(bottom, head_size, 1)).astype(jnp.bfloat16)
        q_send[pair, 1] = jnp.where(low, pltpu.roll(top, head_size, 1), bottom).astype(jnp.bfloat16)
    loads[3].wait()
    loads[4].wait()

    my_home = split_of(me)

    def stamp_copy(target, kind):
        return remote(
            stamps_ref, stamp_all.at[me], stamp_send_sem.at[kind], stamp_sem.at[kind], target
        )

    def all_stamps(kind):
        some = stamp_all.at[pl.ds(0, side - 1 + kind)]
        return remote(some, some, stamp_send_sem.at[kind], stamp_sem.at[kind], near_peer(1))

    def kv_copy(place, target):
        return remote(kv_send.at[place], kv_all.at[me], kv_send_sem, kv_sem.at[me], target)

    def q_copy(place, target):
        return remote(
            q_send.at[place], q_all.at[my_group], q_send_sem, q_sem.at[my_place], target
        )

    def late_kv_copy(place, target):
        return remote(
            kv_send.at[place, 1], kv_all.at[me, 1], far_send_sem, kv_sem.at[me], target
        )

    def early_q_copy(place, target):
        return remote(
            q_send.at[place, 0], q_all.at[my_group, 0], far_send_sem, far_q_sem, target
        )

    def each_near(act):
        def one(step, carry):
            place = my_place ^ jnp.where(step == 0, 0, near - step)
            target = (near_first + place) * splits + my_home

            @pl.when(target != me)
            def _():
                act(place, target)

            return carry

        lax.fori_loop(0, near, one, 0)

    relays = (1 - upper) * (my_place // (near // 2)) * (near // 2)
    farther = jnp.maximum(relays, upper * (near // 2))

    def far_place(step):
        place = step + (my_place % 2) * (1 - 2 * (step % 2))
        return place + upper * (near - 1 - 2 * place)

    def each_far(first, count, act):
        def one(step, carry):
            place = far_place(step)
            target = (far_first + place) * splits + my_home

            @pl.when(upper == 0)
            def _():
                act(late_kv_copy(place, target))

            @pl.when(upper == 1)
            def _():
                act(early_q_copy(place, target))

            return carry

        lax.fori_loop(first, first + count, one, 0)

    def send_near_stamps(step, carry):
        stamp_copy(near_peer(step), 0).start()
        return carry

    def send_far_stamps(step, carry):
        stamp_copy(far_peer(step), 1).start()
        return carry

    def start_both(place, target):
        q_copy(place, target).start()
        kv_copy(place, target).start()

    pl.semaphore_wait(barrier, side)

    def pass_on(step, carry):
        signal(far_ready, near_peer(step))
        return carry

    lax.fori_loop(1, side, pass_on, 0)
    lax.fori_loop(1, side, send_near_stamps, 0)
    each_near(start_both)

    stamp_all[me] = stamps_ref[...]

    @pl.when(my_home == my_split)
    def _():
        kv_all[me] = kv_send[my_place]
        q_all[my_group] = q_send[my_place]

    gate_store = pltpu.make_async_copy(gate_buf, gate_out, own_sem.at[2])
    no_part = pltpu.make_async_copy(zero_buf, part_out, own_sem.at[3])

    @pl.when(upper == 0)
    def _():
        zero_buf[...] = jnp.zeros_like(zero_buf)
        no_part.start()

    loads[5].wait()
    gate_proj = jnp.dot(normed, w_proj_ref[:, :width], preferred_element_type=jnp.float32)
    gate_buf[...] = jax.nn.silu(gate_proj).astype(jnp.bfloat16)
    gate_store.start()
    total_buf[...] = jnp.zeros_like(total_buf)

    pl.semaphore_wait(far_ready, side - 1)
    lax.fori_loop(0, side, send_far_stamps, 0)
    each_far(0, near // 2, lambda copy: copy.start())

    lane_id = lax.broadcasted_iota(jnp.int32, (8, LANES), 1)
    place_id = lax.broadcasted_iota(jnp.int32, (8, LANES), 0)

    def tables_of(head):
        def half_bias(bucket):
            table = jnp.zeros((8, LANES), jnp.float32)
            for bucket_id in range(buckets):
                table = jnp.where(bucket == bucket_id, 0.5 * bias_ref[head, bucket_id], table)
            return table

        return (
            half_bias(jnp.clip((33 - lane_id) >> 1, 0, buckets - 1))[:1],
            half_bias(jnp.where(place_id == 0, 8, 16 - place_id)),
            half_bias(jnp.where(place_id == 0, 0, 8 - place_id)),
        )

    near_tables = [tables_of(2 * my_place), tables_of(2 * my_place + 1)]
    square_tables = [tables_of(2 * my_place + upper)]

    def biases_of(elapsed, tables, by_rows):
        if not by_rows:
            index = lax.clz(elapsed)
            return [look_up(jnp.broadcast_to(lane, elapsed.shape), index, LANE_LOOKUP) for lane, _, _ in tables]
        tiles = (elapsed.shape[0] // 8, 8, LANES)
        zeros_count = lax.clz(jnp.minimum(elapsed, 2**30 - 1))
        index = ((zeros_count >> 1) & 7).reshape(tiles)
        old = elapsed >= 4**7
        biases = []
        for _, far_table, close_table in tables:
            far_bias = look_up(jnp.broadcast_to(far_table[None], tiles), index, ROW_LOOKUP)
            close_bias = look_up(jnp.broadcast_to(close_table[None], tiles), index, ROW_LOOKUP)
            biases.append(
                jnp.where(old, far_bias.reshape(elapsed.shape), close_bias.reshape(elapsed.shape))
            )
        return biases

    def join_stamps(tile, carry):
        stamp_keys[tile] = jnp.concatenate(
            [stamp_all[tile * blocks_per_tile + place] for place in range(blocks_per_tile)], axis=1
        )
        return carry

    def turn_stamps(slot, carry):
        block = block_of(slot, my_split)
        stamp_rows[slot] = jnp.transpose(jnp.broadcast_to(stamp_all[block], (LANES, rows)))
        return carry

    all_stamps(0).wait_recv()
    lax.fori_loop(near_first * group_tiles, (near_first + near) * group_tiles, join_stamps, 0)
    lax.fori_loop(near_first, near_first + near, turn_stamps, 0)

    def forward(source, step):
        peer = my_group * splits + lax.rem(my_split + step, splits)
        return remote(
            kv_all.at[source], kv_all.at[source], fwd_sem.at[0], kv_sem.at[source], peer
        )

    def late_forward(source, step):
        peer = my_group * splits + lax.rem(my_split + step, splits)
        return remote(
            kv_all.at[source, 1], kv_all.at[source, 1], fwd_sem.at[1], kv_sem.at[source], peer
        )

    def relay(source):
        return remote(
            kv_all.at[source, 1],
            kv_all.at[source, 1],
            fwd_sem.at[1],
            kv_sem.at[source],
            (far_first + my_place) * splits + my_split,
        )

    def take_direct(slot):
        source = block_of(slot, my_split)

        @pl.when(source != me)
        def _():
            remote(
                kv_send.at[0], kv_all.at[source], kv_send_sem, kv_sem.at[source], source
            ).wait_recv()

        for step in range(1, splits):
            forward(source, step).start()

        @pl.when(slot < relays)
        def _():
            relay(source).start()

    def take_forwarded(slot):
        for step in range(1, splits):
            source = block_of(slot, lax.rem(my_split + step, splits))
            forward(source, step).wait_recv()

    def take_late_direct(slot):
        source = block_of(slot, my_split)
        remote(
            kv_send.at[0, 1], kv_all.at[source, 1], far_send_sem, kv_sem.at[source], source
        ).wait_recv()
        for step in range(1, splits):
            late_forward(source, step).start()

    def take_late_forwarded(slot):
        for step in range(1, splits):
            source = block_of(slot, lax.rem(my_split + step, splits))
            late_forward(source, step).wait_recv()

    def unpack(packed):
        packed = packed.astype(jnp.float32)
        return jnp.concatenate(
            [jnp.where(low, packed, 0.0), jnp.where(low, pltpu.roll(packed, head_size, 1), 0.0)], axis=0
        ).astype(jnp.bfloat16)

    def take_query(slot):
        source = block_of(slot, my_split)

        @pl.when(source != me)
        def _():
            remote(
                q_send.at[0], q_all.at[slot], q_send_sem, q_sem.at[slot - near_first], source
            ).wait_recv()

        for head in range(2):
            query_buf[head, slot - near_first] = unpack(q_all[slot, head])

    def take_far_query(slot, carry):
        query_buf[2, slot - near] = unpack(q_all[slot, 0])
        return carry

    def all_far_queries():
        some = q_all.at[pl.ds(0, near), 0]
        return remote(some, some, far_send_sem, far_q_sem, near_peer(1))

    chunk = 64
    row_id = lax.broadcasted_iota(jnp.int32, (chunk, LANES), 0)
    col_id = lax.broadcasted_iota(jnp.int32, (chunk, LANES), 1)
    spread = col_id - row_id

    def visit_tiles(sections, jobs, tables):
        for slot, count, tile, span, masked in sections:
            unit = slot - jnp.where(slot >= near, near, 0)
            keys = span * key_tile
            key_values, scores = [], []
            for query_head, key_head in jobs:
                key_value = kv_all[pl.ds(tile * blocks_per_tile, span * blocks_per_tile), key_head]
                key_values.append(key_value.reshape(keys, LANES))
                queries = query_buf[query_head, pl.ds(unit, count)].reshape(count * rows, LANES)
                scores.append(
                    lax.dot_general(
                        queries,
                        key_values[-1],
                        (((1,), (1,)), ((), ())),
                        preferred_element_type=jnp.float32,
                    )
                )
            weights = [[] for _ in jobs]
            for first in range(0, keys, LANES):
                columns = [[] for _ in jobs]
                key_stamp = stamp_keys[
                    tile + first // key_tile, :, first % key_tile : first % key_tile + LANES
                ]
                for top in range(0, count * rows, chunk):
                    place, start = top // rows, top % rows
                    query_stamp = stamp_rows[slot + place, start : start + chunk]
                    elapsed = query_stamp - key_stamp
                    biases = biases_of(elapsed, tables, (top // chunk + first // LANES) % 3 != 0)
                    for score, bias, column in zip(scores, biases, columns):
                        halved = score[top : top + chunk, first : first + LANES] + bias
                        halved = halved.astype(jnp.bfloat16)
                        weight = halved + halved * jnp.tanh(halved)
                        if masked:
                            ahead = tile * key_tile + first - block_of(slot, my_split) * rows - start
                            weight = jnp.where(spread <= -ahead, weight.astype(jnp.float32), 0.0)
                            weight = weight.astype(jnp.bfloat16)
                        column.append(weight)
                for weight, column in zip(weights, columns):
                    weight.append(jnp.concatenate(column, axis=0))
            for (query_head, _), weight, key_value in zip(jobs, weights, key_values):
                sums = jnp.dot(
                    jnp.concatenate(weight, axis=1), key_value, preferred_element_type=jnp.float32
                )
                total_buf[query_head, pl.ds(unit, count)] += sums.reshape(count, rows, LANES)

    def visit(sections, jobs, tables):
        def one(step, carry):
            visit_tiles(
                [
                    (slot, count, group * group_tiles + span * step, span, masked)
                    for slot, count, group, span, masked in sections
                ],
                jobs,
                tables,
            )
            return carry

        if group_tiles == 1:
            one(0, 0)
        else:
            lax.fori_loop(0, group_tiles, one, 0)

    def visit_near(*pairs):
        visit(
            [
                (jnp.maximum(one, other), 1, jnp.minimum(one, other), 1, masked)
                for one, other, masked in pairs
            ],
            [(0, 0), (1, 1)],
            near_tables,
        )

    def back_copy(kind, unit):
        slot = unit + (near if kind == 2 else near_first)
        target, semaphore = (
            (part_out.at[my_place], part_sem)
            if kind == 2
            else (att_out.at[2 * my_place + kind], att_sem)
        )
        block = block_of(slot, my_split)
        return block, remote(
            back_buf.at[kind, unit], target, back_sem.at[kind], semaphore, block
        )

    def own_copy(kind, unit):
        return pltpu.make_async_copy(
            back_buf.at[kind, unit], att_out.at[2 * my_place + kind], own_sem.at[kind]
        )

    def finish(kind, first, count):
        def one(unit, carry):
            block, copy = back_copy(kind, unit)
            total = total_buf[kind, unit]
            result = jnp.where(low, pltpu.roll(total[:half], head_size, 1), total[half:])
            result = result.astype(jnp.bfloat16)
            back_buf[kind, unit] = result
            if kind == 2:
                copy.start()
                return carry

            @pl.when(block == me)
            def _():
                own_copy(kind, unit).start()

            @pl.when(block != me)
            def _():
                copy.start()

            return carry

        lax.fori_loop(first, first + count, one, 0)

    def near_at(step):
        return near_first + (my_place ^ jnp.where(step == 0, 0, near - step))

    take_direct(near_at(0))

    def near_step(step, carry):
        group = near_at(step)

        @pl.when((step == 1) & (farther > 0))
        def _():
            each_far(near // 2, farther, lambda copy: copy.start())

        @pl.when(step + 1 < near)
        def _():
            take_direct(near_at(step + 1))

        take_forwarded(group)
        take_query(group)

        @pl.when((upper == 1) & (step + 1 == near))
        def _():
            for late in range(near // 2, near):
                take_late_direct(late)

        @pl.when(step == 0)
        def _():
            visit_near((group, group, True))

        @pl.when(step > 0)
        def _():
            visit_near((group, group, True), (group, near_at(step - 1), False))

        def two(pair, inner):
            visit_near((group, near_at(2 * pair), False), (group, near_at(2 * pair + 1), False))
            return inner

        lax.fori_loop(0, jnp.maximum(step - 1, 0) // 2, two, 0)

        @pl.when((step > 1) & (step % 2 == 0))
        def _():
            visit_near((group, near_at(step - 2), False))

        return carry

    lax.fori_loop(0, near, near_step, 0)

    @pl.when(upper == 0)
    def _():
        finish(0, 0, near)
        finish(1, 0, near)
        all_stamps(1).wait_recv()
        lax.fori_loop(near, 2 * near, turn_stamps, 0)
        all_far_queries().wait_recv()
        lax.fori_loop(near, 2 * near, take_far_query, 0)

    @pl.when(upper == 1)
    def _():
        for late in range(near // 2):
            take_late_direct(late)
        finish(0, 0, near)
        all_stamps(1).wait_recv()
        lax.fori_loop(0, near * group_tiles, join_stamps, 0)

    halves = near // 2

    def square(step, carry):
        major, minor = step // halves, step % halves
        slots = 2 * jnp.where(upper == 0, halves - 1 - major, minor)
        groups = 2 * (halves - 1 - jnp.where(upper == 0, minor, major))

        @pl.when((upper == 1) & (minor == 0))
        def _():
            take_late_forwarded(groups)
            take_late_forwarded(groups + 1)

        visit([(near + slots, 2, groups, 2, False)], [(2 - upper, upper)], square_tables)

        @pl.when((upper == 0) & (minor == halves - 1))
        def _():
            finish(2, slots, 2)

        @pl.when((upper == 1) & (major == halves - 1))
        def _():
            finish(1, slots, 2)

        return carry

    lax.fori_loop(0, halves * halves, square, 0)

    all_stamps(0).wait_send()
    all_stamps(1).wait_send()

    def forwards():
        some = kv_all.at[pl.ds(0, near * (splits - 1))]
        return remote(some, some, fwd_sem.at[0], fwd_sem.at[0], near_peer(1))

    def late_forwards():
        some = kv_all.at[pl.ds(0, near * (splits - 1)), 1]
        return remote(some, some, fwd_sem.at[1], fwd_sem.at[1], near_peer(1))

    def wait_near(count):
        some = kv_all.at[pl.ds(0, count)]
        remote(some, some, kv_send_sem, kv_send_sem, near_peer(1)).wait_send()
        some = q_all.at[pl.ds(0, count)]
        remote(some, some, q_send_sem, q_send_sem, near_peer(1)).wait_send()

    def results(count, send, receive):
        some = att_out.at[pl.ds(0, count)]
        return remote(some, some, send, receive, near_peer(1))

    home = my_home == my_split
    forwards().wait_send()

    @pl.when(home)
    def _():
        wait_near(near - 1)
        results(2 * near - 2, att_sem, att_sem).wait_recv()
        for kind in range(2):
            own_copy(kind, 0).wait()
            results(near - 1, back_sem.at[kind], back_sem.at[kind]).wait_send()

    @pl.when(jnp.logical_not(home))
    def _():
        wait_near(near)
        results(2 * near, att_sem, att_sem).wait_recv()
        for kind in range(2):
            results(near, back_sem.at[kind], back_sem.at[kind]).wait_send()

    @pl.when(upper == 0)
    def _():
        def wait_late(count, semaphore):
            some = kv_send.at[pl.ds(0, count), 1]
            remote(some, some, semaphore, semaphore, near_peer(1)).wait_send()

        wait_late(near // 2, far_send_sem)

        @pl.when(relays > 0)
        def _():
            wait_late(near // 2, far_send_sem)
            wait_late(near // 2, fwd_sem.at[1])

        results(near, back_sem.at[2], back_sem.at[2]).wait_send()
        no_part.wait()

    @pl.when(upper == 1)
    def _():
        all_far_queries().wait_send()
        late_forwards().wait_send()
        results(near, part_sem, part_sem).wait_recv()

    gate_store.wait()


def final_kernel(
    att_hbm,
    part_hbm,
    gate_hbm,
    tokens_hbm,
    attn_gain_hbm,
    w_out_hbm,
    out_hbm,
    att_buf,
    part_buf,
    gate_buf,
    tokens_ref,
    attn_gain_ref,
    w_out_ref,
    out_buf,
    load_sem,
    store_sem,
):
    loads = [
        pltpu.make_async_copy(source, target, load_sem.at[index])
        for index, (source, target) in enumerate(
            [
                (att_hbm, att_buf),
                (part_hbm, part_buf),
                (gate_hbm, gate_buf),
                (attn_gain_hbm, attn_gain_ref),
                (w_out_hbm, w_out_ref),
                (tokens_hbm, tokens_ref),
            ]
        )
    ]
    for load in loads:
        load.start()
    heads, half, _ = att_buf.shape
    head_size = tokens_ref.shape[1] // heads
    low = lax.broadcasted_iota(jnp.int32, (1, LANES), 1) < head_size
    for load in loads[:4]:
        load.wait()
    stores = []
    for side in range(2):
        pieces = []
        for pair in range(heads // 2):
            even = att_buf[2 * pair].astype(jnp.float32) + part_buf[pair].astype(jnp.float32)
            odd = att_buf[2 * pair + 1].astype(jnp.float32)
            if side == 0:
                pieces.append(jnp.where(low, even, pltpu.roll(odd, head_size, 1)))
            else:
                pieces.append(jnp.where(low, pltpu.roll(even, head_size, 1), odd))
        attended = jnp.concatenate(pieces, axis=1)
        part = slice(side * half, (side + 1) * half)
        gated = layer_norm(attended, attn_gain_ref[...]) * gate_buf[part].astype(jnp.float32)
        if side == 0:
            loads[4].wait()
            loads[5].wait()
        mixed = tokens_ref[part].astype(jnp.float32) + jnp.dot(
            gated.astype(jnp.bfloat16), w_out_ref[...], preferred_element_type=jnp.float32
        )
        out_buf[part] = mixed.astype(jnp.bfloat16)
        rows = pl.ds(side * half, half)
        stores.append(
            pltpu.make_async_copy(out_buf.at[rows], out_hbm.at[rows], store_sem.at[side])
        )
        stores[-1].start()
    for store in stores:
        store.wait()


def solution(mesh):
    parts = mesh.shape["pb"]

    def body(tokens, stamps, norm_gain, w_proj, rel_bias, attn_gain, w_out):
        rows, width = tokens.shape
        heads = rel_bias.shape[0]
        splits = parts // heads
        near = heads // 2
        blocks_per_tile = max(1, 384 // rows)
        att, part, gate = pl.pallas_call(
            functools.partial(kernel, parts, heads),
            out_shape=[
                jax.ShapeDtypeStruct((heads, rows // 2, LANES), jnp.bfloat16),
                jax.ShapeDtypeStruct((near, rows // 2, LANES), jnp.bfloat16),
                jax.ShapeDtypeStruct((rows, width), jnp.bfloat16),
            ],
            in_specs=[pl.BlockSpec(memory_space=pltpu.HBM)] * 5,
            out_specs=[pl.BlockSpec(memory_space=pltpu.HBM)] * 3,
            scratch_shapes=[
                pltpu.VMEM((rows, width), jnp.bfloat16),
                pltpu.VMEM((1, rows), jnp.int32),
                pltpu.VMEM((1, width), jnp.float32),
                pltpu.VMEM(w_proj.shape, jnp.bfloat16),
                pltpu.SMEM(rel_bias.shape, jnp.float32),
                pltpu.VMEM((near, 2, rows, LANES), jnp.bfloat16),
                pltpu.VMEM((near, 2, rows // 2, LANES), jnp.bfloat16),
                pltpu.VMEM((parts, 2, rows, LANES), jnp.bfloat16),
                pltpu.VMEM((heads, 2, rows // 2, LANES), jnp.bfloat16),
                pltpu.VMEM((3, near, rows, LANES), jnp.bfloat16),
                pltpu.VMEM((parts, 1, rows), jnp.int32),
                pltpu.VMEM((parts // blocks_per_tile, 1, blocks_per_tile * rows), jnp.int32),
                pltpu.VMEM((heads, rows, LANES), jnp.int32),
                pltpu.VMEM((3, near, rows, LANES), jnp.float32),
                pltpu.VMEM((rows, width), jnp.bfloat16),
                pltpu.VMEM((3, near, rows // 2, LANES), jnp.bfloat16),
                pltpu.VMEM((near, rows // 2, LANES), jnp.bfloat16),
                pltpu.SemaphoreType.DMA((6,)),
                pltpu.SemaphoreType.DMA,
                pltpu.SemaphoreType.DMA,
                pltpu.SemaphoreType.DMA,
                pltpu.SemaphoreType.DMA((2,)),
                pltpu.SemaphoreType.DMA((parts,)),
                pltpu.SemaphoreType.DMA((near,)),
                pltpu.SemaphoreType.DMA,
                pltpu.SemaphoreType.DMA((2,)),
                pltpu.SemaphoreType.DMA((2,)),
                pltpu.SemaphoreType.DMA((3,)),
                pltpu.SemaphoreType.DMA,
                pltpu.SemaphoreType.DMA,
                pltpu.SemaphoreType.REGULAR,
                pltpu.SemaphoreType.DMA((4,)),
            ],
            compiler_params=pltpu.CompilerParams(
                collective_id=0, has_side_effects=True
            ),
        )(
            tokens,
            stamps.reshape(1, rows),
            norm_gain.reshape(1, width),
            w_proj,
            rel_bias,
        )
        hbm = pl.BlockSpec(memory_space=pltpu.HBM)
        return pl.pallas_call(
            final_kernel,
            out_shape=jax.ShapeDtypeStruct((rows, width), jnp.bfloat16),
            in_specs=[hbm] * 6,
            out_specs=hbm,
            scratch_shapes=[
                pltpu.VMEM((heads, rows // 2, LANES), jnp.bfloat16),
                pltpu.VMEM((near, rows // 2, LANES), jnp.bfloat16),
                pltpu.VMEM((rows, width), jnp.bfloat16),
                pltpu.VMEM((rows, width), jnp.bfloat16),
                pltpu.VMEM((1, width), jnp.float32),
                pltpu.VMEM(w_out.shape, jnp.bfloat16),
                pltpu.VMEM((rows, width), jnp.bfloat16),
                pltpu.SemaphoreType.DMA((6,)),
                pltpu.SemaphoreType.DMA((2,)),
            ],
        )(att, part, gate, tokens, attn_gain.reshape(1, width), w_out)

    return jax.shard_map(
        body,
        mesh=mesh,
        in_specs=(P(("groups", "pb"), None), P(("groups", "pb")), P(), P(), P(), P(), P()),
        out_specs=P(("groups", "pb"), None),
        check_vma=False,
    )
```

```python
import functools

import jax
import jax.numpy as jnp
from jax import lax
from jax.experimental import pallas as pl
from jax.experimental.pallas import tpu as pltpu
from jax.sharding import PartitionSpec as P

EPSILON = 1e-05
LANES = 128


def layer_norm(values, gain):
    centered = values - jnp.mean(values, axis=-1, keepdims=True)
    spread = jnp.mean(centered * centered, axis=-1, keepdims=True)
    return centered * lax.rsqrt(spread + EPSILON) * gain


LANE_LOOKUP = lax.GatherDimensionNumbers(
    offset_dims=(),
    collapsed_slice_dims=(1,),
    start_index_map=(1,),
    operand_batching_dims=(0,),
    start_indices_batching_dims=(0,),
)
ROW_LOOKUP = lax.GatherDimensionNumbers(
    offset_dims=(),
    collapsed_slice_dims=(1,),
    start_index_map=(1,),
    operand_batching_dims=(0, 2),
    start_indices_batching_dims=(0, 2),
)


def look_up(table, index, dimensions):
    return lax.gather(
        table,
        index[..., None],
        dimensions,
        (1,) * table.ndim,
        mode=lax.GatherScatterMode.PROMISE_IN_BOUNDS,
    )


def kernel(
    parts,
    heads,
    tokens_hbm,
    stamps_hbm,
    norm_gain_hbm,
    w_proj_hbm,
    bias_hbm,
    att_out,
    part_out,
    gate_out,
    tokens_ref,
    stamps_ref,
    norm_gain_ref,
    w_proj_ref,
    bias_ref,
    kv_send,
    q_send,
    kv_all,
    q_all,
    query_buf,
    stamp_all,
    stamp_keys,
    stamp_rows,
    total_buf,
    gate_buf,
    back_buf,
    zero_buf,
    load_sem,
    kv_send_sem,
    q_send_sem,
    far_send_sem,
    fwd_sem,
    kv_sem,
    q_sem,
    far_q_sem,
    stamp_send_sem,
    stamp_sem,
    back_sem,
    att_sem,
    part_sem,
    far_ready,
    own_sem,
):
    rows, width = tokens_ref.shape
    half = rows // 2
    head_size = width // heads
    splits = parts // heads
    near = heads // 2
    side = parts // 2
    blocks_per_tile = max(1, 384 // rows)
    key_tile = blocks_per_tile * rows
    group_tiles = splits // blocks_per_tile
    buckets = bias_ref.shape[1]

    loads = [
        pltpu.make_async_copy(source, target, load_sem.at[index])
        for index, (source, target) in enumerate(
            [
                (tokens_hbm, tokens_ref),
                (norm_gain_hbm, norm_gain_ref),
                (w_proj_hbm.at[:, width:], w_proj_ref.at[:, width:]),
                (stamps_hbm, stamps_ref),
                (bias_hbm, bias_ref),
                (w_proj_hbm.at[:, :width], w_proj_ref.at[:, :width]),
            ]
        )
    ]
    for load in loads:
        load.start()

    me = lax.axis_index("pb")
    my_group = me // splits
    my_split = me % splits
    upper = my_group // near
    my_place = my_group % near
    near_first = upper * near
    far_first = near - near_first
    side_first = upper * side

    def split_of(block):
        place = block % splits
        odd = (block // splits) % 2
        return place + odd * (splits - 1 - 2 * place)

    def block_of(slot, split):
        odd = slot % 2
        return slot * splits + split + odd * (splits - 1 - 2 * split)

    def remote(source, target, send, receive, device):
        return pltpu.make_async_remote_copy(
            src_ref=source,
            dst_ref=target,
            send_sem=send,
            recv_sem=receive,
            device_id={"pb": device},
            device_id_type=pl.DeviceIdType.MESH,
        )

    barrier = pltpu.get_barrier_semaphore()

    def signal(semaphore, other):
        pl.semaphore_signal(
            semaphore, inc=1, device_id={"pb": other}, device_id_type=pl.DeviceIdType.MESH
        )

    def near_peer(step):
        return side_first + lax.rem(me - side_first + step, side)

    def far_peer(step):
        return side - side_first + lax.rem(me - side_first + step, side)

    def greet(step, carry):
        signal(barrier, near_peer(step))
        return carry

    lax.fori_loop(1, side, greet, 0)
    signal(barrier, far_peer(0))

    low = lax.broadcasted_iota(jnp.int32, (1, LANES), 1) < head_size

    for load in loads[:3]:
        load.wait()
    normed = layer_norm(tokens_ref[...].astype(jnp.float32), norm_gain_ref[...]).astype(jnp.bfloat16)
    front = jnp.dot(normed, w_proj_ref[:, width : 2 * width], preferred_element_type=jnp.float32)
    scaled = front.astype(jnp.bfloat16).astype(jnp.float32) * (0.5 * head_size ** (-0.5))
    back = jnp.dot(normed, w_proj_ref[:, 2 * width :], preferred_element_type=jnp.float32)
    for pair in range(near):
        cols = slice(pair * LANES, (pair + 1) * LANES)
        key_cols = back[:, :width][:, cols]
        value_cols = back[:, width:][:, cols]
        query_cols = scaled[:, cols]
        kv_send[pair, 0] = jnp.where(
            low, key_cols, pltpu.roll(value_cols, head_size, 1)
        ).astype(jnp.bfloat16)
        kv_send[pair, 1] = jnp.where(
            low, pltpu.roll(key_cols, head_size, 1), value_cols
        ).astype(jnp.bfloat16)
        top, bottom = query_cols[:half], query_cols[half:]
        q_send[pair, 0] = jnp.where(low, top, pltpu.roll(bottom, head_size, 1)).astype(jnp.bfloat16)
        q_send[pair, 1] = jnp.where(low, pltpu.roll(top, head_size, 1), bottom).astype(jnp.bfloat16)
    loads[3].wait()
    loads[4].wait()

    my_home = split_of(me)

    def stamp_copy(target, kind):
        return remote(
            stamps_ref, stamp_all.at[me], stamp_send_sem.at[kind], stamp_sem.at[kind], target
        )

    def all_stamps(kind):
        some = stamp_all.at[pl.ds(0, side - 1 + kind)]
        return remote(some, some, stamp_send_sem.at[kind], stamp_sem.at[kind], near_peer(1))

    def kv_copy(place, target):
        return remote(kv_send.at[place], kv_all.at[me], kv_send_sem, kv_sem.at[me], target)

    def q_copy(place, target):
        return remote(
            q_send.at[place], q_all.at[my_group], q_send_sem, q_sem.at[my_place], target
        )

    def late_kv_copy(place, target):
        return remote(
            kv_send.at[place, 1], kv_all.at[me, 1], far_send_sem, kv_sem.at[me], target
        )

    def early_q_copy(place, target):
        return remote(
            q_send.at[place, 0], q_all.at[my_group, 0], far_send_sem, far_q_sem, target
        )

    def each_near(act):
        def one(step, carry):
            place = my_place ^ step
            target = (near_first + place) * splits + my_home

            @pl.when(target != me)
            def _():
                act(place, target)

            return carry

        lax.fori_loop(0, near, one, 0)

    relays = (1 - upper) * (my_place // (near // 2)) * (near // 2)
    farther = jnp.maximum(relays, upper * (near // 2))

    def far_place(step):
        place = step + (my_place % 2) * (1 - 2 * (step % 2))
        return place + upper * (near - 1 - 2 * place)

    def each_far(first, count, act):
        def one(step, carry):
            place = far_place(step)
            target = (far_first + place) * splits + my_home

            @pl.when(upper == 0)
            def _():
                act(late_kv_copy(place, target))

            @pl.when(upper == 1)
            def _():
                act(early_q_copy(place, target))

            return carry

        lax.fori_loop(first, first + count, one, 0)

    def send_near_stamps(step, carry):
        stamp_copy(near_peer(step), 0).start()
        return carry

    def send_far_stamps(step, carry):
        stamp_copy(far_peer(step), 1).start()
        return carry

    def start_both(place, target):
        q_copy(place, target).start()
        kv_copy(place, target).start()

    pl.semaphore_wait(barrier, side)

    def pass_on(step, carry):
        signal(far_ready, near_peer(step))
        return carry

    lax.fori_loop(1, side, pass_on, 0)
    lax.fori_loop(1, side, send_near_stamps, 0)
    each_near(start_both)

    stamp_all[me] = stamps_ref[...]

    @pl.when(my_home == my_split)
    def _():
        kv_all[me] = kv_send[my_place]
        q_all[my_group] = q_send[my_place]

    gate_store = pltpu.make_async_copy(gate_buf, gate_out, own_sem.at[2])
    no_part = pltpu.make_async_copy(zero_buf, part_out, own_sem.at[3])

    @pl.when(upper == 0)
    def _():
        zero_buf[...] = jnp.zeros_like(zero_buf)
        no_part.start()

    loads[5].wait()
    gate_proj = jnp.dot(normed, w_proj_ref[:, :width], preferred_element_type=jnp.float32)
    gate_buf[...] = jax.nn.silu(gate_proj).astype(jnp.bfloat16)
    gate_store.start()
    total_buf[...] = jnp.zeros_like(total_buf)

    pl.semaphore_wait(far_ready, side - 1)
    lax.fori_loop(0, side, send_far_stamps, 0)
    each_far(0, near // 2, lambda copy: copy.start())

    lane_id = lax.broadcasted_iota(jnp.int32, (8, LANES), 1)
    place_id = lax.broadcasted_iota(jnp.int32, (8, LANES), 0)

    def tables_of(head):
        def half_bias(bucket):
            table = jnp.zeros((8, LANES), jnp.float32)
            for bucket_id in range(buckets):
                table = jnp.where(bucket == bucket_id, 0.5 * bias_ref[head, bucket_id], table)
            return table

        return (
            half_bias(jnp.clip((33 - lane_id) >> 1, 0, buckets - 1))[:1],
            half_bias(jnp.where(place_id == 0, 8, 16 - place_id)),
            half_bias(jnp.where(place_id == 0, 0, 8 - place_id)),
        )

    near_tables = [tables_of(2 * my_place), tables_of(2 * my_place + 1)]
    square_tables = [tables_of(2 * my_place + upper)]

    def biases_of(elapsed, tables, by_rows):
        if not by_rows:
            index = lax.clz(elapsed)
            return [look_up(jnp.broadcast_to(lane, elapsed.shape), index, LANE_LOOKUP) for lane, _, _ in tables]
        tiles = (elapsed.shape[0] // 8, 8, LANES)
        zeros_count = lax.clz(jnp.minimum(elapsed, 2**30 - 1))
        index = ((zeros_count >> 1) & 7).reshape(tiles)
        old = elapsed >= 4**7
        biases = []
        for _, far_table, close_table in tables:
            far_bias = look_up(jnp.broadcast_to(far_table[None], tiles), index, ROW_LOOKUP)
            close_bias = look_up(jnp.broadcast_to(close_table[None], tiles), index, ROW_LOOKUP)
            biases.append(
                jnp.where(old, far_bias.reshape(elapsed.shape), close_bias.reshape(elapsed.shape))
            )
        return biases

    def join_stamps(tile, carry):
        stamp_keys[tile] = jnp.concatenate(
            [stamp_all[tile * blocks_per_tile + place] for place in range(blocks_per_tile)], axis=1
        )
        return carry

    def turn_stamps(slot, carry):
        block = block_of(slot, my_split)
        stamp_rows[slot] = jnp.transpose(jnp.broadcast_to(stamp_all[block], (LANES, rows)))
        return carry

    all_stamps(0).wait_recv()
    lax.fori_loop(near_first * group_tiles, (near_first + near) * group_tiles, join_stamps, 0)
    lax.fori_loop(near_first, near_first + near, turn_stamps, 0)

    def forward(source, step):
        peer = my_group * splits + lax.rem(my_split + step, splits)
        return remote(
            kv_all.at[source], kv_all.at[source], fwd_sem.at[0], kv_sem.at[source], peer
        )

    def late_forward(source, step):
        peer = my_group * splits + lax.rem(my_split + step, splits)
        return remote(
            kv_all.at[source, 1], kv_all.at[source, 1], fwd_sem.at[1], kv_sem.at[source], peer
        )

    def relay(source):
        return remote(
            kv_all.at[source, 1],
            kv_all.at[source, 1],
            fwd_sem.at[1],
            kv_sem.at[source],
            (far_first + my_place) * splits + my_split,
        )

    def take_direct(slot):
        source = block_of(slot, my_split)

        @pl.when(source != me)
        def _():
            remote(
                kv_send.at[0], kv_all.at[source], kv_send_sem, kv_sem.at[source], source
            ).wait_recv()

        for step in range(1, splits):
            forward(source, step).start()

        @pl.when(slot < relays)
        def _():
            relay(source).start()

    def take_forwarded(slot):
        for step in range(1, splits):
            source = block_of(slot, lax.rem(my_split + step, splits))
            forward(source, step).wait_recv()

    def take_late_direct(slot):
        source = block_of(slot, my_split)
        remote(
            kv_send.at[0, 1], kv_all.at[source, 1], far_send_sem, kv_sem.at[source], source
        ).wait_recv()
        for step in range(1, splits):
            late_forward(source, step).start()

    def take_late_forwarded(slot):
        for step in range(1, splits):
            source = block_of(slot, lax.rem(my_split + step, splits))
            late_forward(source, step).wait_recv()

    def unpack(packed):
        packed = packed.astype(jnp.float32)
        return jnp.concatenate(
            [jnp.where(low, packed, 0.0), jnp.where(low, pltpu.roll(packed, head_size, 1), 0.0)], axis=0
        ).astype(jnp.bfloat16)

    def take_query(slot):
        source = block_of(slot, my_split)

        @pl.when(source != me)
        def _():
            remote(
                q_send.at[0], q_all.at[slot], q_send_sem, q_sem.at[slot - near_first], source
            ).wait_recv()

        for head in range(2):
            query_buf[head, slot - near_first] = unpack(q_all[slot, head])

    def take_far_query(slot, carry):
        query_buf[2, slot - near] = unpack(q_all[slot, 0])
        return carry

    def all_far_queries():
        some = q_all.at[pl.ds(0, near), 0]
        return remote(some, some, far_send_sem, far_q_sem, near_peer(1))

    chunk = 64
    row_id = lax.broadcasted_iota(jnp.int32, (chunk, LANES), 0)
    col_id = lax.broadcasted_iota(jnp.int32, (chunk, LANES), 1)
    spread = col_id - row_id

    def visit_tiles(sections, jobs, tables):
        for slot, count, tile, span, masked in sections:
            unit = slot - jnp.where(slot >= near, near, 0)
            keys = span * key_tile
            key_values, scores = [], []
            for query_head, key_head in jobs:
                key_value = kv_all[pl.ds(tile * blocks_per_tile, span * blocks_per_tile), key_head]
                key_values.append(key_value.reshape(keys, LANES))
                queries = query_buf[query_head, pl.ds(unit, count)].reshape(count * rows, LANES)
                scores.append(
                    lax.dot_general(
                        queries,
                        key_values[-1],
                        (((1,), (1,)), ((), ())),
                        preferred_element_type=jnp.float32,
                    )
                )
            weights = [[] for _ in jobs]
            for first in range(0, keys, LANES):
                columns = [[] for _ in jobs]
                key_stamp = stamp_keys[
                    tile + first // key_tile, :, first % key_tile : first % key_tile + LANES
                ]
                for top in range(0, count * rows, chunk):
                    place, start = top // rows, top % rows
                    query_stamp = stamp_rows[slot + place, start : start + chunk]
                    elapsed = query_stamp - key_stamp
                    biases = biases_of(elapsed, tables, (top // chunk + first // LANES) % 3 != 0)
                    for score, bias, column in zip(scores, biases, columns):
                        halved = score[top : top + chunk, first : first + LANES] + bias
                        weight = halved + halved * jnp.tanh(halved)
                        if masked:
                            ahead = tile * key_tile + first - block_of(slot, my_split) * rows - start
                            weight = jnp.where(spread <= -ahead, weight, 0.0)
                        column.append(weight.astype(jnp.bfloat16))
                for weight, column in zip(weights, columns):
                    weight.append(jnp.concatenate(column, axis=0))
            for (query_head, _), weight, key_value in zip(jobs, weights, key_values):
                sums = jnp.dot(
                    jnp.concatenate(weight, axis=1), key_value, preferred_element_type=jnp.float32
                )
                total_buf[query_head, pl.ds(unit, count)] += sums.reshape(count, rows, LANES)

    def visit(sections, jobs, tables):
        def one(step, carry):
            visit_tiles(
                [
                    (slot, count, group * group_tiles + span * step, span, masked)
                    for slot, count, group, span, masked in sections
                ],
                jobs,
                tables,
            )
            return carry

        if group_tiles == 1:
            one(0, 0)
        else:
            lax.fori_loop(0, group_tiles, one, 0)

    def visit_near(*pairs):
        visit(
            [
                (jnp.maximum(one, other), 1, jnp.minimum(one, other), 1, masked)
                for one, other, masked in pairs
            ],
            [(0, 0), (1, 1)],
            near_tables,
        )

    def back_copy(kind, unit):
        slot = unit + (near if kind == 2 else near_first)
        target, semaphore = (
            (part_out.at[my_place], part_sem)
            if kind == 2
            else (att_out.at[2 * my_place + kind], att_sem)
        )
        block = block_of(slot, my_split)
        return block, remote(
            back_buf.at[kind, unit], target, back_sem.at[kind], semaphore, block
        )

    def own_copy(kind, unit):
        return pltpu.make_async_copy(
            back_buf.at[kind, unit], att_out.at[2 * my_place + kind], own_sem.at[kind]
        )

    def finish(kind, first, count):
        def one(unit, carry):
            block, copy = back_copy(kind, unit)
            total = total_buf[kind, unit]
            result = jnp.where(low, pltpu.roll(total[:half], head_size, 1), total[half:])
            result = result.astype(jnp.bfloat16)
            back_buf[kind, unit] = result
            if kind == 2:
                copy.start()
                return carry

            @pl.when(block == me)
            def _():
                own_copy(kind, unit).start()

            @pl.when(block != me)
            def _():
                copy.start()

            return carry

        lax.fori_loop(first, first + count, one, 0)

    def near_at(step):
        return near_first + (my_place ^ step)

    take_direct(near_at(0))

    def near_step(step, carry):
        group = near_at(step)

        @pl.when((step == 1) & (farther > 0))
        def _():
            each_far(near // 2, farther, lambda copy: copy.start())

        @pl.when(step + 1 < near)
        def _():
            take_direct(near_at(step + 1))

        take_forwarded(group)
        take_query(group)

        @pl.when((upper == 1) & (step + 1 == near))
        def _():
            for late in range(near // 2, near):
                take_late_direct(late)

        @pl.when(step == 0)
        def _():
            visit_near((group, group, True))

        @pl.when(step > 0)
        def _():
            visit_near((group, group, True), (group, near_at(step - 1), False))

        def two(pair, inner):
            visit_near((group, near_at(2 * pair), False), (group, near_at(2 * pair + 1), False))
            return inner

        lax.fori_loop(0, jnp.maximum(step - 1, 0) // 2, two, 0)

        @pl.when((step > 1) & (step % 2 == 0))
        def _():
            visit_near((group, near_at(step - 2), False))

        return carry

    lax.fori_loop(0, near, near_step, 0)

    @pl.when(upper == 0)
    def _():
        finish(0, 0, near)
        finish(1, 0, near)
        all_stamps(1).wait_recv()
        lax.fori_loop(near, 2 * near, turn_stamps, 0)
        all_far_queries().wait_recv()
        lax.fori_loop(near, 2 * near, take_far_query, 0)

    @pl.when(upper == 1)
    def _():
        for late in range(near // 2):
            take_late_direct(late)
        finish(0, 0, near)
        all_stamps(1).wait_recv()
        lax.fori_loop(0, near * group_tiles, join_stamps, 0)

    halves = near // 2

    def square(step, carry):
        major, minor = step // halves, step % halves
        slots = 2 * jnp.where(upper == 0, halves - 1 - major, minor)
        groups = 2 * (halves - 1 - jnp.where(upper == 0, minor, major))

        @pl.when((upper == 1) & (minor == 0))
        def _():
            take_late_forwarded(groups)
            take_late_forwarded(groups + 1)

        visit([(near + slots, 2, groups, 2, False)], [(2 - upper, upper)], square_tables)

        @pl.when((upper == 0) & (minor == halves - 1))
        def _():
            finish(2, slots, 2)

        @pl.when((upper == 1) & (major == halves - 1))
        def _():
            finish(1, slots, 2)

        return carry

    lax.fori_loop(0, halves * halves, square, 0)

    all_stamps(0).wait_send()
    all_stamps(1).wait_send()

    def forwards():
        some = kv_all.at[pl.ds(0, near * (splits - 1))]
        return remote(some, some, fwd_sem.at[0], fwd_sem.at[0], near_peer(1))

    def late_forwards():
        some = kv_all.at[pl.ds(0, near * (splits - 1)), 1]
        return remote(some, some, fwd_sem.at[1], fwd_sem.at[1], near_peer(1))

    def wait_near(count):
        some = kv_all.at[pl.ds(0, count)]
        remote(some, some, kv_send_sem, kv_send_sem, near_peer(1)).wait_send()
        some = q_all.at[pl.ds(0, count)]
        remote(some, some, q_send_sem, q_send_sem, near_peer(1)).wait_send()

    def results(count, send, receive):
        some = att_out.at[pl.ds(0, count)]
        return remote(some, some, send, receive, near_peer(1))

    home = my_home == my_split
    forwards().wait_send()

    @pl.when(home)
    def _():
        wait_near(near - 1)
        results(2 * near - 2, att_sem, att_sem).wait_recv()
        for kind in range(2):
            own_copy(kind, 0).wait()
            results(near - 1, back_sem.at[kind], back_sem.at[kind]).wait_send()

    @pl.when(jnp.logical_not(home))
    def _():
        wait_near(near)
        results(2 * near, att_sem, att_sem).wait_recv()
        for kind in range(2):
            results(near, back_sem.at[kind], back_sem.at[kind]).wait_send()

    @pl.when(upper == 0)
    def _():
        def wait_late(count, semaphore):
            some = kv_send.at[pl.ds(0, count), 1]
            remote(some, some, semaphore, semaphore, near_peer(1)).wait_send()

        wait_late(near // 2, far_send_sem)

        @pl.when(relays > 0)
        def _():
            wait_late(near // 2, far_send_sem)
            wait_late(near // 2, fwd_sem.at[1])

        results(near, back_sem.at[2], back_sem.at[2]).wait_send()
        no_part.wait()

    @pl.when(upper == 1)
    def _():
        all_far_queries().wait_send()
        late_forwards().wait_send()
        results(near, part_sem, part_sem).wait_recv()

    gate_store.wait()


def final_kernel(
    att_hbm,
    part_hbm,
    gate_hbm,
    tokens_hbm,
    attn_gain_hbm,
    w_out_hbm,
    out_hbm,
    att_buf,
    part_buf,
    gate_buf,
    tokens_ref,
    attn_gain_ref,
    w_out_ref,
    out_buf,
    load_sem,
    store_sem,
):
    loads = [
        pltpu.make_async_copy(source, target, load_sem.at[index])
        for index, (source, target) in enumerate(
            [
                (att_hbm, att_buf),
                (part_hbm, part_buf),
                (gate_hbm, gate_buf),
                (attn_gain_hbm, attn_gain_ref),
                (w_out_hbm, w_out_ref),
                (tokens_hbm, tokens_ref),
            ]
        )
    ]
    for load in loads:
        load.start()
    heads, half, _ = att_buf.shape
    head_size = tokens_ref.shape[1] // heads
    low = lax.broadcasted_iota(jnp.int32, (1, LANES), 1) < head_size
    for load in loads[:4]:
        load.wait()
    stores = []
    for side in range(2):
        pieces = []
        for pair in range(heads // 2):
            even = att_buf[2 * pair].astype(jnp.float32) + part_buf[pair].astype(jnp.float32)
            odd = att_buf[2 * pair + 1].astype(jnp.float32)
            if side == 0:
                pieces.append(jnp.where(low, even, pltpu.roll(odd, head_size, 1)))
            else:
                pieces.append(jnp.where(low, pltpu.roll(even, head_size, 1), odd))
        attended = jnp.concatenate(pieces, axis=1)
        part = slice(side * half, (side + 1) * half)
        gated = layer_norm(attended, attn_gain_ref[...]) * gate_buf[part].astype(jnp.float32)
        if side == 0:
            loads[4].wait()
            loads[5].wait()
        mixed = tokens_ref[part].astype(jnp.float32) + jnp.dot(
            gated.astype(jnp.bfloat16), w_out_ref[...], preferred_element_type=jnp.float32
        )
        out_buf[part] = mixed.astype(jnp.bfloat16)
        rows = pl.ds(side * half, half)
        stores.append(
            pltpu.make_async_copy(out_buf.at[rows], out_hbm.at[rows], store_sem.at[side])
        )
        stores[-1].start()
    for store in stores:
        store.wait()


def solution(mesh):
    parts = mesh.shape["pb"]

    def body(tokens, stamps, norm_gain, w_proj, rel_bias, attn_gain, w_out):
        rows, width = tokens.shape
        heads = rel_bias.shape[0]
        splits = parts // heads
        near = heads // 2
        blocks_per_tile = max(1, 384 // rows)
        att, part, gate = pl.pallas_call(
            functools.partial(kernel, parts, heads),
            out_shape=[
                jax.ShapeDtypeStruct((heads, rows // 2, LANES), jnp.bfloat16),
                jax.ShapeDtypeStruct((near, rows // 2, LANES), jnp.bfloat16),
                jax.ShapeDtypeStruct((rows, width), jnp.bfloat16),
            ],
            in_specs=[pl.BlockSpec(memory_space=pltpu.HBM)] * 5,
            out_specs=[pl.BlockSpec(memory_space=pltpu.HBM)] * 3,
            scratch_shapes=[
                pltpu.VMEM((rows, width), jnp.bfloat16),
                pltpu.VMEM((1, rows), jnp.int32),
                pltpu.VMEM((1, width), jnp.float32),
                pltpu.VMEM(w_proj.shape, jnp.bfloat16),
                pltpu.SMEM(rel_bias.shape, jnp.float32),
                pltpu.VMEM((near, 2, rows, LANES), jnp.bfloat16),
                pltpu.VMEM((near, 2, rows // 2, LANES), jnp.bfloat16),
                pltpu.VMEM((parts, 2, rows, LANES), jnp.bfloat16),
                pltpu.VMEM((heads, 2, rows // 2, LANES), jnp.bfloat16),
                pltpu.VMEM((3, near, rows, LANES), jnp.bfloat16),
                pltpu.VMEM((parts, 1, rows), jnp.int32),
                pltpu.VMEM((parts // blocks_per_tile, 1, blocks_per_tile * rows), jnp.int32),
                pltpu.VMEM((heads, rows, LANES), jnp.int32),
                pltpu.VMEM((3, near, rows, LANES), jnp.float32),
                pltpu.VMEM((rows, width), jnp.bfloat16),
                pltpu.VMEM((3, near, rows // 2, LANES), jnp.bfloat16),
                pltpu.VMEM((near, rows // 2, LANES), jnp.bfloat16),
                pltpu.SemaphoreType.DMA((6,)),
                pltpu.SemaphoreType.DMA,
                pltpu.SemaphoreType.DMA,
                pltpu.SemaphoreType.DMA,
                pltpu.SemaphoreType.DMA((2,)),
                pltpu.SemaphoreType.DMA((parts,)),
                pltpu.SemaphoreType.DMA((near,)),
                pltpu.SemaphoreType.DMA,
                pltpu.SemaphoreType.DMA((2,)),
                pltpu.SemaphoreType.DMA((2,)),
                pltpu.SemaphoreType.DMA((3,)),
                pltpu.SemaphoreType.DMA,
                pltpu.SemaphoreType.DMA,
                pltpu.SemaphoreType.REGULAR,
                pltpu.SemaphoreType.DMA((4,)),
            ],
            compiler_params=pltpu.CompilerParams(
                collective_id=0, has_side_effects=True
            ),
        )(
            tokens,
            stamps.reshape(1, rows),
            norm_gain.reshape(1, width),
            w_proj,
            rel_bias,
        )
        hbm = pl.BlockSpec(memory_space=pltpu.HBM)
        return pl.pallas_call(
            final_kernel,
            out_shape=jax.ShapeDtypeStruct((rows, width), jnp.bfloat16),
            in_specs=[hbm] * 6,
            out_specs=hbm,
            scratch_shapes=[
                pltpu.VMEM((heads, rows // 2, LANES), jnp.bfloat16),
                pltpu.VMEM((near, rows // 2, LANES), jnp.bfloat16),
                pltpu.VMEM((rows, width), jnp.bfloat16),
                pltpu.VMEM((rows, width), jnp.bfloat16),
                pltpu.VMEM((1, width), jnp.float32),
                pltpu.VMEM(w_out.shape, jnp.bfloat16),
                pltpu.VMEM((rows, width), jnp.bfloat16),
                pltpu.SemaphoreType.DMA((6,)),
                pltpu.SemaphoreType.DMA((2,)),
            ],
        )(att, part, gate, tokens, attn_gain.reshape(1, width), w_out)

    return jax.shard_map(
        body,
        mesh=mesh,
        in_specs=(P(("groups", "pb"), None), P(("groups", "pb")), P(), P(), P(), P(), P()),
        out_specs=P(("groups", "pb"), None),
        check_vma=False,
    )
```

```python
import functools

import jax
import jax.numpy as jnp
from jax import lax
from jax.experimental import pallas as pl
from jax.experimental.pallas import tpu as pltpu
from jax.sharding import PartitionSpec as P

EPSILON = 1e-05
LANES = 128


def layer_norm(values, gain):
    centered = values - jnp.mean(values, axis=-1, keepdims=True)
    spread = jnp.mean(centered * centered, axis=-1, keepdims=True)
    return centered * lax.rsqrt(spread + EPSILON) * gain


LANE_LOOKUP = lax.GatherDimensionNumbers(
    offset_dims=(),
    collapsed_slice_dims=(1,),
    start_index_map=(1,),
    operand_batching_dims=(0,),
    start_indices_batching_dims=(0,),
)
ROW_LOOKUP = lax.GatherDimensionNumbers(
    offset_dims=(),
    collapsed_slice_dims=(1,),
    start_index_map=(1,),
    operand_batching_dims=(0, 2),
    start_indices_batching_dims=(0, 2),
)


def look_up(table, index, dimensions):
    return lax.gather(
        table,
        index[..., None],
        dimensions,
        (1,) * table.ndim,
        mode=lax.GatherScatterMode.PROMISE_IN_BOUNDS,
    )


def kernel(
    parts,
    heads,
    tokens_hbm,
    stamps_hbm,
    norm_gain_hbm,
    w_proj_hbm,
    bias_hbm,
    att_out,
    part_out,
    gate_out,
    tokens_ref,
    stamps_ref,
    norm_gain_ref,
    w_proj_ref,
    bias_ref,
    kv_send,
    q_send,
    kv_all,
    q_all,
    query_buf,
    stamp_all,
    stamp_keys,
    stamp_rows,
    total_buf,
    gate_buf,
    back_buf,
    zero_buf,
    load_sem,
    kv_send_sem,
    q_send_sem,
    far_send_sem,
    fwd_sem,
    kv_sem,
    q_sem,
    far_q_sem,
    stamp_send_sem,
    stamp_sem,
    back_sem,
    att_sem,
    part_sem,
    far_ready,
    own_sem,
):
    rows, width = tokens_ref.shape
    half = rows // 2
    head_size = width // heads
    splits = parts // heads
    near = heads // 2
    side = parts // 2
    blocks_per_tile = max(1, 384 // rows)
    key_tile = blocks_per_tile * rows
    group_tiles = splits // blocks_per_tile
    buckets = bias_ref.shape[1]

    loads = [
        pltpu.make_async_copy(source, target, load_sem.at[index])
        for index, (source, target) in enumerate(
            [
                (tokens_hbm, tokens_ref),
                (norm_gain_hbm, norm_gain_ref),
                (w_proj_hbm.at[:, width:], w_proj_ref.at[:, width:]),
                (stamps_hbm, stamps_ref),
                (bias_hbm, bias_ref),
                (w_proj_hbm.at[:, :width], w_proj_ref.at[:, :width]),
            ]
        )
    ]
    for load in loads:
        load.start()

    me = lax.axis_index("pb")
    my_group = me // splits
    my_split = me % splits
    upper = my_group // near
    my_place = my_group % near
    near_first = upper * near
    far_first = near - near_first
    side_first = upper * side

    def split_of(block):
        place = block % splits
        odd = (block // splits) % 2
        return place + odd * (splits - 1 - 2 * place)

    def block_of(slot, split):
        odd = slot % 2
        return slot * splits + split + odd * (splits - 1 - 2 * split)

    def remote(source, target, send, receive, device):
        return pltpu.make_async_remote_copy(
            src_ref=source,
            dst_ref=target,
            send_sem=send,
            recv_sem=receive,
            device_id={"pb": device},
            device_id_type=pl.DeviceIdType.MESH,
        )

    barrier = pltpu.get_barrier_semaphore()

    def signal(semaphore, other):
        pl.semaphore_signal(
            semaphore, inc=1, device_id={"pb": other}, device_id_type=pl.DeviceIdType.MESH
        )

    def near_peer(step):
        return side_first + lax.rem(me - side_first + step, side)

    def far_peer(step):
        return side - side_first + lax.rem(me - side_first + step, side)

    def greet(step, carry):
        signal(barrier, near_peer(step))
        return carry

    lax.fori_loop(1, side, greet, 0)
    signal(barrier, far_peer(0))

    low = lax.broadcasted_iota(jnp.int32, (1, LANES), 1) < head_size

    for load in loads[:3]:
        load.wait()
    normed = layer_norm(tokens_ref[...].astype(jnp.float32), norm_gain_ref[...]).astype(jnp.bfloat16)
    front = jnp.dot(normed, w_proj_ref[:, width : 2 * width], preferred_element_type=jnp.float32)
    scaled = front.astype(jnp.bfloat16).astype(jnp.float32) * (0.5 * head_size ** (-0.5))
    back = jnp.dot(normed, w_proj_ref[:, 2 * width :], preferred_element_type=jnp.float32)
    for pair in range(near):
        cols = slice(pair * LANES, (pair + 1) * LANES)
        key_cols = back[:, :width][:, cols]
        value_cols = back[:, width:][:, cols]
        query_cols = scaled[:, cols]
        kv_send[pair, 0] = jnp.where(
            low, key_cols, pltpu.roll(value_cols, head_size, 1)
        ).astype(jnp.bfloat16)
        kv_send[pair, 1] = jnp.where(
            low, pltpu.roll(key_cols, head_size, 1), value_cols
        ).astype(jnp.bfloat16)
        top, bottom = query_cols[:half], query_cols[half:]
        q_send[pair, 0] = jnp.where(low, top, pltpu.roll(bottom, head_size, 1)).astype(jnp.bfloat16)
        q_send[pair, 1] = jnp.where(low, pltpu.roll(top, head_size, 1), bottom).astype(jnp.bfloat16)
    loads[3].wait()
    loads[4].wait()

    my_home = split_of(me)

    def stamp_copy(target, kind):
        return remote(
            stamps_ref, stamp_all.at[me], stamp_send_sem.at[kind], stamp_sem.at[kind], target
        )

    def all_stamps(kind):
        some = stamp_all.at[pl.ds(0, side - 1 + kind)]
        return remote(some, some, stamp_send_sem.at[kind], stamp_sem.at[kind], near_peer(1))

    def kv_copy(place, target):
        return remote(kv_send.at[place], kv_all.at[me], kv_send_sem, kv_sem.at[me], target)

    def q_copy(place, target):
        return remote(
            q_send.at[place], q_all.at[my_group], q_send_sem, q_sem.at[my_place], target
        )

    def late_kv_copy(place, target):
        return remote(
            kv_send.at[place, 1], kv_all.at[me, 1], far_send_sem, kv_sem.at[me], target
        )

    def early_q_copy(place, target):
        return remote(
            q_send.at[place, 0], q_all.at[my_group, 0], far_send_sem, far_q_sem, target
        )

    def each_near(act):
        def one(step, carry):
            place = my_place ^ step
            target = (near_first + place) * splits + my_home

            @pl.when(target != me)
            def _():
                act(place, target)

            return carry

        lax.fori_loop(0, near, one, 0)

    relays = (1 - upper) * (my_place // (near // 2)) * (near // 2)
    farther = jnp.maximum(relays, upper * (near // 2))

    def far_place(step):
        place = step + (my_place % 2) * (1 - 2 * (step % 2))
        return place + upper * (near - 1 - 2 * place)

    def each_far(first, count, act):
        def one(step, carry):
            place = far_place(step)
            target = (far_first + place) * splits + my_home

            @pl.when(upper == 0)
            def _():
                act(late_kv_copy(place, target))

            @pl.when(upper == 1)
            def _():
                act(early_q_copy(place, target))

            return carry

        lax.fori_loop(first, first + count, one, 0)

    def send_near_stamps(step, carry):
        stamp_copy(near_peer(step), 0).start()
        return carry

    def send_far_stamps(step, carry):
        stamp_copy(far_peer(step), 1).start()
        return carry

    def start_both(place, target):
        q_copy(place, target).start()
        kv_copy(place, target).start()

    pl.semaphore_wait(barrier, side)

    def pass_on(step, carry):
        signal(far_ready, near_peer(step))
        return carry

    lax.fori_loop(1, side, pass_on, 0)
    lax.fori_loop(1, side, send_near_stamps, 0)
    each_near(start_both)

    stamp_all[me] = stamps_ref[...]

    @pl.when(my_home == my_split)
    def _():
        kv_all[me] = kv_send[my_place]
        q_all[my_group] = q_send[my_place]

    gate_store = pltpu.make_async_copy(gate_buf, gate_out, own_sem.at[2])
    no_part = pltpu.make_async_copy(zero_buf, part_out, own_sem.at[3])

    @pl.when(upper == 0)
    def _():
        zero_buf[...] = jnp.zeros_like(zero_buf)
        no_part.start()

    loads[5].wait()
    gate_proj = jnp.dot(normed, w_proj_ref[:, :width], preferred_element_type=jnp.float32)
    gate_buf[...] = jax.nn.silu(gate_proj).astype(jnp.bfloat16)
    gate_store.start()
    total_buf[...] = jnp.zeros_like(total_buf)

    pl.semaphore_wait(far_ready, side - 1)
    lax.fori_loop(0, side, send_far_stamps, 0)
    each_far(0, near // 2, lambda copy: copy.start())

    lane_id = lax.broadcasted_iota(jnp.int32, (8, LANES), 1)
    place_id = lax.broadcasted_iota(jnp.int32, (8, LANES), 0)

    def tables_of(head):
        def half_bias(bucket):
            table = jnp.zeros((8, LANES), jnp.float32)
            for bucket_id in range(buckets):
                table = jnp.where(bucket == bucket_id, 0.5 * bias_ref[head, bucket_id], table)
            return table

        return (
            half_bias(jnp.clip((33 - lane_id) >> 1, 0, buckets - 1))[:1],
            half_bias(jnp.where(place_id == 0, 8, 16 - place_id)),
            half_bias(jnp.where(place_id == 0, 0, 8 - place_id)),
        )

    near_tables = [tables_of(2 * my_place), tables_of(2 * my_place + 1)]
    square_tables = [tables_of(2 * my_place + upper)]

    def biases_of(elapsed, tables, by_rows):
        if not by_rows:
            index = lax.clz(elapsed)
            return [look_up(jnp.broadcast_to(lane, elapsed.shape), index, LANE_LOOKUP) for lane, _, _ in tables]
        tiles = (elapsed.shape[0] // 8, 8, LANES)
        zeros_count = lax.clz(jnp.minimum(elapsed, 2**30 - 1))
        index = ((zeros_count >> 1) & 7).reshape(tiles)
        old = elapsed >= 4**7
        biases = []
        for _, far_table, close_table in tables:
            far_bias = look_up(jnp.broadcast_to(far_table[None], tiles), index, ROW_LOOKUP)
            close_bias = look_up(jnp.broadcast_to(close_table[None], tiles), index, ROW_LOOKUP)
            biases.append(
                jnp.where(old, far_bias.reshape(elapsed.shape), close_bias.reshape(elapsed.shape))
            )
        return biases

    def join_stamps(tile, carry):
        stamp_keys[tile] = jnp.concatenate(
            [stamp_all[tile * blocks_per_tile + place] for place in range(blocks_per_tile)], axis=1
        )
        return carry

    def turn_stamps(slot, carry):
        block = block_of(slot, my_split)
        stamp_rows[slot] = jnp.transpose(jnp.broadcast_to(stamp_all[block], (LANES, rows)))
        return carry

    all_stamps(0).wait_recv()
    lax.fori_loop(near_first * group_tiles, (near_first + near) * group_tiles, join_stamps, 0)
    lax.fori_loop(near_first, near_first + near, turn_stamps, 0)

    def forward(source, step):
        peer = my_group * splits + lax.rem(my_split + step, splits)
        return remote(
            kv_all.at[source], kv_all.at[source], fwd_sem.at[0], kv_sem.at[source], peer
        )

    def late_forward(source, step):
        peer = my_group * splits + lax.rem(my_split + step, splits)
        return remote(
            kv_all.at[source, 1], kv_all.at[source, 1], fwd_sem.at[1], kv_sem.at[source], peer
        )

    def relay(source):
        return remote(
            kv_all.at[source, 1],
            kv_all.at[source, 1],
            fwd_sem.at[1],
            kv_sem.at[source],
            (far_first + my_place) * splits + my_split,
        )

    def take_direct(slot):
        source = block_of(slot, my_split)

        @pl.when(source != me)
        def _():
            remote(
                kv_send.at[0], kv_all.at[source], kv_send_sem, kv_sem.at[source], source
            ).wait_recv()

        for step in range(1, splits):
            forward(source, step).start()

        @pl.when(slot < relays)
        def _():
            relay(source).start()

    def take_forwarded(slot):
        for step in range(1, splits):
            source = block_of(slot, lax.rem(my_split + step, splits))
            forward(source, step).wait_recv()

    def take_late_direct(slot):
        source = block_of(slot, my_split)
        remote(
            kv_send.at[0, 1], kv_all.at[source, 1], far_send_sem, kv_sem.at[source], source
        ).wait_recv()
        for step in range(1, splits):
            late_forward(source, step).start()

    def take_late_forwarded(slot):
        for step in range(1, splits):
            source = block_of(slot, lax.rem(my_split + step, splits))
            late_forward(source, step).wait_recv()

    def unpack(packed):
        packed = packed.astype(jnp.float32)
        return jnp.concatenate(
            [jnp.where(low, packed, 0.0), jnp.where(low, pltpu.roll(packed, head_size, 1), 0.0)], axis=0
        ).astype(jnp.bfloat16)

    def take_query(slot):
        source = block_of(slot, my_split)

        @pl.when(source != me)
        def _():
            remote(
                q_send.at[0], q_all.at[slot], q_send_sem, q_sem.at[slot - near_first], source
            ).wait_recv()

        for head in range(2):
            query_buf[head, slot - near_first] = unpack(q_all[slot, head])

    def take_far_query(slot, carry):
        query_buf[2, slot - near] = unpack(q_all[slot, 0])
        return carry

    def all_far_queries():
        some = q_all.at[pl.ds(0, near), 0]
        return remote(some, some, far_send_sem, far_q_sem, near_peer(1))

    chunk = 64
    row_id = lax.broadcasted_iota(jnp.int32, (chunk, LANES), 0)
    col_id = lax.broadcasted_iota(jnp.int32, (chunk, LANES), 1)
    spread = col_id - row_id

    def visit_tiles(sections, jobs, tables):
        for slot, count, tile, span, masked in sections:
            unit = slot - jnp.where(slot >= near, near, 0)
            keys = span * key_tile
            key_values, scores = [], []
            for query_head, key_head in jobs:
                key_value = kv_all[pl.ds(tile * blocks_per_tile, span * blocks_per_tile), key_head]
                key_values.append(key_value.reshape(keys, LANES))
                queries = query_buf[query_head, pl.ds(unit, count)].reshape(count * rows, LANES)
                scores.append(
                    lax.dot_general(
                        queries,
                        key_values[-1],
                        (((1,), (1,)), ((), ())),
                        preferred_element_type=jnp.float32,
                    )
                )
            weights = [[] for _ in jobs]
            for first in range(0, keys, LANES):
                columns = [[] for _ in jobs]
                key_stamp = stamp_keys[
                    tile + first // key_tile, :, first % key_tile : first % key_tile + LANES
                ]
                for top in range(0, count * rows, chunk):
                    place, start = top // rows, top % rows
                    query_stamp = stamp_rows[slot + place, start : start + chunk]
                    elapsed = query_stamp - key_stamp
                    biases = biases_of(elapsed, tables, (top // chunk + first // LANES) % 3 != 0)
                    for score, bias, column in zip(scores, biases, columns):
                        halved = score[top : top + chunk, first : first + LANES] + bias
                        weight = halved + halved * jnp.tanh(halved)
                        if masked:
                            ahead = tile * key_tile + first - block_of(slot, my_split) * rows - start
                            weight = jnp.where(spread <= -ahead, weight, 0.0)
                        column.append(weight.astype(jnp.bfloat16))
                for weight, column in zip(weights, columns):
                    weight.append(jnp.concatenate(column, axis=0))
            for (query_head, _), weight, key_value in zip(jobs, weights, key_values):
                sums = jnp.dot(
                    jnp.concatenate(weight, axis=1), key_value, preferred_element_type=jnp.float32
                )
                total_buf[query_head, pl.ds(unit, count)] += sums.reshape(count, rows, LANES)

    def visit(sections, jobs, tables):
        def one(step, carry):
            visit_tiles(
                [
                    (slot, count, group * group_tiles + span * step, span, masked)
                    for slot, count, group, span, masked in sections
                ],
                jobs,
                tables,
            )
            return carry

        if group_tiles == 1:
            one(0, 0)
        else:
            lax.fori_loop(0, group_tiles, one, 0)

    def visit_near(*pairs):
        visit(
            [
                (jnp.maximum(one, other), 1, jnp.minimum(one, other), 1, masked)
                for one, other, masked in pairs
            ],
            [(0, 0), (1, 1)],
            near_tables,
        )

    def back_copy(kind, unit):
        slot = unit + (near if kind == 2 else near_first)
        target, semaphore = (
            (part_out.at[my_place], part_sem)
            if kind == 2
            else (att_out.at[2 * my_place + kind], att_sem)
        )
        block = block_of(slot, my_split)
        return block, remote(
            back_buf.at[kind, unit], target, back_sem.at[kind], semaphore, block
        )

    def own_copy(kind, unit):
        return pltpu.make_async_copy(
            back_buf.at[kind, unit], att_out.at[2 * my_place + kind], own_sem.at[kind]
        )

    def finish(kinds, first, count):
        def one(unit, carry):
            results = []
            for kind in kinds:
                total = total_buf[kind, unit]
                result = jnp.where(low, pltpu.roll(total[:half], head_size, 1), total[half:])
                results.append(result.astype(jnp.bfloat16))
            for kind, result in zip(kinds, results):
                back_buf[kind, unit] = result
            for kind in kinds:
                block, copy = back_copy(kind, unit)
                if kind == 2:
                    copy.start()
                    continue

                @pl.when(block == me)
                def _(kind=kind):
                    own_copy(kind, unit).start()

                @pl.when(block != me)
                def _(copy=copy):
                    copy.start()

            return carry

        lax.fori_loop(first, first + count, one, 0)

    def near_at(step):
        return near_first + (my_place ^ step)

    take_direct(near_at(0))

    def near_step(step, carry):
        group = near_at(step)

        @pl.when((step == 1) & (farther > 0))
        def _():
            each_far(near // 2, farther, lambda copy: copy.start())

        @pl.when(step + 1 < near)
        def _():
            take_direct(near_at(step + 1))

        take_forwarded(group)
        take_query(group)

        @pl.when((upper == 1) & (step + 1 == near))
        def _():
            for late in range(near // 2, near):
                take_late_direct(late)

        @pl.when(step == 0)
        def _():
            visit_near((group, group, True))

        @pl.when(step > 0)
        def _():
            visit_near((group, group, True), (group, near_at(step - 1), False))

        def two(pair, inner):
            visit_near((group, near_at(2 * pair), False), (group, near_at(2 * pair + 1), False))
            return inner

        lax.fori_loop(0, jnp.maximum(step - 1, 0) // 2, two, 0)

        @pl.when((step > 1) & (step % 2 == 0))
        def _():
            visit_near((group, near_at(step - 2), False))

        return carry

    lax.fori_loop(0, near, near_step, 0)

    @pl.when(upper == 0)
    def _():
        finish((0, 1), 0, near)
        all_stamps(1).wait_recv()
        lax.fori_loop(near, 2 * near, turn_stamps, 0)
        all_far_queries().wait_recv()
        lax.fori_loop(near, 2 * near, take_far_query, 0)

    @pl.when(upper == 1)
    def _():
        for late in range(near // 2):
            take_late_direct(late)
        finish((0,), 0, near)
        all_stamps(1).wait_recv()
        lax.fori_loop(0, near * group_tiles, join_stamps, 0)

    halves = near // 2

    def square(step, carry):
        major, minor = step // halves, step % halves
        slots = 2 * jnp.where(upper == 0, halves - 1 - major, minor)
        groups = 2 * (halves - 1 - jnp.where(upper == 0, minor, major))

        @pl.when((upper == 1) & (minor == 0))
        def _():
            take_late_forwarded(groups)
            take_late_forwarded(groups + 1)

        visit([(near + slots, 2, groups, 2, False)], [(2 - upper, upper)], square_tables)

        @pl.when((upper == 0) & (minor == halves - 1))
        def _():
            finish((2,), slots, 2)

        @pl.when((upper == 1) & (major == halves - 1))
        def _():
            finish((1,), slots, 2)

        return carry

    lax.fori_loop(0, halves * halves, square, 0)

    all_stamps(0).wait_send()
    all_stamps(1).wait_send()

    def forwards():
        some = kv_all.at[pl.ds(0, near * (splits - 1))]
        return remote(some, some, fwd_sem.at[0], fwd_sem.at[0], near_peer(1))

    def late_forwards():
        some = kv_all.at[pl.ds(0, near * (splits - 1)), 1]
        return remote(some, some, fwd_sem.at[1], fwd_sem.at[1], near_peer(1))

    def wait_near(count):
        some = kv_all.at[pl.ds(0, count)]
        remote(some, some, kv_send_sem, kv_send_sem, near_peer(1)).wait_send()
        some = q_all.at[pl.ds(0, count)]
        remote(some, some, q_send_sem, q_send_sem, near_peer(1)).wait_send()

    def results(count, send, receive):
        some = att_out.at[pl.ds(0, count)]
        return remote(some, some, send, receive, near_peer(1))

    home = my_home == my_split
    forwards().wait_send()

    @pl.when(home)
    def _():
        wait_near(near - 1)
        results(2 * near - 2, att_sem, att_sem).wait_recv()
        for kind in range(2):
            own_copy(kind, 0).wait()
            results(near - 1, back_sem.at[kind], back_sem.at[kind]).wait_send()

    @pl.when(jnp.logical_not(home))
    def _():
        wait_near(near)
        results(2 * near, att_sem, att_sem).wait_recv()
        for kind in range(2):
            results(near, back_sem.at[kind], back_sem.at[kind]).wait_send()

    @pl.when(upper == 0)
    def _():
        def wait_late(count, semaphore):
            some = kv_send.at[pl.ds(0, count), 1]
            remote(some, some, semaphore, semaphore, near_peer(1)).wait_send()

        wait_late(near // 2, far_send_sem)

        @pl.when(relays > 0)
        def _():
            wait_late(near // 2, far_send_sem)
            wait_late(near // 2, fwd_sem.at[1])

        results(near, back_sem.at[2], back_sem.at[2]).wait_send()
        no_part.wait()

    @pl.when(upper == 1)
    def _():
        all_far_queries().wait_send()
        late_forwards().wait_send()
        results(near, part_sem, part_sem).wait_recv()

    gate_store.wait()


def final_kernel(
    att_hbm,
    part_hbm,
    gate_hbm,
    tokens_hbm,
    attn_gain_hbm,
    w_out_hbm,
    out_hbm,
    att_buf,
    part_buf,
    gate_buf,
    tokens_ref,
    attn_gain_ref,
    w_out_ref,
    out_buf,
    load_sem,
    store_sem,
):
    loads = [
        pltpu.make_async_copy(source, target, load_sem.at[index])
        for index, (source, target) in enumerate(
            [
                (att_hbm, att_buf),
                (part_hbm, part_buf),
                (gate_hbm, gate_buf),
                (attn_gain_hbm, attn_gain_ref),
                (w_out_hbm, w_out_ref),
                (tokens_hbm, tokens_ref),
            ]
        )
    ]
    for load in loads:
        load.start()
    heads, half, _ = att_buf.shape
    head_size = tokens_ref.shape[1] // heads
    low = lax.broadcasted_iota(jnp.int32, (1, LANES), 1) < head_size
    for load in loads[:4]:
        load.wait()
    stores = []
    for side in range(2):
        pieces = []
        for pair in range(heads // 2):
            even = att_buf[2 * pair].astype(jnp.float32) + part_buf[pair].astype(jnp.float32)
            odd = att_buf[2 * pair + 1].astype(jnp.float32)
            if side == 0:
                pieces.append(jnp.where(low, even, pltpu.roll(odd, head_size, 1)))
            else:
                pieces.append(jnp.where(low, pltpu.roll(even, head_size, 1), odd))
        attended = jnp.concatenate(pieces, axis=1)
        part = slice(side * half, (side + 1) * half)
        gated = layer_norm(attended, attn_gain_ref[...]) * gate_buf[part].astype(jnp.float32)
        if side == 0:
            loads[4].wait()
            loads[5].wait()
        mixed = tokens_ref[part].astype(jnp.float32) + jnp.dot(
            gated.astype(jnp.bfloat16), w_out_ref[...], preferred_element_type=jnp.float32
        )
        out_buf[part] = mixed.astype(jnp.bfloat16)
        rows = pl.ds(side * half, half)
        stores.append(
            pltpu.make_async_copy(out_buf.at[rows], out_hbm.at[rows], store_sem.at[side])
        )
        stores[-1].start()
    for store in stores:
        store.wait()


def solution(mesh):
    parts = mesh.shape["pb"]

    def body(tokens, stamps, norm_gain, w_proj, rel_bias, attn_gain, w_out):
        rows, width = tokens.shape
        heads = rel_bias.shape[0]
        splits = parts // heads
        near = heads // 2
        blocks_per_tile = max(1, 384 // rows)
        att, part, gate = pl.pallas_call(
            functools.partial(kernel, parts, heads),
            out_shape=[
                jax.ShapeDtypeStruct((heads, rows // 2, LANES), jnp.bfloat16),
                jax.ShapeDtypeStruct((near, rows // 2, LANES), jnp.bfloat16),
                jax.ShapeDtypeStruct((rows, width), jnp.bfloat16),
            ],
            in_specs=[pl.BlockSpec(memory_space=pltpu.HBM)] * 5,
            out_specs=[pl.BlockSpec(memory_space=pltpu.HBM)] * 3,
            scratch_shapes=[
                pltpu.VMEM((rows, width), jnp.bfloat16),
                pltpu.VMEM((1, rows), jnp.int32),
                pltpu.VMEM((1, width), jnp.float32),
                pltpu.VMEM(w_proj.shape, jnp.bfloat16),
                pltpu.SMEM(rel_bias.shape, jnp.float32),
                pltpu.VMEM((near, 2, rows, LANES), jnp.bfloat16),
                pltpu.VMEM((near, 2, rows // 2, LANES), jnp.bfloat16),
                pltpu.VMEM((parts, 2, rows, LANES), jnp.bfloat16),
                pltpu.VMEM((heads, 2, rows // 2, LANES), jnp.bfloat16),
                pltpu.VMEM((3, near, rows, LANES), jnp.bfloat16),
                pltpu.VMEM((parts, 1, rows), jnp.int32),
                pltpu.VMEM((parts // blocks_per_tile, 1, blocks_per_tile * rows), jnp.int32),
                pltpu.VMEM((heads, rows, LANES), jnp.int32),
                pltpu.VMEM((3, near, rows, LANES), jnp.float32),
                pltpu.VMEM((rows, width), jnp.bfloat16),
                pltpu.VMEM((3, near, rows // 2, LANES), jnp.bfloat16),
                pltpu.VMEM((near, rows // 2, LANES), jnp.bfloat16),
                pltpu.SemaphoreType.DMA((6,)),
                pltpu.SemaphoreType.DMA,
                pltpu.SemaphoreType.DMA,
                pltpu.SemaphoreType.DMA,
                pltpu.SemaphoreType.DMA((2,)),
                pltpu.SemaphoreType.DMA((parts,)),
                pltpu.SemaphoreType.DMA((near,)),
                pltpu.SemaphoreType.DMA,
                pltpu.SemaphoreType.DMA((2,)),
                pltpu.SemaphoreType.DMA((2,)),
                pltpu.SemaphoreType.DMA((3,)),
                pltpu.SemaphoreType.DMA,
                pltpu.SemaphoreType.DMA,
                pltpu.SemaphoreType.REGULAR,
                pltpu.SemaphoreType.DMA((4,)),
            ],
            compiler_params=pltpu.CompilerParams(
                collective_id=0, has_side_effects=True
            ),
        )(
            tokens,
            stamps.reshape(1, rows),
            norm_gain.reshape(1, width),
            w_proj,
            rel_bias,
        )
        hbm = pl.BlockSpec(memory_space=pltpu.HBM)
        return pl.pallas_call(
            final_kernel,
            out_shape=jax.ShapeDtypeStruct((rows, width), jnp.bfloat16),
            in_specs=[hbm] * 6,
            out_specs=hbm,
            scratch_shapes=[
                pltpu.VMEM((heads, rows // 2, LANES), jnp.bfloat16),
                pltpu.VMEM((near, rows // 2, LANES), jnp.bfloat16),
                pltpu.VMEM((rows, width), jnp.bfloat16),
                pltpu.VMEM((rows, width), jnp.bfloat16),
                pltpu.VMEM((1, width), jnp.float32),
                pltpu.VMEM(w_out.shape, jnp.bfloat16),
                pltpu.VMEM((rows, width), jnp.bfloat16),
                pltpu.SemaphoreType.DMA((6,)),
                pltpu.SemaphoreType.DMA((2,)),
            ],
        )(att, part, gate, tokens, attn_gain.reshape(1, width), w_out)

    return jax.shard_map(
        body,
        mesh=mesh,
        in_specs=(P(("groups", "pb"), None), P(("groups", "pb")), P(), P(), P(), P(), P()),
        out_specs=P(("groups", "pb"), None),
        check_vma=False,
    )
```
